32 devices in a mesh: tm: 2 (over x), src: 16 (over z, y, core).
Axes of the slice: x: 2, y: 2, z: 4, core: 2. Of those that a mesh axis runs over, the one named last changes fastest.
Arguments:
- design: float32 [16, 524288], P(None, ('tm', 'src')), may hold values from -2 to 2
- unit_index: int32 [524288], P(('tm', 'src')), may hold values from 0 to 255, as said below
- residual: float32 [524288], P(('tm', 'src')), may hold values from -6 to 6
- weight: float32 [524288], P(('tm', 'src')), may hold values from 0.25 to 4
- obs_count: int32 [32], P(('tm', 'src')), may hold values from 1 to 16384, as said below
- damping: float32 [256], P(('tm', 'src')), may hold values from 1 to 10
Outputs:
- solution: float32 [16, 256], P(None, ('tm', 'src'))
- misfit: float32 [], replicated
The draws below stay inside these ranges and needn't reach their ends.
Inputs may be any that keep to these rules, and one draw needn't show every extreme that they name: `unit_index`: an observation on a device of tm index g names a unit in [g * 128, (g + 1) * 128). `obs_count`: some device has all 16384 slots live.
All inputs are finite; a program needn't handle non-finite values.
Results may differ from the reference program's by a relative error of at most 0.0003.
Values sent between devices are 32-bit elements; how exact they have to be, the bound alone decides.
A program may use at most 64 MiB of HBM per device.

```python
import math
import jax
import jax.numpy as jnp
from jax import lax

WIDTH = 16
OBS_DEV = 16384
UNITS_GRP = 128
UNITS = 256
OBS_ALL = 524288
N_SRC = 16
DEVICES = 32


def draw_unit_index(key, part):
    total = OBS_DEV * DEVICES
    group = jnp.arange(total, dtype=jnp.int32) // (OBS_DEV * N_SRC)
    picks = jax.random.randint(jax.random.fold_in(key, 11), (total,), 0, UNITS_GRP, dtype=jnp.int32)
    return picks + group * UNITS_GRP


def draw_obs_count(key, part):
    counts = jax.random.randint(jax.random.fold_in(key, 23), (DEVICES,), OBS_DEV // 8, OBS_DEV // 2 + 1, dtype=jnp.int32)
    return counts.at[0].set(OBS_DEV)


def block_scale(stream_key, extent, shards, least, top_value):
    def one(axis_at, blocks):
        steps = jax.random.uniform(jax.random.fold_in(jax.random.fold_in(stream_key, 6), axis_at), (blocks,), jnp.float32, least / len(shards), top_value / len(shards))
        return jnp.repeat(jnp.exp(steps), extent[axis_at] // blocks).reshape((-1,) + (1,) * (len(extent) - axis_at - 1))

    factor_of = one(*shards[0])
    for cut in shards[1:]:
        factor_of = factor_of * one(*cut)
    return factor_of


def bell_draw(own_key, dims, spread, bound, pieces=(), held_as=jnp.bfloat16):
    entries = spread * jax.random.normal(own_key, dims, jnp.float32)
    if pieces:
        entries = entries * block_scale(own_key, dims, pieces, -0.22, 0.18)
    return jnp.clip(entries, -bound, bound).astype(held_as)


def setup_inputs(seed: int = 0) -> dict:
    key_of = jax.random.split(jax.random.key(seed), 7)
    design = bell_draw(key_of[0], (WIDTH, OBS_ALL), 0.25, 2.0, ((1, 32),), jnp.float32)
    unit_index = draw_unit_index(jax.random.fold_in(key_of[6], 71), 0)
    residual = bell_draw(key_of[2], (OBS_ALL,), 1.0, 6.0, ((0, 32),), jnp.float32)
    weight = jnp.clip(jnp.exp(math.log(4.0) - 2.7725887 * jax.random.uniform(key_of[3], (OBS_ALL,), jnp.float32) ** block_scale(key_of[3], (OBS_ALL,), ((0, 32),), -0.2, 0.2)), 0.25, 4.0)
    obs_count = draw_obs_count(jax.random.fold_in(key_of[6], 71), 0)
    damping = jnp.clip(jnp.exp(math.log(10.0) - 2.3025851 * jax.random.uniform(key_of[5], (UNITS,), jnp.float32) ** block_scale(key_of[5], (UNITS,), ((0, 32),), -0.2, 0.2)), 1.0, 10.0)
    return dict(design=design, unit_index=unit_index, residual=residual, weight=weight, obs_count=obs_count, damping=damping)


def block_solve(normal, rhs, damping):
    lower = {}
    for j in range(16):
        running = normal[j * 16 + j] + damping
        for k in range(j):
            running = running - lower[j, k] * lower[j, k]
        diag_term = jnp.sqrt(running)
        lower[j, j] = diag_term
        for i in range(j + 1, 16):
            running = normal[i * 16 + j]
            for k in range(j):
                running = running - lower[i, k] * lower[j, k]
            lower[i, j] = running / diag_term
    forward = []
    for i in range(16):
        running = rhs[i]
        for k in range(i):
            running = running - lower[i, k] * forward[k]
        forward.append(running / lower[i, i])
    backward = [None] * 16
    for i in range(15, -1, -1):
        running = forward[i]
        for k in range(i + 1, 16):
            running = running - lower[k, i] * backward[k]
        backward[i] = running / lower[i, i]
    return jnp.stack(backward)

def reference(design, unit_index, residual, weight, obs_count, damping):
    units = damping.shape[0]
    blocks = obs_count.shape[0]
    design_blocks = design.reshape(16, blocks, -1).transpose(1, 0, 2)
    unit_blocks = unit_index.reshape(blocks, -1)
    resid_blocks = residual.reshape(blocks, -1)
    weight_blocks = weight.reshape(blocks, -1)
    slots = design_blocks.shape[2]

    def accumulate(carry, item):
        normal_sum, rhs_sum, weight_sum = carry
        rows, units_of, resid, weights, count = item
        weights_on = jnp.where(jnp.arange(slots, dtype=jnp.int32) < count, weights, jnp.zeros_like(weights))
        outer = (rows[:, None, :] * rows[None, :, :]).reshape(256, slots) * weights_on
        normal_sum = normal_sum.at[:, units_of].add(outer)
        rhs_sum = rhs_sum.at[:, units_of].add(rows * (weights_on * resid))
        return ((normal_sum, rhs_sum, weight_sum + jnp.sum(weights_on)), None)
    start = (jnp.zeros((256, units), jnp.float32), jnp.zeros((16, units), jnp.float32), jnp.zeros((), jnp.float32))
    (normal, rhs, weight_total), _ = lax.scan(accumulate, start, (design_blocks, unit_blocks, resid_blocks, weight_blocks, obs_count))
    solution = block_solve(normal, rhs, damping)

    def squares(carry, item):
        rows, units_of, resid, weights, count = item
        weights_on = jnp.where(jnp.arange(slots, dtype=jnp.int32) < count, weights, jnp.zeros_like(weights))
        fitted = lax.optimization_barrier(jnp.sum(rows * solution[:, units_of], axis=0))
        after = resid - fitted
        return (carry + jnp.sum(weights_on * after * after), None)
    chi_total, _ = lax.scan(squares, jnp.zeros((), jnp.float32), (design_blocks, unit_blocks, resid_blocks, weight_blocks, obs_count))
    return (solution, chi_total / weight_total)
```

```python
import functools

import jax
import jax.numpy as jnp
from jax import lax
from jax.experimental import pallas as pl
from jax.experimental.pallas import tpu as pltpu
from jax.sharding import PartitionSpec as P

WIDTH = 16
HALF = 8
PAIRS = WIDTH * (WIDTH + 1) // 2
ROWS = PAIRS + WIDTH
LANES = 128
FOLD = 4


def pair_row(i, j):
    k = (j - i) % WIDTH
    if k > HALF or (k == HALF and i >= HALF):
        i, j = j, i
        k = (j - i) % WIDTH
    return k * WIDTH + i


def stacked_rows(d0, d1, w, wr):
    w0, w1 = d0 * w, d1 * w
    rows = [d0 * w0, d1 * w1]
    sub = lax.broadcasted_iota(jnp.int32, d0.shape, 0)
    for k in range(1, HALF):
        r0 = pltpu.roll(w0, HALF - k, 0)
        r1 = pltpu.roll(w1, HALF - k, 0)
        low = sub < HALF - k
        rows.append(d0 * jnp.where(low, r0, r1))
        rows.append(d1 * jnp.where(low, r1, r0))
    rows.append(d0 * w1)
    rows.append(d0 * wr)
    rows.append(d1 * wr)
    return rows


def rsqrt(value):
    guess = lax.rsqrt(value)
    return guess * (1.5 - 0.5 * value * guess * guess)


def solve(entry, rhs, damping):
    a = {}
    for i in range(WIDTH):
        for j in range(i + 1):
            a[i, j] = entry(i, j)
        a[i, i] = a[i, i] + damping
    b = [rhs(i) for i in range(WIDTH)]
    inverse, forward = [], []
    for j in range(WIDTH):
        inv = rsqrt(a[j, j])
        inverse.append(inv)
        for i in range(j + 1, WIDTH):
            a[i, j] = a[i, j] * inv
        y = b[j] * inv
        forward.append(y)
        for i in range(j + 1, WIDTH):
            b[i] = b[i] - a[i, j] * y
            for k in range(j + 1, i + 1):
                a[i, k] = a[i, k] - a[i, j] * a[k, j]
    run = list(forward)
    x = [None] * WIDTH
    for i in reversed(range(WIDTH)):
        x[i] = run[i] * inverse[i]
        for k in range(i):
            run[k] = run[k] - a[i, k] * x[i]
    return x, forward


def far_first(n):
    q = max(n // 4, 1)
    order = []
    for i in range(q):
        order += [3 * q + i, q + i]
    order += list(range(2 * q, 3 * q)) + list(range(1, q))
    return [p for p in dict.fromkeys(order) if 0 < p < n]


def each(pairs, body, start):
    if len(pairs) <= 32:
        for dt, dp in pairs:
            start = body(dt, dp, start)
        return start
    n_src = max(dp for _, dp in pairs) + 1
    return lax.fori_loop(
        1, len(pairs) + 1, lambda i, c: body(i // n_src, i % n_src, c), start
    )


def kernel(
    n_tm, n_src, chunk,
    count_hbm, design_hbm, unit_hbm, resid_hbm, weight_hbm, damp_hbm,
    out_ref,
    count_ref, design_ref, unit_ref, resid_ref, weight_ref, damp_ref,
    acc, extra, part, got, summed, spread, mine, heard,
    load, small, send_a, recv_a, send_b, recv_b,
):
    tm, src = lax.axis_index("tm"), lax.axis_index("src")
    n_all = n_tm * n_src
    me = tm * n_src + src
    own = damp_ref.shape[1]
    units = own * n_src
    slots = design_ref.shape[1]
    turns = slots // chunk
    order = far_first(n_src)
    near = [(0, p) for p in order]
    everyone = [(dt, p) for dt in range(n_tm - 1, 0, -1) for p in order + [0]] + near

    arrays = (
        (design_hbm, design_ref), (unit_hbm, unit_ref),
        (resid_hbm, resid_ref), (weight_hbm, weight_ref),
    )

    def fetch(step, which):
        far, here = arrays[which]
        cols = pl.ds(pl.multiple_of(step * chunk, chunk), chunk)
        return pltpu.make_async_copy(far.at[:, cols], here.at[:, cols], load.at[step, which])

    count_copy = pltpu.make_async_copy(count_hbm, count_ref, small.at[0])
    damp_copy = pltpu.make_async_copy(damp_hbm, damp_ref, small.at[1])
    count_copy.start()
    for which in range(4):
        fetch(0, which).start()
    for step in range(1, turns):
        for which in range(4):
            fetch(step, which).start()
    damp_copy.start()

    def at(dt, dp):
        return {"tm": (tm + dt) % n_tm, "src": (src + dp) % n_src}

    barrier = pltpu.get_barrier_semaphore()

    def greet(dt, dp, c):
        pl.semaphore_signal(
            barrier, inc=1, device_id=at(dt, dp), device_id_type=pl.DeviceIdType.MESH
        )
        return c

    each(everyone, greet, 0)

    first_unit = tm * units
    zero = jnp.zeros((1, LANES), jnp.float32)
    count_copy.wait()
    count = count_ref[0]

    def accumulate(step, carry):
        chi, total = carry
        for which in range(4):
            fetch(step, which).wait()
        begin = pl.multiple_of(step * chunk, chunk)
        cols = pl.ds(begin, chunk)
        w = weight_ref[:, cols]
        live = begin + lax.broadcasted_iota(jnp.int32, w.shape, 1) < count
        w = jnp.where(live, w, 0.0)
        r = resid_ref[:, cols]
        wr = w * r
        rows = stacked_rows(design_ref[0:HALF, cols], design_ref[HALF:WIDTH, cols], w, wr)
        x = jnp.concatenate(rows, axis=0)
        high = x.astype(jnp.bfloat16).astype(jnp.float32)
        lhs = jnp.concatenate([high, x - high], axis=0).astype(jnp.bfloat16)
        unit = unit_ref[:, cols] - first_unit
        hot = lax.broadcasted_iota(jnp.int32, (units, chunk), 0) == unit
        hot = jnp.where(hot, 1.0, 0.0).astype(jnp.bfloat16)
        acc[...] += lax.dot_general(
            lhs, hot, (((1,), (1,)), ((), ())), preferred_element_type=jnp.float32
        )
        wrr = wr * r
        for t in range(chunk // LANES):
            chi = chi + wrr[:, t * LANES:(t + 1) * LANES]
            total = total + w[:, t * LANES:(t + 1) * LANES]
        return chi, total

    acc[...] = jnp.zeros_like(acc)
    chi, total = lax.fori_loop(0, turns, accumulate, (zero, zero))

    sums = acc[0:ROWS] + acc[ROWS:2 * ROWS]
    left = jnp.concatenate(
        [sums[LANES:ROWS], jnp.zeros((2 * LANES - ROWS, units), jnp.float32)], axis=0
    )
    extra[...] = jnp.transpose(left)
    part[:, 0:own, :] = jnp.transpose(sums[0:LANES]).reshape(n_src, own, LANES)
    packed = extra[pl.ds(0, units // FOLD, stride=FOLD), :]
    for b in range(1, FOLD):
        packed = packed + pltpu.roll(
            extra[pl.ds(b, units // FOLD, stride=FOLD), :], b * (LANES // FOLD), 1
        )
    part[:, own:, :] = packed.reshape(n_src, own // FOLD, LANES)

    pl.semaphore_wait(barrier, n_all - 1)

    def send_one(dt, dp, c):
        to = (src + dp) % n_src
        pltpu.make_async_remote_copy(
            src_ref=part.at[to], dst_ref=got.at[src], send_sem=send_a, recv_sem=recv_a,
            device_id={"tm": tm, "src": to}, device_id_type=pl.DeviceIdType.MESH,
        ).start()
        return c

    each(near, send_one, 0)
    got[src] = part[src]
    others = got.at[pl.ds(0, n_src - 1)]
    pltpu.make_async_copy(others, others, recv_a).wait()
    both = got[0]
    for p in range(1, n_src):
        both = both + got[p]
    whole, ends = both[0:own], both[own:]
    for a in range(own // FOLD):
        for b in range(FOLD):
            row = ends[a:a + 1]
            spread[pl.ds(a * FOLD + b, 1), :] = (
                pltpu.roll(row, LANES - b * (LANES // FOLD), 1) if b else row
            )
    summed[0:LANES, :] = jnp.transpose(whole)
    summed[LANES:2 * LANES, :] = jnp.transpose(spread[...])

    damp_copy.wait()
    damping = damp_ref[...]
    x, forward = solve(
        lambda i, j: summed[pl.ds(pair_row(i, j), 1), :],
        lambda i: summed[pl.ds(PAIRS + i, 1), :],
        damping,
    )
    terms = jnp.zeros_like(damping)
    squared = jnp.zeros_like(damping)
    for i in range(WIDTH):
        terms = terms + forward[i] * forward[i]
        squared = squared + x[i] * x[i]
    terms = terms + damping * squared
    chi = chi - jnp.concatenate([terms, jnp.zeros((1, LANES - own), jnp.float32)], axis=1)
    lane = lax.broadcasted_iota(jnp.int32, (1, LANES), 1)
    front = lane < LANES // 2
    chi = chi + pltpu.roll(chi, LANES // 2, 1)
    total = total + pltpu.roll(total, LANES // 2, 1)
    mine[...] = jnp.where(front, chi, total)
    heard[me] = mine[...]

    def tell_one(dt, dp, c):
        pltpu.make_async_remote_copy(
            src_ref=mine, dst_ref=heard.at[me], send_sem=send_b, recv_sem=recv_b,
            device_id=at(dt, dp), device_id_type=pl.DeviceIdType.MESH,
        ).start()
        return c

    each(everyone, tell_one, 0)

    out_ref[:, 0:WIDTH] = jnp.transpose(jnp.concatenate(x, axis=0))
    sent = part.at[pl.ds(0, n_src - 1)]
    pltpu.make_async_copy(sent, sent, send_a).wait()
    told = heard.at[pl.ds(0, n_all - 1)]
    pltpu.make_async_copy(told, told, recv_b).wait()
    both = jnp.sum(heard[...].reshape(n_all, LANES), axis=0, keepdims=True)
    chi_all = jnp.sum(jnp.where(front, both, 0.0), axis=1, keepdims=True)
    total_all = jnp.sum(jnp.where(front, 0.0, both), axis=1, keepdims=True)
    out_ref[0:1, WIDTH:WIDTH + 1] = chi_all / total_all
    pltpu.make_async_copy(told, told, send_b).wait()


def hand_on(both_ref, x_out, misfit_out):
    x_out[...] = both_ref[:, 0:WIDTH]
    misfit_out[...] = both_ref[0:1, WIDTH:WIDTH + 1]


def solution(mesh):
    n_tm, n_src = mesh.shape["tm"], mesh.shape["src"]
    n_all = n_tm * n_src

    def on_device(design, unit_index, residual, weight, obs_count, damping):
        own = damping.shape[0]
        units = own * n_src
        slots = design.shape[1]
        chunk = 8192 if slots % 8192 == 0 else LANES
        turns = slots // chunk
        anywhere = pl.BlockSpec(memory_space=pl.ANY)
        vmem = pl.BlockSpec(memory_space=pltpu.VMEM)
        result = pl.pallas_call(
            functools.partial(kernel, n_tm, n_src, chunk),
            out_shape=pltpu.VMEM((own, LANES), jnp.float32),
            in_specs=[anywhere] * 6,
            out_specs=vmem,
            scratch_shapes=[
                pltpu.SMEM((1,), jnp.int32),
                pltpu.VMEM((WIDTH, slots), jnp.float32),
                pltpu.VMEM((1, slots), jnp.int32),
                pltpu.VMEM((1, slots), jnp.float32),
                pltpu.VMEM((1, slots), jnp.float32),
                pltpu.VMEM((1, own), jnp.float32),
                pltpu.VMEM((2 * ROWS, units), jnp.float32),
                pltpu.VMEM((units, LANES), jnp.float32),
                pltpu.VMEM((n_src, own + own // FOLD, LANES), jnp.float32),
                pltpu.VMEM((n_src, own + own // FOLD, LANES), jnp.float32),
                pltpu.VMEM((2 * LANES, own), jnp.float32),
                pltpu.VMEM((own, LANES), jnp.float32),
                pltpu.VMEM((1, LANES), jnp.float32),
                pltpu.VMEM((n_all, 1, LANES), jnp.float32),
                pltpu.SemaphoreType.DMA((turns, 4)),
                pltpu.SemaphoreType.DMA((2,)),
                pltpu.SemaphoreType.DMA,
                pltpu.SemaphoreType.DMA,
                pltpu.SemaphoreType.DMA,
                pltpu.SemaphoreType.DMA,
            ],
            compiler_params=pltpu.CompilerParams(collective_id=0, has_side_effects=True),
            name="calibrate",
        )(
            obs_count,
            design,
            unit_index.reshape(1, slots),
            residual.reshape(1, slots),
            weight.reshape(1, slots),
            damping.reshape(1, own),
        )
        result = pltpu.with_memory_space_constraint(result, pltpu.VMEM)
        x, misfit = pl.pallas_call(
            hand_on,
            out_shape=(
                jax.ShapeDtypeStruct((own, WIDTH), jnp.float32),
                jax.ShapeDtypeStruct((1, 1), jnp.float32),
            ),
            in_specs=[vmem],
            out_specs=(vmem, vmem),
            name="hand_on",
        )(result)
        return x.T, misfit.reshape(())

    both = ("tm", "src")
    return jax.shard_map(
        on_device,
        mesh=mesh,
        in_specs=(P(None, both), P(both), P(both), P(both), P(both), P(both)),
        out_specs=(P(None, both), P()),
        check_vma=False,
    )
```

```python
import functools

import jax
import jax.numpy as jnp
from jax import lax
from jax.experimental import pallas as pl
from jax.experimental.pallas import tpu as pltpu
from jax.sharding import PartitionSpec as P

WIDTH = 16
HALF = 8
PAIRS = WIDTH * (WIDTH + 1) // 2
ROWS = PAIRS + WIDTH
LANES = 128
TILE = 256
FOLD = 4


def pair_row(i, j):
    k = (j - i) % WIDTH
    if k > HALF or (k == HALF and i >= HALF):
        i, j = j, i
        k = (j - i) % WIDTH
    return k * WIDTH + i


def stacked_rows(d0, d1, w, wr):
    w0, w1 = d0 * w, d1 * w
    rows = [d0 * w0, d1 * w1]
    sub = lax.broadcasted_iota(jnp.int32, d0.shape, 0)
    for k in range(1, HALF):
        r0 = pltpu.roll(w0, HALF - k, 0)
        r1 = pltpu.roll(w1, HALF - k, 0)
        low = sub < HALF - k
        rows.append(d0 * jnp.where(low, r0, r1))
        rows.append(d1 * jnp.where(low, r1, r0))
    rows.append(d0 * w1)
    rows.append(d0 * wr)
    rows.append(d1 * wr)
    return rows


def rsqrt(value):
    guess = lax.rsqrt(value)
    return guess * (1.5 - 0.5 * value * guess * guess)


def solve(entry, rhs, damping):
    a = {}
    for i in range(WIDTH):
        for j in range(i + 1):
            a[i, j] = entry(i, j)
        a[i, i] = a[i, i] + damping
    b = [rhs(i) for i in range(WIDTH)]
    inverse, forward = [], []
    for j in range(WIDTH):
        inv = rsqrt(a[j, j])
        inverse.append(inv)
        for i in range(j + 1, WIDTH):
            a[i, j] = a[i, j] * inv
        y = b[j] * inv
        forward.append(y)
        for i in range(j + 1, WIDTH):
            b[i] = b[i] - a[i, j] * y
            for k in range(j + 1, i + 1):
                a[i, k] = a[i, k] - a[i, j] * a[k, j]
    run = list(forward)
    x = [None] * WIDTH
    for i in reversed(range(WIDTH)):
        x[i] = run[i] * inverse[i]
        for k in range(i):
            run[k] = run[k] - a[i, k] * x[i]
    return x, forward


def ranked(k, me, n):
    up = me >= n // 2
    mine = jnp.where(up, me, n - 1 - me)
    k = k + jnp.where(k >= mine, 1, 0)
    return jnp.where(up, k, n - 1 - k)


def far_first(n):
    q = max(n // 4, 1)
    order = []
    for i in range(q):
        order += [3 * q + i, q + i]
    order += list(range(2 * q, 3 * q)) + list(range(1, q))
    return [p for p in dict.fromkeys(order) if 0 < p < n]


def repeat(n, body, start):
    if n <= 32:
        for k in range(n):
            start = body(k, start)
        return start
    return lax.fori_loop(0, n, body, start)


def each(pairs, body, start):
    if len(pairs) <= 32:
        for dt, dp in pairs:
            start = body(dt, dp, start)
        return start
    n_src = max(dp for _, dp in pairs) + 1
    return lax.fori_loop(
        1, len(pairs) + 1, lambda i, c: body(i // n_src, i % n_src, c), start
    )


def add_slots(accs, refs, begin, chunk, first_unit, count, weights):
    design_ref, unit_ref, resid_ref, weight_ref = refs
    chi, total = weights
    for t in range(chunk // TILE):
        cols = pl.ds(begin + t * TILE, TILE)
        w = weight_ref[:, cols]
        live = begin + t * TILE + lax.broadcasted_iota(jnp.int32, w.shape, 1) < count
        w = jnp.where(live, w, 0.0)
        r = resid_ref[:, cols]
        wr = w * r
        rows = stacked_rows(design_ref[0:HALF, cols], design_ref[HALF:WIDTH, cols], w, wr)
        x = jnp.concatenate(rows, axis=0)
        high = x.astype(jnp.bfloat16)
        low = (x - high.astype(jnp.float32)).astype(jnp.bfloat16)
        lhs = jnp.concatenate([high, low], axis=0)
        unit = unit_ref[:, cols] - first_unit
        wrr = wr * r
        for k in range(TILE // LANES):
            chi = chi + wrr[:, k * LANES:(k + 1) * LANES]
            total = total + w[:, k * LANES:(k + 1) * LANES]
        q = t % 2
        for n, acc in enumerate(accs[q]):
            pltpu.matmul_push_rhs(
                one_hot(unit, n), staging_register=0, mxu_index=q, transpose=True
            )
            pltpu.matmul_acc_lhs(acc, lhs, load_staged_rhs=0)
    return chi, total


def one_hot(unit, n):
    here = lax.broadcasted_iota(jnp.int32, (TILE, unit.shape[1]), 0) + n * TILE == unit
    return jnp.where(here, 1.0, 0.0).astype(jnp.bfloat16)


def clear(accs):
    for q in range(2):
        for acc in accs[q]:
            pltpu.matmul_pop(acc)


def drained(accs, units):
    tiles = []
    for n in range(len(accs[0])):
        both = pltpu.matmul_pop(accs[0][n]) + pltpu.matmul_pop(accs[1][n])
        tiles.append(both[0:ROWS] + both[ROWS:2 * ROWS])
    return jnp.concatenate(tiles, axis=1)[:, 0:units]


def with_sums(body, units):
    tiles = -(-units // TILE)
    shape = (2 * ROWS, TILE)
    pl.run_scoped(
        lambda *accs: body((accs[0:tiles], accs[tiles:2 * tiles])),
        *[pltpu.ACC(q)(shape, jnp.float32) for q in range(2) for _ in range(tiles)],
    )


def beyond(
    start, chunk,
    count_ref, design_hbm, unit_hbm, resid_hbm, weight_hbm,
    sums_ref, weights_ref,
    design_ref, unit_ref, resid_ref, weight_ref, load,
):
    units = sums_ref.shape[1]
    slots = design_hbm.shape[1]
    first_unit = lax.axis_index("tm") * units
    count = count_ref[0]
    turns = (jnp.clip(count, start, slots) - start + chunk - 1) // chunk
    arrays = (
        (design_hbm, design_ref), (unit_hbm, unit_ref),
        (resid_hbm, resid_ref), (weight_hbm, weight_ref),
    )

    def fetch(step, which):
        far, here = arrays[which]
        size = pl.ds(pl.multiple_of(start + step * chunk, LANES), chunk)
        to = pl.ds(pl.multiple_of(step * chunk, LANES), chunk)
        return pltpu.make_async_copy(far.at[:, size], here.at[:, to], load.at[step, which])

    def fetch_all(step, c):
        for which in range(4):
            fetch(step, which).start()
        return c

    lax.fori_loop(0, turns, fetch_all, 0)

    def body(accs):
        zero = jnp.zeros((1, LANES), jnp.float32)

        def add(step, weights):
            for which in range(4):
                fetch(step, which).wait()
            return add_slots(
                accs, (design_ref, unit_ref, resid_ref, weight_ref),
                pl.multiple_of(step * chunk, LANES), chunk, first_unit, count - start, weights,
            )

        @pl.when(turns > 0)
        def _():
            clear(accs)
            chi, total = lax.fori_loop(0, turns, add, (zero, zero))
            sums_ref[...] = drained(accs, units)
            weights_ref[:, 0:LANES] = chi
            weights_ref[:, LANES:2 * LANES] = total

        @pl.when(turns == 0)
        def _():
            sums_ref[...] = jnp.zeros_like(sums_ref)
            weights_ref[...] = jnp.zeros_like(weights_ref)

    with_sums(body, units)


def kernel(
    n_tm, n_src, pieces,
    count_hbm, design_hbm, unit_hbm, resid_hbm, weight_hbm, damp_hbm, beyond_ref, weights_ref,
    out_ref,
    count_ref, design_ref, unit_ref, resid_ref, weight_ref, damp_ref,
    sums_ref, kept_ref, extra, part, got, summed, spread, mine, heard,
    load, small, send_a, recv_a, send_b, recv_b,
):
    tm, src = lax.axis_index("tm"), lax.axis_index("src")
    n_all = n_tm * n_src
    me = tm * n_src + src
    own = damp_ref.shape[1]
    units = own * n_src
    starts = [sum(pieces[:i]) for i in range(len(pieces))]
    order = far_first(n_src)
    near = [(0, p) for p in order]
    everyone = [(dt, p) for dt in range(n_tm - 1, 0, -1) for p in order + [0]] + near

    arrays = (
        (design_hbm, design_ref), (unit_hbm, unit_ref),
        (resid_hbm, resid_ref), (weight_hbm, weight_ref),
    )

    def fetch(step, which):
        far, here = arrays[which]
        cols = pl.ds(starts[step], pieces[step])
        return pltpu.make_async_copy(far.at[:, cols], here.at[:, cols], load.at[step, which])

    count_copy = pltpu.make_async_copy(count_hbm, count_ref, small.at[0])
    damp_copy = pltpu.make_async_copy(damp_hbm, damp_ref, small.at[1])
    count_copy.start()
    for step in range(len(pieces)):
        for which in range(4):
            fetch(step, which).start()
    damp_copy.start()

    def at(dt, dp):
        return {"tm": (tm + dt) % n_tm, "src": (src + dp) % n_src}

    barrier = pltpu.get_barrier_semaphore()

    def greet(dt, dp, c):
        pl.semaphore_signal(
            barrier, inc=1, device_id=at(dt, dp), device_id_type=pl.DeviceIdType.MESH
        )
        return c

    each(everyone, greet, 0)

    first_unit = tm * units
    count_copy.wait()
    count = count_ref[0]

    def body(accs):
        clear(accs)
        weights = weights_ref[:, 0:LANES], weights_ref[:, LANES:2 * LANES]
        for step in range(len(pieces)):
            for which in range(4):
                fetch(step, which).wait()
            weights = add_slots(
                accs, (design_ref, unit_ref, resid_ref, weight_ref),
                starts[step], pieces[step], first_unit, count, weights,
            )
        sums_ref[...] = beyond_ref[...] + drained(accs, units)
        kept_ref[:, 0:LANES], kept_ref[:, LANES:2 * LANES] = weights

    with_sums(body, units)
    sums = sums_ref[...]
    chi, total = kept_ref[:, 0:LANES], kept_ref[:, LANES:2 * LANES]
    left = jnp.concatenate(
        [sums[LANES:ROWS], jnp.zeros((2 * LANES - ROWS, units), jnp.float32)], axis=0
    )
    extra[...] = jnp.transpose(left)
    part[:, 0:own, :] = jnp.transpose(sums[0:LANES]).reshape(n_src, own, LANES)
    packed = extra[pl.ds(0, units // FOLD, stride=FOLD), :]
    for b in range(1, FOLD):
        packed = packed + pltpu.roll(
            extra[pl.ds(b, units // FOLD, stride=FOLD), :], b * (LANES // FOLD), 1
        )
    part[:, own:, :] = packed.reshape(n_src, own // FOLD, LANES)

    pl.semaphore_wait(barrier, n_all - 1)

    def send_one(k, c):
        to = ranked(k, src, n_src)
        pltpu.make_async_remote_copy(
            src_ref=part.at[to], dst_ref=got.at[src], send_sem=send_a, recv_sem=recv_a,
            device_id={"tm": tm, "src": to}, device_id_type=pl.DeviceIdType.MESH,
        ).start()
        return c

    repeat(n_src - 1, send_one, 0)
    got[src] = part[src]
    others = got.at[pl.ds(0, n_src - 1)]
    pltpu.make_async_copy(others, others, recv_a).wait()
    both = got[0]
    for p in range(1, n_src):
        both = both + got[p]
    whole, ends = both[0:own], both[own:]
    for a in range(own // FOLD):
        for b in range(FOLD):
            row = ends[a:a + 1]
            spread[pl.ds(a * FOLD + b, 1), :] = (
                pltpu.roll(row, LANES - b * (LANES // FOLD), 1) if b else row
            )
    summed[0:LANES, :] = jnp.transpose(whole)
    summed[LANES:2 * LANES, :] = jnp.transpose(spread[...])

    damp_copy.wait()
    damping = damp_ref[...]
    x, forward = solve(
        lambda i, j: summed[pl.ds(pair_row(i, j), 1), :],
        lambda i: summed[pl.ds(PAIRS + i, 1), :],
        damping,
    )
    terms = jnp.zeros_like(damping)
    squared = jnp.zeros_like(damping)
    for i in range(WIDTH):
        terms = terms + forward[i] * forward[i]
        squared = squared + x[i] * x[i]
    terms = terms + damping * squared
    chi = chi - jnp.concatenate([terms, jnp.zeros((1, LANES - own), jnp.float32)], axis=1)
    lane = lax.broadcasted_iota(jnp.int32, (1, LANES), 1)
    front = lane < LANES // 2
    chi = chi + pltpu.roll(chi, LANES // 2, 1)
    total = total + pltpu.roll(total, LANES // 2, 1)
    mine[...] = jnp.where(front, chi, total)
    heard[me] = mine[...]

    def tell_one(dt, dp, c):
        pltpu.make_async_remote_copy(
            src_ref=mine, dst_ref=heard.at[me], send_sem=send_b, recv_sem=recv_b,
            device_id=at(dt, dp), device_id_type=pl.DeviceIdType.MESH,
        ).start()
        return c

    each(everyone, tell_one, 0)

    out_ref[:, 0:WIDTH] = jnp.transpose(jnp.concatenate(x, axis=0))
    sent = part.at[pl.ds(0, n_src - 1)]
    pltpu.make_async_copy(sent, sent, send_a).wait()
    told = heard.at[pl.ds(0, n_all - 1)]
    pltpu.make_async_copy(told, told, recv_b).wait()
    both = jnp.sum(heard[...].reshape(n_all, LANES), axis=0, keepdims=True)
    chi_all = jnp.sum(jnp.where(front, both, 0.0), axis=1, keepdims=True)
    total_all = jnp.sum(jnp.where(front, 0.0, both), axis=1, keepdims=True)
    out_ref[0:1, WIDTH:WIDTH + 1] = chi_all / total_all
    pltpu.make_async_copy(told, told, send_b).wait()


def hand_on(both_ref, x_out, misfit_out):
    x_out[...] = both_ref[:, 0:WIDTH]
    misfit_out[...] = both_ref[0:1, WIDTH:WIDTH + 1]


def solution(mesh):
    n_tm, n_src = mesh.shape["tm"], mesh.shape["src"]
    n_all = n_tm * n_src

    def on_device(design, unit_index, residual, weight, obs_count, damping):
        own = damping.shape[0]
        units = own * n_src
        slots = design.shape[1]
        half = slots // 2
        piece = half // 4 if half % 2048 == 0 else half
        pieces = (piece, half - piece) if half > piece else (half,)
        chunk = next(c for c in (4096, 2048, 1024, 512, 256) if (slots - half) % c == 0)
        anywhere = pl.BlockSpec(memory_space=pl.ANY)
        vmem = pl.BlockSpec(memory_space=pltpu.VMEM)
        kept = lambda v: pltpu.with_memory_space_constraint(v, pltpu.VMEM)
        unit_index, residual, weight = (
            v.reshape(1, slots) for v in (unit_index, residual, weight)
        )
        rest = slots - half
        sums, weights = pl.pallas_call(
            functools.partial(beyond, half, chunk),
            out_shape=(
                pltpu.VMEM((ROWS, units), jnp.float32),
                pltpu.VMEM((1, 2 * LANES), jnp.float32),
            ),
            in_specs=[pl.BlockSpec(memory_space=pltpu.SMEM)] + [anywhere] * 4,
            out_specs=(vmem, vmem),
            scratch_shapes=[
                pltpu.VMEM((WIDTH, rest), jnp.float32),
                pltpu.VMEM((1, rest), jnp.int32),
                pltpu.VMEM((1, rest), jnp.float32),
                pltpu.VMEM((1, rest), jnp.float32),
                pltpu.SemaphoreType.DMA((rest // chunk, 4)),
            ],
            name="beyond",
        )(obs_count, design, unit_index, residual, weight)
        result = pl.pallas_call(
            functools.partial(kernel, n_tm, n_src, pieces),
            out_shape=pltpu.VMEM((own, LANES), jnp.float32),
            in_specs=[anywhere] * 6 + [vmem] * 2,
            out_specs=vmem,
            scratch_shapes=[
                pltpu.SMEM((1,), jnp.int32),
                pltpu.VMEM((WIDTH, half), jnp.float32),
                pltpu.VMEM((1, half), jnp.int32),
                pltpu.VMEM((1, half), jnp.float32),
                pltpu.VMEM((1, half), jnp.float32),
                pltpu.VMEM((1, own), jnp.float32),
                pltpu.VMEM((ROWS, units), jnp.float32),
                pltpu.VMEM((1, 2 * LANES), jnp.float32),
                pltpu.VMEM((units, LANES), jnp.float32),
                pltpu.VMEM((n_src, own + own // FOLD, LANES), jnp.float32),
                pltpu.VMEM((n_src, own + own // FOLD, LANES), jnp.float32),
                pltpu.VMEM((2 * LANES, own), jnp.float32),
                pltpu.VMEM((own, LANES), jnp.float32),
                pltpu.VMEM((1, LANES), jnp.float32),
                pltpu.VMEM((n_all, 1, LANES), jnp.float32),
                pltpu.SemaphoreType.DMA((len(pieces), 4)),
                pltpu.SemaphoreType.DMA((2,)),
                pltpu.SemaphoreType.DMA,
                pltpu.SemaphoreType.DMA,
                pltpu.SemaphoreType.DMA,
                pltpu.SemaphoreType.DMA,
            ],
            compiler_params=pltpu.CompilerParams(collective_id=0, has_side_effects=True),
            name="calibrate",
        )(
            obs_count,
            design,
            unit_index,
            residual,
            weight,
            damping.reshape(1, own),
            kept(sums),
            kept(weights),
        )
        result = kept(result)
        x, misfit = pl.pallas_call(
            hand_on,
            out_shape=(
                jax.ShapeDtypeStruct((own, WIDTH), jnp.float32),
                jax.ShapeDtypeStruct((1, 1), jnp.float32),
            ),
            in_specs=[vmem],
            out_specs=(vmem, vmem),
            name="hand_on",
        )(result)
        return x.T, misfit.reshape(())

    both = ("tm", "src")
    return jax.shard_map(
        on_device,
        mesh=mesh,
        in_specs=(P(None, both), P(both), P(both), P(both), P(both), P(both)),
        out_specs=(P(None, both), P()),
        check_vma=False,
    )
```

```python
import functools

import jax
import jax.numpy as jnp
from jax import lax
from jax.experimental import pallas as pl
from jax.experimental.pallas import tpu as pltpu
from jax.sharding import PartitionSpec as P

WIDTH = 16
HALF = 8
PAIRS = WIDTH * (WIDTH + 1) // 2
ROWS = PAIRS + WIDTH
EVEN = ROWS // WIDTH * WIDTH
LANES = 128
TILE = 256
FOLD = 4


def pair_row(i, j):
    k = (j - i) % WIDTH
    if k > HALF or (k == HALF and i >= HALF):
        i, j = j, i
        k = (j - i) % WIDTH
    return k * WIDTH + i


def stacked_rows(d0, d1, w, wr):
    w0, w1 = d0 * w, d1 * w
    rows = [d0 * w0, d1 * w1]
    sub = lax.broadcasted_iota(jnp.int32, d0.shape, 0)
    for k in range(1, HALF):
        r0 = pltpu.roll(w0, HALF - k, 0)
        r1 = pltpu.roll(w1, HALF - k, 0)
        low = sub < HALF - k
        rows.append(d0 * jnp.where(low, r0, r1))
        rows.append(d1 * jnp.where(low, r1, r0))
    rows.append(d0 * w1)
    rows.append(d0 * wr)
    rows.append(d1 * wr)
    return rows


def rsqrt(value):
    guess = lax.rsqrt(value)
    return guess * (1.5 - 0.5 * value * guess * guess)


def solve(entry, rhs, damping):
    a = {}
    for i in range(WIDTH):
        for j in range(i + 1):
            a[i, j] = entry(i, j)
        a[i, i] = a[i, i] + damping
    b = [rhs(i) for i in range(WIDTH)]
    inverse, forward = [], []
    for j in range(WIDTH):
        inv = rsqrt(a[j, j])
        inverse.append(inv)
        for i in range(j + 1, WIDTH):
            a[i, j] = a[i, j] * inv
        y = b[j] * inv
        forward.append(y)
        for i in range(j + 1, WIDTH):
            b[i] = b[i] - a[i, j] * y
            for k in range(j + 1, i + 1):
                a[i, k] = a[i, k] - a[i, j] * a[k, j]
    run = list(forward)
    x = [None] * WIDTH
    for i in reversed(range(WIDTH)):
        x[i] = run[i] * inverse[i]
        for k in range(i):
            run[k] = run[k] - a[i, k] * x[i]
    return x, forward


def skipping(k, me):
    return k + jnp.where(k >= me, 1, 0)


def ranked(k, me, n, up):
    k = skipping(k, jnp.where(up, me, n - 1 - me))
    return jnp.where(up, k, n - 1 - k)


def repeat(n, body):
    if n <= 32:
        for k in range(n):
            body(k)
    elif n:
        lax.fori_loop(0, n, lambda k, c: (body(k), c)[1], 0)


def solved_by(n_src):
    q = n_src // 4
    return [(w, w - q if w < 2 * q else w + q) for w in range(q, n_src - q)]


def add_slots(accs, refs, begin, chunk, first_unit, units, count, weights):
    design_ref, unit_ref, resid_ref, weight_ref = refs
    chi, total = weights
    for t in range(chunk // TILE):
        cols = pl.ds(begin + t * TILE, TILE)
        w = weight_ref[:, cols]
        live = begin + t * TILE + lax.broadcasted_iota(jnp.int32, w.shape, 1) < count
        w = jnp.where(live, w, 0.0)
        r = resid_ref[:, cols]
        wr = w * r
        rows = stacked_rows(design_ref[0:HALF, cols], design_ref[HALF:WIDTH, cols], w, wr)
        x = jnp.concatenate(rows, axis=0)
        high = x.astype(jnp.bfloat16).astype(jnp.float32)
        low = x - high
        lhs = jnp.concatenate(
            [high[0:EVEN], low[0:EVEN], high[EVEN:ROWS], low[EVEN:ROWS]], axis=0
        ).astype(jnp.bfloat16)
        unit = unit_ref[:, cols] - first_unit
        wrr = wr * r
        for k in range(TILE // LANES):
            chi = chi + wrr[:, k * LANES:(k + 1) * LANES]
            total = total + w[:, k * LANES:(k + 1) * LANES]
        q = t % 2
        for n, acc in enumerate(accs[q]):
            pltpu.matmul_push_rhs(
                one_hot(unit, n, units), staging_register=0, mxu_index=q, transpose=True
            )
            pltpu.matmul_acc_lhs(acc, lhs, load_staged_rhs=0)
    return chi, total


def one_hot(unit, n, units):
    rows = min(units - n * TILE, TILE)
    here = lax.broadcasted_iota(jnp.int16, (rows, TILE), 0) == (unit - n * TILE).astype(jnp.int16)
    hot = jnp.where(here, jnp.bfloat16(1), jnp.bfloat16(0))
    if rows < TILE:
        hot = jnp.concatenate([hot, jnp.zeros((TILE - rows, TILE), jnp.bfloat16)], axis=0)
    return hot


def clear(accs):
    for q in range(2):
        for acc in accs[q]:
            pltpu.matmul_pop(acc)


def drained(accs, units):
    tiles = []
    for n in range(len(accs[0])):
        both = pltpu.matmul_pop(accs[0][n]) + pltpu.matmul_pop(accs[1][n])
        tiles.append(jnp.concatenate(
            [both[0:EVEN] + both[EVEN:2 * EVEN], both[2 * EVEN:EVEN + ROWS] + both[EVEN + ROWS:]],
            axis=0,
        ))
    return jnp.concatenate(tiles, axis=1)[:, 0:units]


def with_sums(body, units):
    tiles = -(-units // TILE)
    shape = (2 * ROWS, TILE)
    pl.run_scoped(
        lambda *accs: body((accs[0:tiles], accs[tiles:2 * tiles])),
        *[pltpu.ACC(q)(shape, jnp.float32) for q in range(2) for _ in range(tiles)],
    )


def beyond(
    start, chunk,
    count_ref, design_hbm, unit_hbm, resid_hbm, weight_hbm,
    sums_ref, weights_ref,
    design_ref, unit_ref, resid_ref, weight_ref, load,
):
    units = sums_ref.shape[1]
    slots = design_hbm.shape[1]
    first_unit = lax.axis_index("tm") * units
    count = count_ref[0]
    turns = (jnp.clip(count, start, slots) - start + chunk - 1) // chunk
    arrays = (
        (design_hbm, design_ref), (unit_hbm, unit_ref),
        (resid_hbm, resid_ref), (weight_hbm, weight_ref),
    )

    def fetch(step, which):
        far, here = arrays[which]
        size = pl.ds(pl.multiple_of(start + step * chunk, LANES), chunk)
        to = pl.ds(pl.multiple_of(step * chunk, LANES), chunk)
        return pltpu.make_async_copy(far.at[:, size], here.at[:, to], load.at[step, which])

    def fetch_all(step, c):
        for which in range(4):
            fetch(step, which).start()
        return c

    lax.fori_loop(0, turns, fetch_all, 0)

    def body(accs):
        zero = jnp.zeros((1, LANES), jnp.float32)

        def add(step, weights):
            for which in range(4):
                fetch(step, which).wait()
            return add_slots(
                accs, (design_ref, unit_ref, resid_ref, weight_ref),
                pl.multiple_of(step * chunk, LANES), chunk, first_unit, units, count - start, weights,
            )

        @pl.when(turns > 0)
        def _():
            clear(accs)
            chi, total = lax.fori_loop(0, turns, add, (zero, zero))
            sums_ref[...] = drained(accs, units)
            weights_ref[:, 0:LANES] = chi
            weights_ref[:, LANES:2 * LANES] = total

        @pl.when(turns == 0)
        def _():
            sums_ref[...] = jnp.zeros_like(sums_ref)
            weights_ref[...] = jnp.zeros_like(weights_ref)

    with_sums(body, units)


def kernel(
    n_tm, n_src, pieces,
    count_ref, design_hbm, unit_hbm, resid_hbm, weight_hbm, damp_hbm, beyond_ref, weights_ref,
    out_ref,
    design_ref, unit_ref, resid_ref, weight_ref, damp_ref,
    sums_ref, kept_ref, extra, part, got, summed, spread, mine, heard, x_away, x_here,
    load, small, send_a, recv_a, send_b, recv_b, send_c, recv_c,
):
    tm, src = lax.axis_index("tm"), lax.axis_index("src")
    own = damp_ref.shape[1]
    units = own * n_src
    pairs = solved_by(n_src)
    n_solve = len(pairs)
    first_solver = pairs[0][0]
    lanes = own * n_src // n_solve
    n_outer = n_src - n_solve
    solves = (src >= first_solver) & (src < first_solver + n_solve)
    rank = src - first_solver
    up = src >= n_src // 2
    starts = [sum(pieces[:i]) for i in range(len(pieces))]

    arrays = (
        (design_hbm, design_ref), (unit_hbm, unit_ref),
        (resid_hbm, resid_ref), (weight_hbm, weight_ref),
    )

    def fetch(step, which):
        far, here = arrays[which]
        cols = pl.ds(starts[step], pieces[step])
        return pltpu.make_async_copy(far.at[:, cols], here.at[:, cols], load.at[step, which])

    x_away[...] = jnp.zeros_like(x_away)
    damp_copy = pltpu.make_async_copy(damp_hbm, damp_ref, small)
    for step in range(len(pieces)):
        for which in range(4):
            fetch(step, which).start()
    damp_copy.start()

    barrier = pltpu.get_barrier_semaphore()

    def greet(t, p):
        pl.semaphore_signal(
            barrier, inc=1, device_id={"tm": t, "src": p}, device_id_type=pl.DeviceIdType.MESH
        )

    @pl.when(solves)
    def _():
        repeat(n_outer, lambda k: greet(tm, k + jnp.where(k >= first_solver, n_solve, 0)))
        repeat(n_solve - 1, lambda k: greet(tm, first_solver + skipping(k, rank)))

    @pl.when(jnp.logical_not(solves))
    def _():
        repeat(n_solve, lambda k: greet(tm, first_solver + k))

    for dt in range(1, n_tm):
        repeat(n_solve, lambda k: greet((tm + dt) % n_tm, first_solver + k))

    first_unit = tm * units
    count = count_ref[0]

    def body(accs):
        clear(accs)
        weights = weights_ref[:, 0:LANES], weights_ref[:, LANES:2 * LANES]
        for step in range(len(pieces)):
            for which in range(4):
                fetch(step, which).wait()
            weights = add_slots(
                accs, (design_ref, unit_ref, resid_ref, weight_ref),
                starts[step], pieces[step], first_unit, units, count, weights,
            )
        sums_ref[...] = beyond_ref[...] + drained(accs, units)
        kept_ref[:, 0:LANES], kept_ref[:, LANES:2 * LANES] = weights

    with_sums(body, units)
    sums = sums_ref[...]
    damp_copy.wait()
    damping = jnp.concatenate([damp_ref[...]] * n_src, axis=1)
    block = lax.broadcasted_iota(jnp.int32, damping.shape, 1) // own
    damping = jnp.where(block == src, damping, 0.0)
    fill = [jnp.zeros((1, units - LANES), jnp.float32)] if units > LANES else []
    chi = jnp.concatenate([kept_ref[:, 0:LANES]] + fill, axis=1)
    total = jnp.concatenate([kept_ref[:, LANES:2 * LANES]] + fill, axis=1)
    left = jnp.concatenate(
        [sums[LANES:ROWS], damping, chi, total,
         jnp.zeros((2 * LANES - ROWS - 3, units), jnp.float32)], axis=0
    )

    def by_solver(rows):
        return jnp.concatenate(
            [rows[b * own:(b + 1) * own] for pair in pairs for b in pair], axis=0
        )

    extra[...] = by_solver(jnp.transpose(left))
    part[:, 0:lanes, :] = by_solver(jnp.transpose(sums[0:LANES])).reshape(n_solve, lanes, LANES)
    packed = extra[pl.ds(0, units // FOLD, stride=FOLD), :]
    lane = lax.broadcasted_iota(jnp.int32, packed.shape, 1) // (LANES // FOLD)
    for b in range(1, FOLD):
        more = extra[pl.ds(b, units // FOLD, stride=FOLD), :]
        packed = jnp.where(lane == b, pltpu.roll(more, b * (LANES // FOLD), 1), packed)
    part[:, lanes:, :] = packed.reshape(n_solve, lanes // FOLD, LANES)

    def send_to(k):
        pltpu.make_async_remote_copy(
            src_ref=part.at[k], dst_ref=got.at[src], send_sem=send_a, recv_sem=recv_a,
            device_id={"tm": tm, "src": first_solver + k},
            device_id_type=pl.DeviceIdType.MESH,
        ).start()

    def wait_bytes(ref, n, sem):
        some = ref.at[pl.ds(0, n)]
        pltpu.make_async_copy(some, some, sem).wait()

    def hand_over(p):
        return pltpu.make_async_remote_copy(
            src_ref=x_away, dst_ref=x_here, send_sem=send_c, recv_sem=recv_c,
            device_id={"tm": tm, "src": p}, device_id_type=pl.DeviceIdType.MESH,
        )

    me = tm * n_solve + rank

    def tell(t, p):
        pltpu.make_async_remote_copy(
            src_ref=mine, dst_ref=heard.at[me], send_sem=send_b, recv_sem=recv_b,
            device_id={"tm": t, "src": p}, device_id_type=pl.DeviceIdType.MESH,
        ).start()

    def tell_both(k):
        p = skipping(k, src)
        for t in range(n_tm):
            tell(t, p)

    @pl.when(solves)
    def _():
        pl.semaphore_wait(barrier, n_tm * n_src - 1)
        repeat(n_solve - 1, lambda k: send_to(ranked(k, rank, n_solve, up)))
        got[src] = part[rank]
        wait_bytes(got, n_src - 1, recv_a)
        both = got[0]
        for p in range(1, n_src):
            both = both + got[p]
        whole, ends = both[0:lanes], both[lanes:]
        for a in range(lanes // FOLD):
            for b in range(FOLD):
                row = ends[a:a + 1]
                spread[pl.ds(a * FOLD + b, 1), :] = (
                    pltpu.roll(row, LANES - b * (LANES // FOLD), 1) if b else row
                )
        summed[0:LANES, :] = jnp.transpose(whole)
        summed[LANES:2 * LANES, :] = jnp.transpose(spread[...])
        damping, chi, total = (summed[pl.ds(ROWS + i, 1), :] for i in range(3))
        x, forward = solve(
            lambda i, j: summed[pl.ds(pair_row(i, j), 1), :],
            lambda i: summed[pl.ds(PAIRS + i, 1), :],
            damping,
        )
        terms = jnp.zeros_like(damping)
        squared = jnp.zeros_like(damping)
        for i in range(WIDTH):
            terms = terms + forward[i] * forward[i]
            squared = squared + x[i] * x[i]
        terms = terms + damping * squared
        none = jnp.zeros((1, LANES // 2 - lanes), jnp.float32)
        mine[...] = jnp.concatenate([chi - terms, none, total, none], axis=1)
        heard[me] = mine[...]
        repeat(n_src - 1, tell_both)
        for dt in range(1, n_tm):
            tell((tm + dt) % n_tm, src)
        answer = jnp.transpose(jnp.concatenate(x, axis=0))
        x_away[:, 0:WIDTH] = answer[own:]
        copy = hand_over(jnp.where(up, src + n_src // 4, src - n_src // 4))
        copy.start()
        out_ref[:, 0:WIDTH] = answer[0:own]
        wait_bytes(part, n_solve - 1, send_a)
        wait_bytes(heard, n_tm * n_solve - 1, recv_b)

    @pl.when(jnp.logical_not(solves))
    def _():
        pl.semaphore_wait(barrier, n_solve)
        repeat(n_solve, lambda k: send_to(jnp.where(up, k, n_solve - 1 - k)))
        hand_over(src).wait_recv()
        out_ref[...] = x_here[...]
        wait_bytes(part, n_solve, send_a)
        wait_bytes(heard, n_tm * n_solve, recv_b)

    both = jnp.sum(heard[...].reshape(n_tm * n_solve, LANES), axis=0, keepdims=True)
    front = lax.broadcasted_iota(jnp.int32, (1, LANES), 1) < LANES // 2
    chi_all = jnp.sum(jnp.where(front, both, 0.0), axis=1, keepdims=True)
    total_all = jnp.sum(jnp.where(front, 0.0, both), axis=1, keepdims=True)
    out_ref[0:1, WIDTH:WIDTH + 1] = chi_all / total_all

    @pl.when(solves)
    def _():
        hand_over(src).wait_send()
        rest = n_tm * n_src - 1
        while rest > 0:
            some = min(rest, n_tm * n_solve)
            wait_bytes(heard, some, send_b)
            rest -= some


def hand_on(both_ref, x_out, misfit_out):
    x_out[...] = both_ref[:, 0:WIDTH]
    misfit_out[...] = both_ref[0:1, WIDTH:WIDTH + 1]


def solution(mesh):
    n_tm, n_src = mesh.shape["tm"], mesh.shape["src"]

    def on_device(design, unit_index, residual, weight, obs_count, damping):
        own = damping.shape[0]
        units = own * n_src
        slots = design.shape[1]
        half = slots // 2
        piece = half // 4 if half % 2048 == 0 else half
        pieces = (piece, half - piece) if half > piece else (half,)
        chunk = next(c for c in (4096, 2048, 1024, 512, 256) if (slots - half) % c == 0)
        n_solve = len(solved_by(n_src))
        lanes = units // n_solve
        anywhere = pl.BlockSpec(memory_space=pl.ANY)
        vmem = pl.BlockSpec(memory_space=pltpu.VMEM)
        kept = lambda v: pltpu.with_memory_space_constraint(v, pltpu.VMEM)
        unit_index, residual, weight = (
            v.reshape(1, slots) for v in (unit_index, residual, weight)
        )
        rest = slots - half
        sums, weights = pl.pallas_call(
            functools.partial(beyond, half, chunk),
            out_shape=(
                pltpu.VMEM((ROWS, units), jnp.float32),
                pltpu.VMEM((1, 2 * LANES), jnp.float32),
            ),
            in_specs=[pl.BlockSpec(memory_space=pltpu.SMEM)] + [anywhere] * 4,
            out_specs=(vmem, vmem),
            scratch_shapes=[
                pltpu.VMEM((WIDTH, rest), jnp.float32),
                pltpu.VMEM((1, rest), jnp.int32),
                pltpu.VMEM((1, rest), jnp.float32),
                pltpu.VMEM((1, rest), jnp.float32),
                pltpu.SemaphoreType.DMA((rest // chunk, 4)),
            ],
            name="beyond",
        )(obs_count, design, unit_index, residual, weight)
        result = pl.pallas_call(
            functools.partial(kernel, n_tm, n_src, pieces),
            out_shape=pltpu.VMEM((own, LANES), jnp.float32),
            in_specs=[pl.BlockSpec(memory_space=pltpu.SMEM)] + [anywhere] * 5 + [vmem] * 2,
            out_specs=vmem,
            scratch_shapes=[
                pltpu.VMEM((WIDTH, half), jnp.float32),
                pltpu.VMEM((1, half), jnp.int32),
                pltpu.VMEM((1, half), jnp.float32),
                pltpu.VMEM((1, half), jnp.float32),
                pltpu.VMEM((1, own), jnp.float32),
                pltpu.VMEM((ROWS, units), jnp.float32),
                pltpu.VMEM((1, 2 * LANES), jnp.float32),
                pltpu.VMEM((units, LANES), jnp.float32),
                pltpu.VMEM((n_solve, lanes + lanes // FOLD, LANES), jnp.float32),
                pltpu.VMEM((n_src, lanes + lanes // FOLD, LANES), jnp.float32),
                pltpu.VMEM((2 * LANES, lanes), jnp.float32),
                pltpu.VMEM((lanes, LANES), jnp.float32),
                pltpu.VMEM((1, LANES), jnp.float32),
                pltpu.VMEM((n_tm * n_solve, 1, LANES), jnp.float32),
                pltpu.VMEM((own, LANES), jnp.float32),
                pltpu.VMEM((own, LANES), jnp.float32),
                pltpu.SemaphoreType.DMA((len(pieces), 4)),
            ] + [pltpu.SemaphoreType.DMA] * 7,
            compiler_params=pltpu.CompilerParams(collective_id=0, has_side_effects=True),
            name="calibrate",
        )(
            obs_count,
            design,
            unit_index,
            residual,
            weight,
            damping.reshape(1, own),
            kept(sums),
            kept(weights),
        )
        result = kept(result)
        x, misfit = pl.pallas_call(
            hand_on,
            out_shape=(
                jax.ShapeDtypeStruct((own, WIDTH), jnp.float32),
                jax.ShapeDtypeStruct((1, 1), jnp.float32),
            ),
            in_specs=[vmem],
            out_specs=(vmem, vmem),
            name="hand_on",
        )(result)
        return x.T, misfit.reshape(())

    both = ("tm", "src")
    return jax.shard_map(
        on_device,
        mesh=mesh,
        in_specs=(P(None, both), P(both), P(both), P(both), P(both), P(both)),
        out_specs=(P(None, both), P()),
        check_vma=False,
    )
```

```python
import functools

import jax
import jax.numpy as jnp
from jax import lax
from jax.experimental import pallas as pl
from jax.experimental.pallas import tpu as pltpu
from jax.sharding import PartitionSpec as P

WIDTH = 16
HALF = 8
PAIRS = WIDTH * (WIDTH + 1) // 2
ROWS = PAIRS + WIDTH
EVEN = ROWS // WIDTH * WIDTH
LANES = 128
TILE = 256
FOLD = 4


def pair_row(i, j):
    k = (j - i) % WIDTH
    if k > HALF or (k == HALF and i >= HALF):
        i, j = j, i
        k = (j - i) % WIDTH
    return k * WIDTH + i


def stacked_rows(d0, d1, w, wr):
    w0, w1 = d0 * w, d1 * w
    rows = [d0 * w0, d1 * w1]
    sub = lax.broadcasted_iota(jnp.int32, d0.shape, 0)
    for k in range(1, HALF):
        r0 = pltpu.roll(w0, HALF - k, 0)
        r1 = pltpu.roll(w1, HALF - k, 0)
        low = sub < HALF - k
        rows.append(d0 * jnp.where(low, r0, r1))
        rows.append(d1 * jnp.where(low, r1, r0))
    rows.append(d0 * w1)
    rows.append(d0 * wr)
    rows.append(d1 * wr)
    return rows


def rsqrt(value):
    guess = lax.rsqrt(value)
    return guess * (1.5 - 0.5 * value * guess * guess)


def solve(entry, rhs, damping):
    a = {}
    for i in range(WIDTH):
        for j in range(i + 1):
            a[i, j] = entry(i, j)
        a[i, i] = a[i, i] + damping
    b = [rhs(i) for i in range(WIDTH)]
    inverse, forward = [], []
    for j in range(WIDTH):
        inv = rsqrt(a[j, j])
        inverse.append(inv)
        for i in range(j + 1, WIDTH):
            a[i, j] = a[i, j] * inv
        y = b[j] * inv
        forward.append(y)
        for i in range(j + 1, WIDTH):
            b[i] = b[i] - a[i, j] * y
            for k in range(j + 1, i + 1):
                a[i, k] = a[i, k] - a[i, j] * a[k, j]
    run = list(forward)
    x = [None] * WIDTH
    for i in reversed(range(WIDTH)):
        x[i] = run[i] * inverse[i]
        for k in range(i):
            run[k] = run[k] - a[i, k] * x[i]
    return x, forward


def skipping(k, me):
    return k + jnp.where(k >= me, 1, 0)


def ranked(k, me, n, up):
    k = skipping(k, jnp.where(up, me, n - 1 - me))
    return jnp.where(up, k, n - 1 - k)


def repeat(n, body):
    if n <= 32:
        for k in range(n):
            body(k)
    elif n:
        lax.fori_loop(0, n, lambda k, c: (body(k), c)[1], 0)


def solved_by(n_src):
    q = n_src // 4
    blocks = []
    for w in range(q + 1, n_src - q, 2):
        away = -q if w < 2 * q else q
        blocks.append((w, w - 1, w + away, w - 1 + away))
    return blocks


def add_slots(accs, refs, begin, chunk, first_unit, units, count, weights):
    design_ref, unit_ref, resid_ref, weight_ref = refs
    chi, total = weights
    for t in range(chunk // TILE):
        cols = pl.ds(begin + t * TILE, TILE)
        w = weight_ref[:, cols]
        live = begin + t * TILE + lax.broadcasted_iota(jnp.int32, w.shape, 1) < count
        w = jnp.where(live, w, 0.0)
        r = resid_ref[:, cols]
        wr = w * r
        rows = stacked_rows(design_ref[0:HALF, cols], design_ref[HALF:WIDTH, cols], w, wr)
        x = jnp.concatenate(rows, axis=0)
        high = x.astype(jnp.bfloat16).astype(jnp.float32)
        low = x - high
        lhs = jnp.concatenate(
            [high[0:EVEN], low[0:EVEN], high[EVEN:ROWS], low[EVEN:ROWS]], axis=0
        ).astype(jnp.bfloat16)
        unit = unit_ref[:, cols] - first_unit
        wrr = wr * r
        for k in range(TILE // LANES):
            chi = chi + wrr[:, k * LANES:(k + 1) * LANES]
            total = total + w[:, k * LANES:(k + 1) * LANES]
        q = t % 2
        for n, acc in enumerate(accs[q]):
            pltpu.matmul_push_rhs(
                one_hot(unit, n, units), staging_register=0, mxu_index=q, transpose=True
            )
            pltpu.matmul_acc_lhs(acc, lhs, load_staged_rhs=0)
    return chi, total


def one_hot(unit, n, units):
    rows = min(units - n * TILE, TILE)
    here = lax.broadcasted_iota(jnp.int16, (rows, TILE), 0) == (unit - n * TILE).astype(jnp.int16)
    hot = jnp.where(here, jnp.bfloat16(1), jnp.bfloat16(0))
    if rows < TILE:
        hot = jnp.concatenate([hot, jnp.zeros((TILE - rows, TILE), jnp.bfloat16)], axis=0)
    return hot


def clear(accs):
    for q in range(2):
        for acc in accs[q]:
            pltpu.matmul_pop(acc)


def drained(accs, units):
    tiles = []
    for n in range(len(accs[0])):
        both = pltpu.matmul_pop(accs[0][n]) + pltpu.matmul_pop(accs[1][n])
        tiles.append(jnp.concatenate(
            [both[0:EVEN] + both[EVEN:2 * EVEN], both[2 * EVEN:EVEN + ROWS] + both[EVEN + ROWS:]],
            axis=0,
        ))
    return jnp.concatenate(tiles, axis=1)[:, 0:units]


def with_sums(body, units):
    tiles = -(-units // TILE)
    shape = (2 * ROWS, TILE)
    pl.run_scoped(
        lambda *accs: body((accs[0:tiles], accs[tiles:2 * tiles])),
        *[pltpu.ACC(q)(shape, jnp.float32) for q in range(2) for _ in range(tiles)],
    )


def beyond(
    start, chunk,
    count_ref, design_hbm, unit_hbm, resid_hbm, weight_hbm,
    sums_ref, weights_ref,
    design_ref, unit_ref, resid_ref, weight_ref, load,
):
    units = sums_ref.shape[1]
    slots = design_hbm.shape[1]
    first_unit = lax.axis_index("tm") * units
    count = count_ref[0]
    turns = (jnp.clip(count, start, slots) - start + chunk - 1) // chunk
    arrays = (
        (design_hbm, design_ref), (unit_hbm, unit_ref),
        (resid_hbm, resid_ref), (weight_hbm, weight_ref),
    )

    def fetch(step, which):
        far, here = arrays[which]
        size = pl.ds(pl.multiple_of(start + step * chunk, LANES), chunk)
        to = pl.ds(pl.multiple_of(step * chunk, LANES), chunk)
        return pltpu.make_async_copy(far.at[:, size], here.at[:, to], load.at[step, which])

    def fetch_all(step, c):
        for which in range(4):
            fetch(step, which).start()
        return c

    lax.fori_loop(0, turns, fetch_all, 0)

    def body(accs):
        zero = jnp.zeros((1, LANES), jnp.float32)

        def add(step, weights):
            for which in range(4):
                fetch(step, which).wait()
            return add_slots(
                accs, (design_ref, unit_ref, resid_ref, weight_ref),
                pl.multiple_of(step * chunk, LANES), chunk, first_unit, units, count - start, weights,
            )

        @pl.when(turns > 0)
        def _():
            clear(accs)
            chi, total = lax.fori_loop(0, turns, add, (zero, zero))
            sums_ref[...] = drained(accs, units)
            weights_ref[:, 0:LANES] = chi
            weights_ref[:, LANES:2 * LANES] = total

        @pl.when(turns == 0)
        def _():
            sums_ref[...] = jnp.zeros_like(sums_ref)
            weights_ref[...] = jnp.zeros_like(weights_ref)

    with_sums(body, units)


def kernel(
    n_tm, n_src, pieces,
    count_ref, design_hbm, unit_hbm, resid_hbm, weight_hbm, damp_hbm, beyond_ref, weights_ref,
    out_ref,
    design_ref, unit_ref, resid_ref, weight_ref, damp_ref,
    sums_ref, kept_ref, extra, part, got, summed, spread, mine, heard, x_away, x_here,
    load, small, send_a, recv_a, send_b, recv_b, send_c, recv_c,
):
    tm, src = lax.axis_index("tm"), lax.axis_index("src")
    own = damp_ref.shape[1]
    units = own * n_src
    shares = solved_by(n_src)
    n_solve = len(shares)
    first_solver = shares[0][0]
    lanes = own * n_src // n_solve
    solves = (src >= first_solver) & (src < first_solver + 2 * n_solve) & (src % 2 == 1)
    rank = (src - first_solver) // 2
    up = src >= n_src // 2
    starts = [sum(pieces[:i]) for i in range(len(pieces))]

    arrays = (
        (design_hbm, design_ref), (unit_hbm, unit_ref),
        (resid_hbm, resid_ref), (weight_hbm, weight_ref),
    )

    def fetch(step, which):
        far, here = arrays[which]
        cols = pl.ds(starts[step], pieces[step])
        return pltpu.make_async_copy(far.at[:, cols], here.at[:, cols], load.at[step, which])

    x_away[...] = jnp.zeros_like(x_away)
    damp_copy = pltpu.make_async_copy(damp_hbm, damp_ref, small)
    for step in range(len(pieces)):
        for which in range(4):
            fetch(step, which).start()
    damp_copy.start()

    barrier = pltpu.get_barrier_semaphore()

    def greet(t, p):
        pl.semaphore_signal(
            barrier, inc=1, device_id={"tm": t, "src": p}, device_id_type=pl.DeviceIdType.MESH
        )

    @pl.when(solves)
    def _():
        repeat(n_src - 1, lambda k: greet(tm, skipping(k, src)))

    @pl.when(jnp.logical_not(solves))
    def _():
        repeat(n_solve, lambda k: greet(tm, first_solver + 2 * k))

    for dt in range(1, n_tm):
        repeat(n_solve, lambda k: greet((tm + dt) % n_tm, first_solver + 2 * k))

    first_unit = tm * units
    count = count_ref[0]

    def body(accs):
        clear(accs)
        weights = weights_ref[:, 0:LANES], weights_ref[:, LANES:2 * LANES]
        for step in range(len(pieces)):
            for which in range(4):
                fetch(step, which).wait()
            weights = add_slots(
                accs, (design_ref, unit_ref, resid_ref, weight_ref),
                starts[step], pieces[step], first_unit, units, count, weights,
            )
        sums_ref[...] = beyond_ref[...] + drained(accs, units)
        kept_ref[:, 0:LANES], kept_ref[:, LANES:2 * LANES] = weights

    with_sums(body, units)
    sums = sums_ref[...]
    damp_copy.wait()
    damping = jnp.concatenate([damp_ref[...]] * n_src, axis=1)
    block = lax.broadcasted_iota(jnp.int32, damping.shape, 1) // own
    damping = jnp.where(block == src, damping, 0.0)
    fill = [jnp.zeros((1, units - LANES), jnp.float32)] if units > LANES else []
    chi = jnp.concatenate([kept_ref[:, 0:LANES]] + fill, axis=1)
    total = jnp.concatenate([kept_ref[:, LANES:2 * LANES]] + fill, axis=1)
    left = jnp.concatenate(
        [sums[LANES:ROWS], damping, chi, total,
         jnp.zeros((2 * LANES - ROWS - 3, units), jnp.float32)], axis=0
    )

    def by_solver(rows):
        return jnp.concatenate(
            [rows[b * own:(b + 1) * own] for share in shares for b in share], axis=0
        )

    extra[...] = by_solver(jnp.transpose(left))
    part[:, 0:lanes, :] = by_solver(jnp.transpose(sums[0:LANES])).reshape(n_solve, lanes, LANES)
    packed = extra[pl.ds(0, units // FOLD, stride=FOLD), :]
    lane = lax.broadcasted_iota(jnp.int32, packed.shape, 1) // (LANES // FOLD)
    for b in range(1, FOLD):
        more = extra[pl.ds(b, units // FOLD, stride=FOLD), :]
        packed = jnp.where(lane == b, pltpu.roll(more, b * (LANES // FOLD), 1), packed)
    part[:, lanes:, :] = packed.reshape(n_solve, lanes // FOLD, LANES)

    def send_to(k):
        pltpu.make_async_remote_copy(
            src_ref=part.at[k], dst_ref=got.at[src], send_sem=send_a, recv_sem=recv_a,
            device_id={"tm": tm, "src": first_solver + 2 * k},
            device_id_type=pl.DeviceIdType.MESH,
        ).start()

    def wait_bytes(ref, n, sem):
        some = ref.at[pl.ds(0, n)]
        pltpu.make_async_copy(some, some, sem).wait()

    away = jnp.where(up, n_src // 4, -(n_src // 4))

    def hand_over(i, p):
        return pltpu.make_async_remote_copy(
            src_ref=x_away.at[pl.ds(i * own, own)], dst_ref=x_here,
            send_sem=send_c, recv_sem=recv_c,
            device_id={"tm": tm, "src": p}, device_id_type=pl.DeviceIdType.MESH,
        )

    me = tm * n_solve + rank

    def tell(t, p):
        pltpu.make_async_remote_copy(
            src_ref=mine, dst_ref=heard.at[me], send_sem=send_b, recv_sem=recv_b,
            device_id={"tm": t, "src": p}, device_id_type=pl.DeviceIdType.MESH,
        ).start()

    def tell_both(k):
        p = skipping(k, src)
        for t in range(n_tm):
            tell(t, p)

    @pl.when(solves)
    def _():
        pl.semaphore_wait(barrier, n_tm * n_src - 1)
        repeat(n_solve - 1, lambda k: send_to(ranked(k, rank, n_solve, up)))
        got[src] = part[rank]
        wait_bytes(got, n_src - 1, recv_a)
        both = got[0]
        for p in range(1, n_src):
            both = both + got[p]
        whole, ends = both[0:lanes], both[lanes:]
        for a in range(lanes // FOLD):
            for b in range(FOLD):
                row = ends[a:a + 1]
                spread[pl.ds(a * FOLD + b, 1), :] = (
                    pltpu.roll(row, LANES - b * (LANES // FOLD), 1) if b else row
                )
        summed[0:LANES, :] = jnp.transpose(whole)
        summed[LANES:2 * LANES, :] = jnp.transpose(spread[...])
        damping, chi, total = (summed[pl.ds(ROWS + i, 1), :] for i in range(3))
        x, forward = solve(
            lambda i, j: summed[pl.ds(pair_row(i, j), 1), :],
            lambda i: summed[pl.ds(PAIRS + i, 1), :],
            damping,
        )
        terms = jnp.zeros_like(damping)
        squared = jnp.zeros_like(damping)
        for i in range(WIDTH):
            terms = terms + forward[i] * forward[i]
            squared = squared + x[i] * x[i]
        terms = terms + damping * squared
        none = jnp.zeros((1, LANES // 2 - lanes), jnp.float32)
        mine[...] = jnp.concatenate([chi - terms, none, total, none], axis=1)
        heard[me] = mine[...]
        repeat(n_src - 1, tell_both)
        for dt in range(1, n_tm):
            tell((tm + dt) % n_tm, src)
        answer = jnp.transpose(jnp.concatenate(x, axis=0))
        x_away[:, 0:WIDTH] = answer
        for i, p in ((2, src + away), (3, src - 1 + away), (1, src - 1)):
            hand_over(i, p).start()
        out_ref[:, 0:WIDTH] = answer[0:own]
        wait_bytes(part, n_solve - 1, send_a)
        wait_bytes(heard, n_tm * n_solve - 1, recv_b)

    @pl.when(jnp.logical_not(solves))
    def _():
        pl.semaphore_wait(barrier, n_solve)
        repeat(n_solve, lambda k: send_to(jnp.where(up, k, n_solve - 1 - k)))
        hand_over(0, src).wait_recv()
        out_ref[...] = x_here[...]
        wait_bytes(part, n_solve, send_a)
        wait_bytes(heard, n_tm * n_solve, recv_b)

    both = jnp.sum(heard[...].reshape(n_tm * n_solve, LANES), axis=0, keepdims=True)
    front = lax.broadcasted_iota(jnp.int32, (1, LANES), 1) < LANES // 2
    chi_all = jnp.sum(jnp.where(front, both, 0.0), axis=1, keepdims=True)
    total_all = jnp.sum(jnp.where(front, 0.0, both), axis=1, keepdims=True)
    out_ref[0:1, WIDTH:WIDTH + 1] = chi_all / total_all

    @pl.when(solves)
    def _():
        some = x_away.at[pl.ds(own, 3 * own)]
        pltpu.make_async_copy(some, some, send_c).wait()
        rest = n_tm * n_src - 1
        while rest > 0:
            some = min(rest, n_tm * n_solve)
            wait_bytes(heard, some, send_b)
            rest -= some


def hand_on(both_ref, x_out, misfit_out):
    x_out[...] = both_ref[:, 0:WIDTH]
    misfit_out[...] = both_ref[0:1, WIDTH:WIDTH + 1]


def solution(mesh):
    n_tm, n_src = mesh.shape["tm"], mesh.shape["src"]

    def on_device(design, unit_index, residual, weight, obs_count, damping):
        own = damping.shape[0]
        units = own * n_src
        slots = design.shape[1]
        half = slots // 2
        piece = half // 4 if half % 2048 == 0 else half
        pieces = (piece, half - piece) if half > piece else (half,)
        chunk = next(c for c in (4096, 2048, 1024, 512, 256) if (slots - half) % c == 0)
        n_solve = len(solved_by(n_src))
        lanes = units // n_solve
        anywhere = pl.BlockSpec(memory_space=pl.ANY)
        vmem = pl.BlockSpec(memory_space=pltpu.VMEM)
        kept = lambda v: pltpu.with_memory_space_constraint(v, pltpu.VMEM)
        unit_index, residual, weight = (
            v.reshape(1, slots) for v in (unit_index, residual, weight)
        )
        rest = slots - half
        sums, weights = pl.pallas_call(
            functools.partial(beyond, half, chunk),
            out_shape=(
                pltpu.VMEM((ROWS, units), jnp.float32),
                pltpu.VMEM((1, 2 * LANES), jnp.float32),
            ),
            in_specs=[pl.BlockSpec(memory_space=pltpu.SMEM)] + [anywhere] * 4,
            out_specs=(vmem, vmem),
            scratch_shapes=[
                pltpu.VMEM((WIDTH, rest), jnp.float32),
                pltpu.VMEM((1, rest), jnp.int32),
                pltpu.VMEM((1, rest), jnp.float32),
                pltpu.VMEM((1, rest), jnp.float32),
                pltpu.SemaphoreType.DMA((rest // chunk, 4)),
            ],
            name="beyond",
        )(obs_count, design, unit_index, residual, weight)
        result = pl.pallas_call(
            functools.partial(kernel, n_tm, n_src, pieces),
            out_shape=pltpu.VMEM((own, LANES), jnp.float32),
            in_specs=[pl.BlockSpec(memory_space=pltpu.SMEM)] + [anywhere] * 5 + [vmem] * 2,
            out_specs=vmem,
            scratch_shapes=[
                pltpu.VMEM((WIDTH, half), jnp.float32),
                pltpu.VMEM((1, half), jnp.int32),
                pltpu.VMEM((1, half), jnp.float32),
                pltpu.VMEM((1, half), jnp.float32),
                pltpu.VMEM((1, own), jnp.float32),
                pltpu.VMEM((ROWS, units), jnp.float32),
                pltpu.VMEM((1, 2 * LANES), jnp.float32),
                pltpu.VMEM((units, LANES), jnp.float32),
                pltpu.VMEM((n_solve, lanes + lanes // FOLD, LANES), jnp.float32),
                pltpu.VMEM((n_src, lanes + lanes // FOLD, LANES), jnp.float32),
                pltpu.VMEM((2 * LANES, lanes), jnp.float32),
                pltpu.VMEM((lanes, LANES), jnp.float32),
                pltpu.VMEM((1, LANES), jnp.float32),
                pltpu.VMEM((n_tm * n_solve, 1, LANES), jnp.float32),
                pltpu.VMEM((lanes, LANES), jnp.float32),
                pltpu.VMEM((own, LANES), jnp.float32),
                pltpu.SemaphoreType.DMA((len(pieces), 4)),
            ] + [pltpu.SemaphoreType.DMA] * 7,
            compiler_params=pltpu.CompilerParams(collective_id=0, has_side_effects=True),
            name="calibrate",
        )(
            obs_count,
            design,
            unit_index,
            residual,
            weight,
            damping.reshape(1, own),
            kept(sums),
            kept(weights),
        )
        result = kept(result)
        x, misfit = pl.pallas_call(
            hand_on,
            out_shape=(
                jax.ShapeDtypeStruct((own, WIDTH), jnp.float32),
                jax.ShapeDtypeStruct((1, 1), jnp.float32),
            ),
            in_specs=[vmem],
            out_specs=(vmem, vmem),
            name="hand_on",
        )(result)
        return x.T, misfit.reshape(())

    both = ("tm", "src")
    return jax.shard_map(
        on_device,
        mesh=mesh,
        in_specs=(P(None, both), P(both), P(both), P(both), P(both), P(both)),
        out_specs=(P(None, both), P()),
        check_vma=False,
    )
```

```python
import functools

import jax
import jax.numpy as jnp
from jax import lax
from jax.experimental import pallas as pl
from jax.experimental.pallas import tpu as pltpu
from jax.sharding import PartitionSpec as P

WIDTH = 16
HALF = 8
PAIRS = WIDTH * (WIDTH + 1) // 2
ROWS = PAIRS + WIDTH
EVEN = ROWS // WIDTH * WIDTH
LANES = 128
TILE = 256
FOLD = 4


def pair_row(i, j):
    k = (j - i) % WIDTH
    if k > HALF or (k == HALF and i >= HALF):
        i, j = j, i
        k = (j - i) % WIDTH
    return k * WIDTH + i


def stacked_rows(d0, d1, w, wr):
    w0, w1 = d0 * w, d1 * w
    rows = [d0 * w0, d1 * w1]
    sub = lax.broadcasted_iota(jnp.int32, d0.shape, 0)
    for k in range(1, HALF):
        r0 = pltpu.roll(w0, HALF - k, 0)
        r1 = pltpu.roll(w1, HALF - k, 0)
        low = sub < HALF - k
        rows.append(d0 * jnp.where(low, r0, r1))
        rows.append(d1 * jnp.where(low, r1, r0))
    rows.append(d0 * w1)
    rows.append(d0 * wr)
    rows.append(d1 * wr)
    return rows


def rsqrt(value):
    guess = lax.rsqrt(value)
    return guess * (1.5 - 0.5 * value * guess * guess)


def solve(entry, rhs, damping):
    a = {}
    for i in range(WIDTH):
        for j in range(i + 1):
            a[i, j] = entry(i, j)
        a[i, i] = a[i, i] + damping
    b = [rhs(i) for i in range(WIDTH)]
    inverse, forward = [], []
    for j in range(WIDTH):
        inv = rsqrt(a[j, j])
        inverse.append(inv)
        for i in range(j + 1, WIDTH):
            a[i, j] = a[i, j] * inv
        y = b[j] * inv
        forward.append(y)
        for i in range(j + 1, WIDTH):
            b[i] = b[i] - a[i, j] * y
            for k in range(j + 1, i + 1):
                a[i, k] = a[i, k] - a[i, j] * a[k, j]
    run = list(forward)
    x = [None] * WIDTH
    for i in reversed(range(WIDTH)):
        x[i] = run[i] * inverse[i]
        for k in range(i):
            run[k] = run[k] - a[i, k] * x[i]
    return x, forward


def skipping(k, me):
    return k + jnp.where(k >= me, 1, 0)


def ranked(k, me, n, up):
    k = skipping(k, jnp.where(up, me, n - 1 - me))
    return jnp.where(up, k, n - 1 - k)


def repeat(n, body):
    if n <= 32:
        for k in range(n):
            body(k)
    elif n:
        lax.fori_loop(0, n, lambda k, c: (body(k), c)[1], 0)


def solved_by(n_src):
    q = n_src // 4
    blocks = []
    for w in range(q + 1, n_src - q, 2):
        away = -q if w < 2 * q else q
        blocks.append((w, w - 1, w + away, w - 1 + away))
    return blocks


def add_slots(accs, refs, begin, chunk, first_unit, units, count, weights):
    design_ref, unit_ref, resid_ref, weight_ref = refs
    chi, total = weights
    for t in range(chunk // TILE):
        cols = pl.ds(begin + t * TILE, TILE)
        w = weight_ref[:, cols]
        live = begin + t * TILE + lax.broadcasted_iota(jnp.int32, w.shape, 1) < count
        w = jnp.where(live, w, 0.0)
        r = resid_ref[:, cols]
        wr = w * r
        rows = stacked_rows(design_ref[0:HALF, cols], design_ref[HALF:WIDTH, cols], w, wr)
        lhs = []
        for k in range(0, len(rows) - 1, 2):
            x = jnp.concatenate(rows[k:k + 2], axis=0)
            high = x.astype(jnp.bfloat16)
            lhs += [high, (x - high.astype(jnp.float32)).astype(jnp.bfloat16)]
        high = rows[-1].astype(jnp.bfloat16).astype(jnp.float32)
        lhs.append(jnp.concatenate([high, rows[-1] - high], axis=0).astype(jnp.bfloat16))
        lhs = jnp.concatenate(lhs, axis=0)
        unit = unit_ref[:, cols] - first_unit
        wrr = wr * r
        for k in range(TILE // LANES):
            chi = chi + wrr[:, k * LANES:(k + 1) * LANES]
            total = total + w[:, k * LANES:(k + 1) * LANES]
        q = t % 2
        for n, acc in enumerate(accs[q]):
            pltpu.matmul_push_rhs(
                one_hot(unit, n, units), staging_register=0, mxu_index=q, transpose=True
            )
            pltpu.matmul_acc_lhs(acc, lhs, load_staged_rhs=0)
    return chi, total


def one_hot(unit, n, units):
    rows = min(units - n * TILE, TILE)
    here = lax.broadcasted_iota(jnp.int16, (rows, TILE), 0) == (unit - n * TILE).astype(jnp.int16)
    hot = jnp.where(here, jnp.bfloat16(1), jnp.bfloat16(0))
    if rows < TILE:
        hot = jnp.concatenate([hot, jnp.zeros((TILE - rows, TILE), jnp.bfloat16)], axis=0)
    return hot


def clear(accs):
    for q in range(2):
        for acc in accs[q]:
            pltpu.matmul_pop(acc)


def drained(accs, units):
    tiles = []
    for n in range(len(accs[0])):
        both = pltpu.matmul_pop(accs[0][n]) + pltpu.matmul_pop(accs[1][n])
        sums = [
            both[2 * k:2 * k + WIDTH] + both[2 * k + WIDTH:2 * k + 2 * WIDTH]
            for k in range(0, EVEN, WIDTH)
        ]
        sums.append(both[2 * EVEN:EVEN + ROWS] + both[EVEN + ROWS:])
        tiles.append(jnp.concatenate(sums, axis=0))
    return jnp.concatenate(tiles, axis=1)[:, 0:units]


def with_sums(body, units):
    tiles = -(-units // TILE)
    shape = (2 * ROWS, TILE)
    pl.run_scoped(
        lambda *accs: body((accs[0:tiles], accs[tiles:2 * tiles])),
        *[pltpu.ACC(q)(shape, jnp.float32) for q in range(2) for _ in range(tiles)],
    )


def beyond(
    start, chunk,
    count_ref, design_hbm, unit_hbm, resid_hbm, weight_hbm,
    sums_ref, weights_ref,
    design_ref, unit_ref, resid_ref, weight_ref, load,
):
    units = sums_ref.shape[1]
    slots = design_hbm.shape[1]
    first_unit = lax.axis_index("tm") * units
    count = count_ref[0]
    turns = (jnp.clip(count, start, slots) - start + chunk - 1) // chunk
    arrays = (
        (design_hbm, design_ref), (unit_hbm, unit_ref),
        (resid_hbm, resid_ref), (weight_hbm, weight_ref),
    )

    def fetch(step, which):
        far, here = arrays[which]
        size = pl.ds(pl.multiple_of(start + step * chunk, LANES), chunk)
        to = pl.ds(pl.multiple_of(step * chunk, LANES), chunk)
        return pltpu.make_async_copy(far.at[:, size], here.at[:, to], load.at[step, which])

    def fetch_all(step, c):
        for which in range(4):
            fetch(step, which).start()
        return c

    lax.fori_loop(0, turns, fetch_all, 0)

    def body(accs):
        zero = jnp.zeros((1, LANES), jnp.float32)

        def add(step, weights):
            for which in range(4):
                fetch(step, which).wait()
            return add_slots(
                accs, (design_ref, unit_ref, resid_ref, weight_ref),
                pl.multiple_of(step * chunk, LANES), chunk, first_unit, units, count - start, weights,
            )

        @pl.when(turns > 0)
        def _():
            clear(accs)
            chi, total = lax.fori_loop(0, turns, add, (zero, zero))
            sums_ref[...] = drained(accs, units)
            weights_ref[:, 0:LANES] = chi
            weights_ref[:, LANES:2 * LANES] = total

        @pl.when(turns == 0)
        def _():
            sums_ref[...] = jnp.zeros_like(sums_ref)
            weights_ref[...] = jnp.zeros_like(weights_ref)

    with_sums(body, units)


def kernel(
    n_tm, n_src, pieces,
    count_ref, design_hbm, unit_hbm, resid_hbm, weight_hbm, damp_hbm, beyond_ref, weights_ref,
    out_ref,
    design_ref, unit_ref, resid_ref, weight_ref, damp_ref,
    sums_ref, kept_ref, extra, part, got, summed, spread, mine, heard, x_away, x_here,
    load, small, send_a, recv_a, send_b, recv_b, send_c, recv_c,
):
    tm, src = lax.axis_index("tm"), lax.axis_index("src")
    own = damp_ref.shape[1]
    units = own * n_src
    shares = solved_by(n_src)
    n_solve = len(shares)
    first_solver = shares[0][0]
    lanes = own * n_src // n_solve
    solves = (src >= first_solver) & (src < first_solver + 2 * n_solve) & (src % 2 == 1)
    rank = (src - first_solver) // 2
    up = src >= n_src // 2
    starts = [sum(pieces[:i]) for i in range(len(pieces))]

    arrays = (
        (design_hbm, design_ref), (unit_hbm, unit_ref),
        (resid_hbm, resid_ref), (weight_hbm, weight_ref),
    )

    def fetch(step, which):
        far, here = arrays[which]
        cols = pl.ds(starts[step], pieces[step])
        return pltpu.make_async_copy(far.at[:, cols], here.at[:, cols], load.at[step, which])

    x_away[...] = jnp.zeros_like(x_away)
    damp_copy = pltpu.make_async_copy(damp_hbm, damp_ref, small)
    for step in range(len(pieces)):
        for which in range(4):
            fetch(step, which).start()
    damp_copy.start()

    barrier = pltpu.get_barrier_semaphore()

    def greet(t, p):
        pl.semaphore_signal(
            barrier, inc=1, device_id={"tm": t, "src": p}, device_id_type=pl.DeviceIdType.MESH
        )

    @pl.when(solves)
    def _():
        repeat(n_src - 1, lambda k: greet(tm, skipping(k, src)))

    @pl.when(jnp.logical_not(solves))
    def _():
        repeat(n_solve, lambda k: greet(tm, first_solver + 2 * k))

    for dt in range(1, n_tm):
        repeat(n_solve, lambda k: greet((tm + dt) % n_tm, first_solver + 2 * k))

    first_unit = tm * units
    count = count_ref[0]

    def body(accs):
        clear(accs)
        weights = weights_ref[:, 0:LANES], weights_ref[:, LANES:2 * LANES]
        for step in range(len(pieces)):
            for which in range(4):
                fetch(step, which).wait()
            weights = add_slots(
                accs, (design_ref, unit_ref, resid_ref, weight_ref),
                starts[step], pieces[step], first_unit, units, count, weights,
            )
        sums_ref[...] = beyond_ref[...] + drained(accs, units)
        kept_ref[:, 0:LANES], kept_ref[:, LANES:2 * LANES] = weights

    with_sums(body, units)
    sums = sums_ref[...]
    damp_copy.wait()
    damping = jnp.concatenate([damp_ref[...]] * n_src, axis=1)
    block = lax.broadcasted_iota(jnp.int32, damping.shape, 1) // own
    damping = jnp.where(block == src, damping, 0.0)
    fill = [jnp.zeros((1, units - LANES), jnp.float32)] if units > LANES else []
    chi = jnp.concatenate([kept_ref[:, 0:LANES]] + fill, axis=1)
    total = jnp.concatenate([kept_ref[:, LANES:2 * LANES]] + fill, axis=1)
    left = jnp.concatenate(
        [sums[LANES:ROWS], damping, chi, total,
         jnp.zeros((2 * LANES - ROWS - 3, units), jnp.float32)], axis=0
    )

    def by_solver(rows):
        return jnp.concatenate(
            [rows[b * own:(b + 1) * own] for share in shares for b in share], axis=0
        )

    extra[...] = by_solver(jnp.transpose(left))
    part[:, 0:lanes, :] = by_solver(jnp.transpose(sums[0:LANES])).reshape(n_solve, lanes, LANES)
    packed = extra[pl.ds(0, units // FOLD, stride=FOLD), :]
    lane = lax.broadcasted_iota(jnp.int32, packed.shape, 1) // (LANES // FOLD)
    for b in range(1, FOLD):
        more = extra[pl.ds(b, units // FOLD, stride=FOLD), :]
        packed = jnp.where(lane == b, pltpu.roll(more, b * (LANES // FOLD), 1), packed)
    part[:, lanes:, :] = packed.reshape(n_solve, lanes // FOLD, LANES)

    def send_to(k):
        pltpu.make_async_remote_copy(
            src_ref=part.at[k], dst_ref=got.at[src], send_sem=send_a, recv_sem=recv_a,
            device_id={"tm": tm, "src": first_solver + 2 * k},
            device_id_type=pl.DeviceIdType.MESH,
        ).start()

    def wait_bytes(ref, n, sem):
        some = ref.at[pl.ds(0, n)]
        pltpu.make_async_copy(some, some, sem).wait()

    away = jnp.where(up, n_src // 4, -(n_src // 4))

    def hand_over(i, p):
        return pltpu.make_async_remote_copy(
            src_ref=x_away.at[pl.ds(i * own, own)], dst_ref=x_here,
            send_sem=send_c, recv_sem=recv_c,
            device_id={"tm": tm, "src": p}, device_id_type=pl.DeviceIdType.MESH,
        )

    me = tm * n_solve + rank

    def tell(t, p):
        pltpu.make_async_remote_copy(
            src_ref=mine, dst_ref=heard.at[me], send_sem=send_b, recv_sem=recv_b,
            device_id={"tm": t, "src": p}, device_id_type=pl.DeviceIdType.MESH,
        ).start()

    def tell_both(k):
        p = skipping(k, src)
        for t in range(n_tm):
            tell(t, p)

    @pl.when(solves)
    def _():
        pl.semaphore_wait(barrier, n_tm * n_src - 1)
        repeat(n_solve - 1, lambda k: send_to(ranked(k, rank, n_solve, up)))
        got[src] = part[rank]
        wait_bytes(got, n_src - 1, recv_a)
        both = got[0]
        for p in range(1, n_src):
            both = both + got[p]
        whole, ends = both[0:lanes], both[lanes:]
        for a in range(lanes // FOLD):
            for b in range(FOLD):
                row = ends[a:a + 1]
                spread[pl.ds(a * FOLD + b, 1), :] = (
                    pltpu.roll(row, LANES - b * (LANES // FOLD), 1) if b else row
                )
        summed[0:LANES, :] = jnp.transpose(whole)
        summed[LANES:2 * LANES, :] = jnp.transpose(spread[...])
        damping, chi, total = (summed[pl.ds(ROWS + i, 1), :] for i in range(3))
        x, forward = solve(
            lambda i, j: summed[pl.ds(pair_row(i, j), 1), :],
            lambda i: summed[pl.ds(PAIRS + i, 1), :],
            damping,
        )
        terms = jnp.zeros_like(damping)
        squared = jnp.zeros_like(damping)
        for i in range(WIDTH):
            terms = terms + forward[i] * forward[i]
            squared = squared + x[i] * x[i]
        terms = terms + damping * squared
        none = jnp.zeros((1, LANES // 2 - lanes), jnp.float32)
        mine[...] = jnp.concatenate([chi - terms, none, total, none], axis=1)
        heard[me] = mine[...]
        repeat(n_src - 1, tell_both)
        for dt in range(1, n_tm):
            tell((tm + dt) % n_tm, src)
        answer = jnp.transpose(jnp.concatenate(x, axis=0))
        x_away[:, 0:WIDTH] = answer
        for i, p in ((2, src + away), (3, src - 1 + away), (1, src - 1)):
            hand_over(i, p).start()
        out_ref[:, 0:WIDTH] = answer[0:own]
        wait_bytes(part, n_solve - 1, send_a)
        wait_bytes(heard, n_tm * n_solve - 1, recv_b)

    @pl.when(jnp.logical_not(solves))
    def _():
        pl.semaphore_wait(barrier, n_solve)
        repeat(n_solve, lambda k: send_to(jnp.where(up, k, n_solve - 1 - k)))
        hand_over(0, src).wait_recv()
        out_ref[...] = x_here[...]
        wait_bytes(part, n_solve, send_a)
        wait_bytes(heard, n_tm * n_solve, recv_b)

    both = jnp.sum(heard[...].reshape(n_tm * n_solve, LANES), axis=0, keepdims=True)
    front = lax.broadcasted_iota(jnp.int32, (1, LANES), 1) < LANES // 2
    chi_all = jnp.sum(jnp.where(front, both, 0.0), axis=1, keepdims=True)
    total_all = jnp.sum(jnp.where(front, 0.0, both), axis=1, keepdims=True)
    out_ref[0:1, WIDTH:WIDTH + 1] = chi_all / total_all

    @pl.when(solves)
    def _():
        some = x_away.at[pl.ds(own, 3 * own)]
        pltpu.make_async_copy(some, some, send_c).wait()
        rest = n_tm * n_src - 1
        while rest > 0:
            some = min(rest, n_tm * n_solve)
            wait_bytes(heard, some, send_b)
            rest -= some


def hand_on(both_ref, x_out, misfit_out):
    x_out[...] = both_ref[:, 0:WIDTH]
    misfit_out[...] = both_ref[0:1, WIDTH:WIDTH + 1]


def solution(mesh):
    n_tm, n_src = mesh.shape["tm"], mesh.shape["src"]

    def on_device(design, unit_index, residual, weight, obs_count, damping):
        own = damping.shape[0]
        units = own * n_src
        slots = design.shape[1]
        half = slots // 2
        piece = half // 4 if half % 2048 == 0 else half
        pieces = (piece, half - piece) if half > piece else (half,)
        chunk = next(c for c in (4096, 2048, 1024, 512, 256) if (slots - half) % c == 0)
        n_solve = len(solved_by(n_src))
        lanes = units // n_solve
        anywhere = pl.BlockSpec(memory_space=pl.ANY)
        vmem = pl.BlockSpec(memory_space=pltpu.VMEM)
        kept = lambda v: pltpu.with_memory_space_constraint(v, pltpu.VMEM)
        unit_index, residual, weight = (
            v.reshape(1, slots) for v in (unit_index, residual, weight)
        )
        rest = slots - half
        sums, weights = pl.pallas_call(
            functools.partial(beyond, half, chunk),
            out_shape=(
                pltpu.VMEM((ROWS, units), jnp.float32),
                pltpu.VMEM((1, 2 * LANES), jnp.float32),
            ),
            in_specs=[pl.BlockSpec(memory_space=pltpu.SMEM)] + [anywhere] * 4,
            out_specs=(vmem, vmem),
            scratch_shapes=[
                pltpu.VMEM((WIDTH, rest), jnp.float32),
                pltpu.VMEM((1, rest), jnp.int32),
                pltpu.VMEM((1, rest), jnp.float32),
                pltpu.VMEM((1, rest), jnp.float32),
                pltpu.SemaphoreType.DMA((rest // chunk, 4)),
            ],
            name="beyond",
        )(obs_count, design, unit_index, residual, weight)
        result = pl.pallas_call(
            functools.partial(kernel, n_tm, n_src, pieces),
            out_shape=pltpu.VMEM((own, LANES), jnp.float32),
            in_specs=[pl.BlockSpec(memory_space=pltpu.SMEM)] + [anywhere] * 5 + [vmem] * 2,
            out_specs=vmem,
            scratch_shapes=[
                pltpu.VMEM((WIDTH, half), jnp.float32),
                pltpu.VMEM((1, half), jnp.int32),
                pltpu.VMEM((1, half), jnp.float32),
                pltpu.VMEM((1, half), jnp.float32),
                pltpu.VMEM((1, own), jnp.float32),
                pltpu.VMEM((ROWS, units), jnp.float32),
                pltpu.VMEM((1, 2 * LANES), jnp.float32),
                pltpu.VMEM((units, LANES), jnp.float32),
                pltpu.VMEM((n_solve, lanes + lanes // FOLD, LANES), jnp.float32),
                pltpu.VMEM((n_src, lanes + lanes // FOLD, LANES), jnp.float32),
                pltpu.VMEM((2 * LANES, lanes), jnp.float32),
                pltpu.VMEM((lanes, LANES), jnp.float32),
                pltpu.VMEM((1, LANES), jnp.float32),
                pltpu.VMEM((n_tm * n_solve, 1, LANES), jnp.float32),
                pltpu.VMEM((lanes, LANES), jnp.float32),
                pltpu.VMEM((own, LANES), jnp.float32),
                pltpu.SemaphoreType.DMA((len(pieces), 4)),
            ] + [pltpu.SemaphoreType.DMA] * 7,
            compiler_params=pltpu.CompilerParams(collective_id=0, has_side_effects=True),
            name="calibrate",
        )(
            obs_count,
            design,
            unit_index,
            residual,
            weight,
            damping.reshape(1, own),
            kept(sums),
            kept(weights),
        )
        result = kept(result)
        x, misfit = pl.pallas_call(
            hand_on,
            out_shape=(
                jax.ShapeDtypeStruct((own, WIDTH), jnp.float32),
                jax.ShapeDtypeStruct((1, 1), jnp.float32),
            ),
            in_specs=[vmem],
            out_specs=(vmem, vmem),
            name="hand_on",
        )(result)
        return x.T, misfit.reshape(())

    both = ("tm", "src")
    return jax.shard_map(
        on_device,
        mesh=mesh,
        in_specs=(P(None, both), P(both), P(both), P(both), P(both), P(both)),
        out_specs=(P(None, both), P()),
        check_vma=False,
    )
```

```python
import functools

import jax
import jax.numpy as jnp
from jax import lax
from jax.experimental import pallas as pl
from jax.experimental.pallas import tpu as pltpu
from jax.sharding import PartitionSpec as P

WIDTH = 16
HALF = 8
PAIRS = WIDTH * (WIDTH + 1) // 2
ROWS = PAIRS + WIDTH
EVEN = ROWS // WIDTH * WIDTH
LANES = 128
TILE = 256
FOLD = 4


def pair_row(i, j):
    k = (j - i) % WIDTH
    if k > HALF or (k == HALF and i >= HALF):
        i, j = j, i
        k = (j - i) % WIDTH
    return k * WIDTH + i


def stacked_rows(d0, d1, w, wr):
    w0, w1 = d0 * w, d1 * w
    rows = [d0 * w0, d1 * w1]
    sub = lax.broadcasted_iota(jnp.int32, d0.shape, 0)
    for k in range(1, HALF):
        r0 = pltpu.roll(w0, HALF - k, 0)
        r1 = pltpu.roll(w1, HALF - k, 0)
        low = sub < HALF - k
        rows.append(d0 * jnp.where(low, r0, r1))
        rows.append(d1 * jnp.where(low, r1, r0))
    rows.append(d0 * w1)
    rows.append(d0 * wr)
    rows.append(d1 * wr)
    return rows


def rsqrt(value):
    guess = lax.rsqrt(value)
    return guess * (1.5 - 0.5 * value * guess * guess)


def solve(entry, rhs, damping):
    a = {}
    for i in range(WIDTH):
        for j in range(i + 1):
            a[i, j] = entry(i, j)
        a[i, i] = a[i, i] + damping
    b = [rhs(i) for i in range(WIDTH)]
    inverse, forward = [], []
    for j in range(WIDTH):
        inv = rsqrt(a[j, j])
        inverse.append(inv)
        for i in range(j + 1, WIDTH):
            a[i, j] = a[i, j] * inv
        y = b[j] * inv
        forward.append(y)
        for i in range(j + 1, WIDTH):
            b[i] = b[i] - a[i, j] * y
            for k in range(j + 1, i + 1):
                a[i, k] = a[i, k] - a[i, j] * a[k, j]
    run = list(forward)
    x = [None] * WIDTH
    for i in reversed(range(WIDTH)):
        x[i] = run[i] * inverse[i]
        for k in range(i):
            run[k] = run[k] - a[i, k] * x[i]
    return x, forward


def skipping(k, me):
    return k + jnp.where(k >= me, 1, 0)


def ranked(k, me, n, up):
    k = skipping(k, jnp.where(up, me, n - 1 - me))
    return jnp.where(up, k, n - 1 - k)


def repeat(n, body):
    if n <= 32:
        for k in range(n):
            body(k)
    elif n:
        lax.fori_loop(0, n, lambda k, c: (body(k), c)[1], 0)


def solved_by(n_src):
    q = n_src // 4
    blocks = []
    for w in range(q + 1, n_src - q, 2):
        away = -q if w < 2 * q else q
        blocks.append((w, w - 1, w + away, w - 1 + away))
    return blocks


def add_slots(accs, refs, begin, chunk, first_unit, units, count, weights):
    design_ref, unit_ref, resid_ref, weight_ref = refs
    chi, total = weights
    for t in range(chunk // TILE):
        cols = pl.ds(begin + t * TILE, TILE)
        w = weight_ref[:, cols]
        live = begin + t * TILE + lax.broadcasted_iota(jnp.int32, w.shape, 1) < count
        w = jnp.where(live, w, 0.0)
        r = resid_ref[:, cols]
        wr = w * r
        rows = stacked_rows(design_ref[0:HALF, cols], design_ref[HALF:WIDTH, cols], w, wr)
        lhs = []
        for k in range(0, len(rows) - 1, 2):
            x = jnp.concatenate(rows[k:k + 2], axis=0)
            high = x.astype(jnp.bfloat16)
            lhs += [high, (x - high.astype(jnp.float32)).astype(jnp.bfloat16)]
        high = rows[-1].astype(jnp.bfloat16).astype(jnp.float32)
        lhs.append(jnp.concatenate([high, rows[-1] - high], axis=0).astype(jnp.bfloat16))
        lhs = jnp.concatenate(lhs, axis=0)
        unit = unit_ref[:, cols] - first_unit
        wrr = wr * r
        for k in range(TILE // LANES):
            chi = chi + wrr[:, k * LANES:(k + 1) * LANES]
            total = total + w[:, k * LANES:(k + 1) * LANES]
        q = t % 2
        for n, acc in enumerate(accs[q]):
            pltpu.matmul_push_rhs(
                one_hot(unit, n, units), staging_register=0, mxu_index=q, transpose=True
            )
            pltpu.matmul_acc_lhs(acc, lhs, load_staged_rhs=0)
    return chi, total


def one_hot(unit, n, units):
    rows = min(units - n * TILE, TILE)
    here = lax.broadcasted_iota(jnp.int16, (rows, TILE), 0) == (unit - n * TILE).astype(jnp.int16)
    hot = jnp.where(here, jnp.bfloat16(1), jnp.bfloat16(0))
    if rows < TILE:
        hot = jnp.concatenate([hot, jnp.zeros((TILE - rows, TILE), jnp.bfloat16)], axis=0)
    return hot


def clear(accs):
    for q in range(2):
        for acc in accs[q]:
            pltpu.matmul_pop(acc)


def drained(accs, units):
    tiles = []
    for n in range(len(accs[0])):
        both = pltpu.matmul_pop(accs[0][n]) + pltpu.matmul_pop(accs[1][n])
        sums = [
            both[2 * k:2 * k + WIDTH] + both[2 * k + WIDTH:2 * k + 2 * WIDTH]
            for k in range(0, EVEN, WIDTH)
        ]
        sums.append(both[2 * EVEN:EVEN + ROWS] + both[EVEN + ROWS:])
        tiles.append(jnp.concatenate(sums, axis=0))
    return jnp.concatenate(tiles, axis=1)[:, 0:units]


def with_sums(body, units):
    tiles = -(-units // TILE)
    shape = (2 * ROWS, TILE)
    pl.run_scoped(
        lambda *accs: body((accs[0:tiles], accs[tiles:2 * tiles])),
        *[pltpu.ACC(q)(shape, jnp.float32) for q in range(2) for _ in range(tiles)],
    )


def arrived(bytes_ref, chunk, sem):
    some = bytes_ref.at[:, pl.ds(0, (WIDTH + 3) * chunk)]
    pltpu.make_async_copy(some, some, sem).wait()


def beyond(
    start, chunk,
    count_ref, design_hbm, unit_hbm, resid_hbm, weight_hbm,
    sums_ref, weights_ref,
    design_ref, unit_ref, resid_ref, weight_ref, bytes_ref, load,
):
    units = sums_ref.shape[1]
    slots = design_hbm.shape[1]
    first_unit = lax.axis_index("tm") * units
    count = count_ref[0]
    turns = (jnp.clip(count, start, slots) - start + chunk - 1) // chunk
    arrays = (
        (design_hbm, design_ref), (unit_hbm, unit_ref),
        (resid_hbm, resid_ref), (weight_hbm, weight_ref),
    )

    def fetch(step, which):
        far, here = arrays[which]
        size = pl.ds(pl.multiple_of(start + step * chunk, LANES), chunk)
        to = pl.ds(pl.multiple_of(step * chunk, LANES), chunk)
        return pltpu.make_async_copy(far.at[:, size], here.at[:, to], load.at[step])

    def fetch_all(step, c):
        for which in range(4):
            fetch(step, which).start()
        return c

    lax.fori_loop(0, turns, fetch_all, 0)

    def body(accs):
        zero = jnp.zeros((1, LANES), jnp.float32)

        def add(step, weights):
            arrived(bytes_ref, chunk, load.at[step])
            return add_slots(
                accs, (design_ref, unit_ref, resid_ref, weight_ref),
                pl.multiple_of(step * chunk, LANES), chunk, first_unit, units, count - start, weights,
            )

        @pl.when(turns > 0)
        def _():
            clear(accs)
            chi, total = lax.fori_loop(0, turns, add, (zero, zero))
            sums_ref[...] = drained(accs, units)
            weights_ref[:, 0:LANES] = chi
            weights_ref[:, LANES:2 * LANES] = total

        @pl.when(turns == 0)
        def _():
            sums_ref[...] = jnp.zeros_like(sums_ref)
            weights_ref[...] = jnp.zeros_like(weights_ref)

    with_sums(body, units)


def kernel(
    n_tm, n_src, pieces,
    count_ref, design_hbm, unit_hbm, resid_hbm, weight_hbm, damp_hbm, beyond_ref, weights_ref,
    out_ref,
    design_ref, unit_ref, resid_ref, weight_ref, damp_ref,
    sums_ref, kept_ref, extra, part, got, summed, spread, mine, heard, x_away, x_here,
    bytes_ref, load, small, send_a, recv_a, send_b, recv_b, send_c, recv_c,
):
    tm, src = lax.axis_index("tm"), lax.axis_index("src")
    own = damp_ref.shape[1]
    units = own * n_src
    shares = solved_by(n_src)
    n_solve = len(shares)
    first_solver = shares[0][0]
    lanes = own * n_src // n_solve
    solves = (src >= first_solver) & (src < first_solver + 2 * n_solve) & (src % 2 == 1)
    rank = (src - first_solver) // 2
    up = src >= n_src // 2
    starts = [sum(pieces[:i]) for i in range(len(pieces))]

    arrays = (
        (design_hbm, design_ref), (unit_hbm, unit_ref),
        (resid_hbm, resid_ref), (weight_hbm, weight_ref),
    )

    def fetch(step, which):
        far, here = arrays[which]
        cols = pl.ds(starts[step], pieces[step])
        return pltpu.make_async_copy(far.at[:, cols], here.at[:, cols], load.at[step])

    x_away[...] = jnp.zeros_like(x_away)
    damp_copy = pltpu.make_async_copy(damp_hbm, damp_ref, small)
    for step in range(len(pieces)):
        for which in range(4):
            fetch(step, which).start()
    damp_copy.start()

    barrier = pltpu.get_barrier_semaphore()

    def greet(t, p):
        pl.semaphore_signal(
            barrier, inc=1, device_id={"tm": t, "src": p}, device_id_type=pl.DeviceIdType.MESH
        )

    @pl.when(solves)
    def _():
        repeat(n_src - 1, lambda k: greet(tm, skipping(k, src)))

    @pl.when(jnp.logical_not(solves))
    def _():
        repeat(n_solve, lambda k: greet(tm, first_solver + 2 * k))

    for dt in range(1, n_tm):
        repeat(n_solve, lambda k: greet((tm + dt) % n_tm, first_solver + 2 * k))

    first_unit = tm * units
    count = count_ref[0]

    def body(accs):
        clear(accs)
        weights = weights_ref[:, 0:LANES], weights_ref[:, LANES:2 * LANES]
        for step in range(len(pieces)):
            arrived(bytes_ref, pieces[step], load.at[step])
            weights = add_slots(
                accs, (design_ref, unit_ref, resid_ref, weight_ref),
                starts[step], pieces[step], first_unit, units, count, weights,
            )
        sums_ref[...] = beyond_ref[...] + drained(accs, units)
        kept_ref[:, 0:LANES], kept_ref[:, LANES:2 * LANES] = weights

    with_sums(body, units)
    sums = sums_ref[...]
    damp_copy.wait()
    damping = jnp.concatenate([damp_ref[...]] * n_src, axis=1)
    block = lax.broadcasted_iota(jnp.int32, damping.shape, 1) // own
    damping = jnp.where(block == src, damping, 0.0)
    fill = [jnp.zeros((1, units - LANES), jnp.float32)] if units > LANES else []
    chi = jnp.concatenate([kept_ref[:, 0:LANES]] + fill, axis=1)
    total = jnp.concatenate([kept_ref[:, LANES:2 * LANES]] + fill, axis=1)
    left = jnp.concatenate(
        [sums[LANES:ROWS], damping, chi, total,
         jnp.zeros((2 * LANES - ROWS - 3, units), jnp.float32)], axis=0
    )

    def by_solver(rows):
        return jnp.concatenate(
            [rows[b * own:(b + 1) * own] for share in shares for b in share], axis=0
        )

    extra[...] = by_solver(jnp.transpose(left))
    part[:, 0:lanes, :] = by_solver(jnp.transpose(sums[0:LANES])).reshape(n_solve, lanes, LANES)
    packed = extra[pl.ds(0, units // FOLD, stride=FOLD), :]
    lane = lax.broadcasted_iota(jnp.int32, packed.shape, 1) // (LANES // FOLD)
    for b in range(1, FOLD):
        more = extra[pl.ds(b, units // FOLD, stride=FOLD), :]
        packed = jnp.where(lane == b, pltpu.roll(more, b * (LANES // FOLD), 1), packed)
    part[:, lanes:, :] = packed.reshape(n_solve, lanes // FOLD, LANES)

    def send_to(k):
        pltpu.make_async_remote_copy(
            src_ref=part.at[k], dst_ref=got.at[src], send_sem=send_a, recv_sem=recv_a,
            device_id={"tm": tm, "src": first_solver + 2 * k},
            device_id_type=pl.DeviceIdType.MESH,
        ).start()

    def wait_bytes(ref, n, sem):
        some = ref.at[pl.ds(0, n)]
        pltpu.make_async_copy(some, some, sem).wait()

    away = jnp.where(up, n_src // 4, -(n_src // 4))

    def hand_over(i, p):
        return pltpu.make_async_remote_copy(
            src_ref=x_away.at[pl.ds(i * own, own)], dst_ref=x_here,
            send_sem=send_c, recv_sem=recv_c,
            device_id={"tm": tm, "src": p}, device_id_type=pl.DeviceIdType.MESH,
        )

    me = tm * n_solve + rank

    def tell(t, p):
        pltpu.make_async_remote_copy(
            src_ref=mine, dst_ref=heard.at[me], send_sem=send_b, recv_sem=recv_b,
            device_id={"tm": t, "src": p}, device_id_type=pl.DeviceIdType.MESH,
        ).start()

    def tell_both(k):
        p = skipping(k, src)
        for t in range(n_tm):
            tell(t, p)

    @pl.when(solves)
    def _():
        pl.semaphore_wait(barrier, n_tm * n_src - 1)
        repeat(n_solve - 1, lambda k: send_to(ranked(k, rank, n_solve, up)))
        got[src] = part[rank]
        wait_bytes(got, n_src - 1, recv_a)
        both = got[0]
        for p in range(1, n_src):
            both = both + got[p]
        whole, ends = both[0:lanes], both[lanes:]
        for a in range(lanes // FOLD):
            for b in range(FOLD):
                row = ends[a:a + 1]
                spread[pl.ds(a * FOLD + b, 1), :] = (
                    pltpu.roll(row, LANES - b * (LANES // FOLD), 1) if b else row
                )
        summed[0:LANES, :] = jnp.transpose(whole)
        summed[LANES:2 * LANES, :] = jnp.transpose(spread[...])
        damping, chi, total = (summed[pl.ds(ROWS + i, 1), :] for i in range(3))
        x, forward = solve(
            lambda i, j: summed[pl.ds(pair_row(i, j), 1), :],
            lambda i: summed[pl.ds(PAIRS + i, 1), :],
            damping,
        )
        terms = jnp.zeros_like(damping)
        squared = jnp.zeros_like(damping)
        for i in range(WIDTH):
            terms = terms + forward[i] * forward[i]
            squared = squared + x[i] * x[i]
        terms = terms + damping * squared
        none = jnp.zeros((1, LANES // 2 - lanes), jnp.float32)
        mine[...] = jnp.concatenate([chi - terms, none, total, none], axis=1)
        heard[me] = mine[...]
        repeat(n_src - 1, tell_both)
        for dt in range(1, n_tm):
            tell((tm + dt) % n_tm, src)
        answer = jnp.transpose(jnp.concatenate(x, axis=0))
        x_away[:, 0:WIDTH] = answer
        for i, p in ((2, src + away), (3, src - 1 + away), (1, src - 1)):
            hand_over(i, p).start()
        out_ref[:, 0:WIDTH] = answer[0:own]
        wait_bytes(part, n_solve - 1, send_a)
        wait_bytes(heard, n_tm * n_solve - 1, recv_b)

    @pl.when(jnp.logical_not(solves))
    def _():
        pl.semaphore_wait(barrier, n_solve)
        repeat(n_solve, lambda k: send_to(jnp.where(up, k, n_solve - 1 - k)))
        hand_over(0, src).wait_recv()
        out_ref[...] = x_here[...]
        wait_bytes(part, n_solve, send_a)
        wait_bytes(heard, n_tm * n_solve, recv_b)

    both = jnp.sum(heard[...].reshape(n_tm * n_solve, LANES), axis=0, keepdims=True)
    front = lax.broadcasted_iota(jnp.int32, (1, LANES), 1) < LANES // 2
    chi_all = jnp.sum(jnp.where(front, both, 0.0), axis=1, keepdims=True)
    total_all = jnp.sum(jnp.where(front, 0.0, both), axis=1, keepdims=True)
    out_ref[0:1, WIDTH:WIDTH + 1] = chi_all / total_all

    @pl.when(solves)
    def _():
        some = x_away.at[pl.ds(own, 3 * own)]
        pltpu.make_async_copy(some, some, send_c).wait()
        rest = n_tm * n_src - 1
        while rest > 0:
            some = min(rest, n_tm * n_solve)
            wait_bytes(heard, some, send_b)
            rest -= some


def hand_on(both_ref, x_out, misfit_out):
    x_out[...] = both_ref[:, 0:WIDTH]
    misfit_out[...] = both_ref[0:1, WIDTH:WIDTH + 1]


def solution(mesh):
    n_tm, n_src = mesh.shape["tm"], mesh.shape["src"]

    def on_device(design, unit_index, residual, weight, obs_count, damping):
        own = damping.shape[0]
        units = own * n_src
        slots = design.shape[1]
        half = slots // 2
        piece = half // 4 if half % 2048 == 0 else half
        pieces = (piece, half - piece) if half > piece else (half,)
        chunk = next(c for c in (4096, 2048, 1024, 512, 256) if (slots - half) % c == 0)
        n_solve = len(solved_by(n_src))
        lanes = units // n_solve
        anywhere = pl.BlockSpec(memory_space=pl.ANY)
        vmem = pl.BlockSpec(memory_space=pltpu.VMEM)
        kept = lambda v: pltpu.with_memory_space_constraint(v, pltpu.VMEM)
        unit_index, residual, weight = (
            v.reshape(1, slots) for v in (unit_index, residual, weight)
        )
        rest = slots - half
        sums, weights = pl.pallas_call(
            functools.partial(beyond, half, chunk),
            out_shape=(
                pltpu.VMEM((ROWS, units), jnp.float32),
                pltpu.VMEM((1, 2 * LANES), jnp.float32),
            ),
            in_specs=[pl.BlockSpec(memory_space=pltpu.SMEM)] + [anywhere] * 4,
            out_specs=(vmem, vmem),
            scratch_shapes=[
                pltpu.VMEM((WIDTH, rest), jnp.float32),
                pltpu.VMEM((1, rest), jnp.int32),
                pltpu.VMEM((1, rest), jnp.float32),
                pltpu.VMEM((1, rest), jnp.float32),
                pltpu.VMEM((1, (WIDTH + 3) * chunk), jnp.float32),
                pltpu.SemaphoreType.DMA((rest // chunk,)),
            ],
            name="beyond",
        )(obs_count, design, unit_index, residual, weight)
        result = pl.pallas_call(
            functools.partial(kernel, n_tm, n_src, pieces),
            out_shape=pltpu.VMEM((own, LANES), jnp.float32),
            in_specs=[pl.BlockSpec(memory_space=pltpu.SMEM)] + [anywhere] * 5 + [vmem] * 2,
            out_specs=vmem,
            scratch_shapes=[
                pltpu.VMEM((WIDTH, half), jnp.float32),
                pltpu.VMEM((1, half), jnp.int32),
                pltpu.VMEM((1, half), jnp.float32),
                pltpu.VMEM((1, half), jnp.float32),
                pltpu.VMEM((1, own), jnp.float32),
                pltpu.VMEM((ROWS, units), jnp.float32),
                pltpu.VMEM((1, 2 * LANES), jnp.float32),
                pltpu.VMEM((units, LANES), jnp.float32),
                pltpu.VMEM((n_solve, lanes + lanes // FOLD, LANES), jnp.float32),
                pltpu.VMEM((n_src, lanes + lanes // FOLD, LANES), jnp.float32),
                pltpu.VMEM((2 * LANES, lanes), jnp.float32),
                pltpu.VMEM((lanes, LANES), jnp.float32),
                pltpu.VMEM((1, LANES), jnp.float32),
                pltpu.VMEM((n_tm * n_solve, 1, LANES), jnp.float32),
                pltpu.VMEM((lanes, LANES), jnp.float32),
                pltpu.VMEM((own, LANES), jnp.float32),
                pltpu.VMEM((1, (WIDTH + 3) * max(pieces)), jnp.float32),
                pltpu.SemaphoreType.DMA((len(pieces),)),
            ] + [pltpu.SemaphoreType.DMA] * 7,
            compiler_params=pltpu.CompilerParams(collective_id=0, has_side_effects=True),
            name="calibrate",
        )(
            obs_count,
            design,
            unit_index,
            residual,
            weight,
            damping.reshape(1, own),
            kept(sums),
            kept(weights),
        )
        result = kept(result)
        x, misfit = pl.pallas_call(
            hand_on,
            out_shape=(
                jax.ShapeDtypeStruct((own, WIDTH), jnp.float32),
                jax.ShapeDtypeStruct((1, 1), jnp.float32),
            ),
            in_specs=[vmem],
            out_specs=(vmem, vmem),
            name="hand_on",
        )(result)
        return x.T, misfit.reshape(())

    both = ("tm", "src")
    return jax.shard_map(
        on_device,
        mesh=mesh,
        in_specs=(P(None, both), P(both), P(both), P(both), P(both), P(both)),
        out_specs=(P(None, both), P()),
        check_vma=False,
    )
```

```python
import functools

import jax
import jax.numpy as jnp
from jax import lax
from jax.experimental import pallas as pl
from jax.experimental.pallas import tpu as pltpu
from jax.sharding import PartitionSpec as P

WIDTH = 16
HALF = 8
PAIRS = WIDTH * (WIDTH + 1) // 2
ROWS = PAIRS + WIDTH
EVEN = ROWS // WIDTH * WIDTH
LANES = 128
TILE = 256
SHARE = 4
FOLD = 4
PACKED = (ROWS + HALF) // FOLD
AUX = LANES // FOLD


def pair_row(i, j):
    k = (j - i) % WIDTH
    if k > HALF or (k == HALF and i >= HALF):
        i, j = j, i
        k = (j - i) % WIDTH
    return k * WIDTH + i


def stacked_rows(d0, d1, w, wr):
    w0, w1 = d0 * w, d1 * w
    rows = [d0 * w0, d1 * w1]
    sub = lax.broadcasted_iota(jnp.int32, d0.shape, 0)
    for k in range(1, HALF):
        r0 = pltpu.roll(w0, HALF - k, 0)
        r1 = pltpu.roll(w1, HALF - k, 0)
        low = sub < HALF - k
        rows.append(d0 * jnp.where(low, r0, r1))
        rows.append(d1 * jnp.where(low, r1, r0))
    rows.append(d0 * w1)
    rows.append(d0 * wr)
    rows.append(d1 * wr)
    return rows


def rsqrt(value):
    guess = lax.rsqrt(value)
    return guess * (1.5 - 0.5 * value * guess * guess)


def solve(entry, rhs, damping):
    a = {}
    for i in range(WIDTH):
        for j in range(i + 1):
            a[i, j] = entry(i, j)
        a[i, i] = a[i, i] + damping
    b = [rhs(i) for i in range(WIDTH)]
    inverse, forward = [], []
    for j in range(WIDTH):
        inv = rsqrt(a[j, j])
        inverse.append(inv)
        for i in range(j + 1, WIDTH):
            a[i, j] = a[i, j] * inv
        y = b[j] * inv
        forward.append(y)
        for i in range(j + 1, WIDTH):
            b[i] = b[i] - a[i, j] * y
            for k in range(j + 1, i + 1):
                a[i, k] = a[i, k] - a[i, j] * a[k, j]
    run = list(forward)
    x = [None] * WIDTH
    for i in reversed(range(WIDTH)):
        x[i] = run[i] * inverse[i]
        for k in range(i):
            run[k] = run[k] - a[i, k] * x[i]
    return x, forward


def skipping(k, me):
    return k + jnp.where(k >= me, 1, 0)


def ranked(k, me, n, up):
    k = skipping(k, jnp.where(up, me, n - 1 - me))
    return jnp.where(up, k, n - 1 - k)


def repeat(n, body):
    if n <= 32:
        for k in range(n):
            body(k)
    elif n:
        lax.fori_loop(0, n, lambda k, c: (body(k), c)[1], 0)


def block_at(place, n_src):
    q = n_src // 4
    solver = q + 1 + 2 * (place // SHARE)
    turn = place % SHARE
    away = jnp.where(solver < 2 * q, -q, q)
    return solver - turn % 2 + jnp.where(turn >= 2, away, 0)


def add_slots(accs, refs, ids, begin, chunk, first_unit, count, weights):
    design_ref, unit_ref, resid_ref, weight_ref = refs
    chi, total = weights
    for t in range(chunk // TILE):
        cols = pl.ds(begin + t * TILE, TILE)
        w = weight_ref[:, cols]
        live = begin + t * TILE + lax.broadcasted_iota(jnp.int32, w.shape, 1) < count
        w = jnp.where(live, w, 0.0)
        r = resid_ref[:, cols]
        wr = w * r
        rows = stacked_rows(design_ref[0:HALF, cols], design_ref[HALF:WIDTH, cols], w, wr)
        lhs = []
        for k in range(0, len(rows) - 1, 2):
            x = jnp.concatenate(rows[k:k + 2], axis=0)
            high = x.astype(jnp.bfloat16)
            lhs += [high, (x - high.astype(jnp.float32)).astype(jnp.bfloat16)]
        high = rows[-1].astype(jnp.bfloat16).astype(jnp.float32)
        lhs.append(jnp.concatenate([high, rows[-1] - high], axis=0).astype(jnp.bfloat16))
        lhs = jnp.concatenate(lhs, axis=0)
        unit = unit_ref[:, cols] - first_unit
        wrr = wr * r
        for k in range(TILE // LANES):
            chi = chi + wrr[:, k * LANES:(k + 1) * LANES]
            total = total + w[:, k * LANES:(k + 1) * LANES]
        q = t % 2
        for n, acc in enumerate(accs[q]):
            pltpu.matmul_push_rhs(
                one_hot(unit, n, ids), staging_register=0, mxu_index=q, transpose=True
            )
            pltpu.matmul_acc_lhs(acc, lhs, load_staged_rhs=0)
    return chi, total


def fill_ids(ids, own, n_src):
    place = lax.broadcasted_iota(jnp.int32, ids.shape, 0)
    unit = block_at(place // own, n_src) * own + place % own
    ids[...] = unit.astype(jnp.int16)


def one_hot(unit, n, ids):
    rows = min(ids.shape[0] - n * TILE, TILE)
    here = ids[pl.ds(n * TILE, rows), :] == unit.astype(jnp.int16)
    hot = jnp.where(here, jnp.bfloat16(1), jnp.bfloat16(0))
    if rows < TILE:
        hot = jnp.concatenate([hot, jnp.zeros((TILE - rows, TILE), jnp.bfloat16)], axis=0)
    return hot


def clear(accs):
    for q in range(2):
        for acc in accs[q]:
            pltpu.matmul_pop(acc)


def drained(accs, units):
    tiles = []
    for n in range(len(accs[0])):
        both = pltpu.matmul_pop(accs[0][n]) + pltpu.matmul_pop(accs[1][n])
        sums = [
            both[2 * k:2 * k + WIDTH] + both[2 * k + WIDTH:2 * k + 2 * WIDTH]
            for k in range(0, EVEN, WIDTH)
        ]
        sums.append(both[2 * EVEN:EVEN + ROWS] + both[EVEN + ROWS:])
        tiles.append(jnp.concatenate(sums, axis=0))
    return jnp.concatenate(tiles, axis=1)[:, 0:units]


def with_sums(body, units):
    tiles = -(-units // TILE)
    shape = (2 * ROWS, TILE)
    pl.run_scoped(
        lambda *accs: body((accs[0:tiles], accs[tiles:2 * tiles])),
        *[pltpu.ACC(q)(shape, jnp.float32) for q in range(2) for _ in range(tiles)],
    )


def arrived(bytes_ref, chunk, sem):
    some = bytes_ref.at[:, pl.ds(0, (WIDTH + 3) * chunk)]
    pltpu.make_async_copy(some, some, sem).wait()


def beyond(
    start, chunk, n_src,
    count_ref, design_hbm, unit_hbm, resid_hbm, weight_hbm,
    sums_ref, weights_ref,
    design_ref, unit_ref, resid_ref, weight_ref, ids, bytes_ref, load,
):
    units = sums_ref.shape[1]
    slots = design_hbm.shape[1]
    first_unit = lax.axis_index("tm") * units
    count = count_ref[0]
    turns = (jnp.clip(count, start, slots) - start + chunk - 1) // chunk
    arrays = (
        (design_hbm, design_ref), (unit_hbm, unit_ref),
        (resid_hbm, resid_ref), (weight_hbm, weight_ref),
    )

    def fetch(step, which):
        far, here = arrays[which]
        size = pl.ds(pl.multiple_of(start + step * chunk, LANES), chunk)
        to = pl.ds(pl.multiple_of(step * chunk, LANES), chunk)
        return pltpu.make_async_copy(far.at[:, size], here.at[:, to], load.at[step])

    def fetch_all(step, c):
        for which in range(4):
            fetch(step, which).start()
        return c

    lax.fori_loop(0, turns, fetch_all, 0)

    def body(accs):
        zero = jnp.zeros((1, LANES), jnp.float32)

        def add(step, weights):
            arrived(bytes_ref, chunk, load.at[step])
            return add_slots(
                accs, (design_ref, unit_ref, resid_ref, weight_ref), ids,
                pl.multiple_of(step * chunk, LANES), chunk, first_unit, count - start, weights,
            )

        @pl.when(turns > 0)
        def _():
            clear(accs)
            fill_ids(ids, units // n_src, n_src)
            chi, total = lax.fori_loop(0, turns, add, (zero, zero))
            sums_ref[...] = drained(accs, units)
            weights_ref[:, 0:LANES] = chi
            weights_ref[:, LANES:2 * LANES] = total

        @pl.when(turns == 0)
        def _():
            sums_ref[...] = jnp.zeros_like(sums_ref)
            weights_ref[...] = jnp.zeros_like(weights_ref)

    with_sums(body, units)


def kernel(
    n_tm, n_src, pieces,
    count_ref, design_hbm, unit_hbm, resid_hbm, weight_hbm, damp_hbm, beyond_ref, weights_ref,
    out_ref,
    design_ref, unit_ref, resid_ref, weight_ref, damp_ref,
    sums_ref, kept_ref, part, got, summed, mine, heard, x_away, x_here,
    ids, bytes_ref, load, small, send_a, recv_a, send_b, recv_b, send_c, recv_c,
):
    tm, src = lax.axis_index("tm"), lax.axis_index("src")
    own = damp_ref.shape[1]
    units = own * n_src
    n_solve = n_src // SHARE
    first_solver = n_src // 4 + 1
    lanes = own * SHARE
    solves = (src >= first_solver) & (src < first_solver + 2 * n_solve) & (src % 2 == 1)
    rank = (src - first_solver) // 2
    up = src >= n_src // 2
    starts = [sum(pieces[:i]) for i in range(len(pieces))]

    arrays = (
        (design_hbm, design_ref), (unit_hbm, unit_ref),
        (resid_hbm, resid_ref), (weight_hbm, weight_ref),
    )

    def fetch(step, which):
        far, here = arrays[which]
        cols = pl.ds(starts[step], pieces[step])
        return pltpu.make_async_copy(far.at[:, cols], here.at[:, cols], load.at[step])

    x_away[...] = jnp.zeros_like(x_away)
    damp_copy = pltpu.make_async_copy(damp_hbm, damp_ref, small)
    for step in range(len(pieces)):
        for which in range(4):
            fetch(step, which).start()
    damp_copy.start()

    barrier = pltpu.get_barrier_semaphore()

    def greet(t, p):
        pl.semaphore_signal(
            barrier, inc=1, device_id={"tm": t, "src": p}, device_id_type=pl.DeviceIdType.MESH
        )

    @pl.when(solves)
    def _():
        repeat(n_src - 1, lambda k: greet(tm, skipping(k, src)))

    @pl.when(jnp.logical_not(solves))
    def _():
        repeat(n_solve, lambda k: greet(tm, first_solver + 2 * k))

    for dt in range(1, n_tm):
        repeat(n_solve, lambda k: greet((tm + dt) % n_tm, first_solver + 2 * k))

    first_unit = tm * units
    count = count_ref[0]
    fill_ids(ids, own, n_src)

    def body(accs):
        clear(accs)
        weights = weights_ref[:, 0:LANES], weights_ref[:, LANES:2 * LANES]
        for step in range(len(pieces)):
            arrived(bytes_ref, pieces[step], load.at[step])
            weights = add_slots(
                accs, (design_ref, unit_ref, resid_ref, weight_ref), ids,
                starts[step], pieces[step], first_unit, count, weights,
            )
        sums_ref[...] = beyond_ref[...] + drained(accs, units)
        kept_ref[:, 0:LANES], kept_ref[:, LANES:2 * LANES] = weights

    with_sums(body, units)
    sums = sums_ref[...]
    damp_copy.wait()
    damping = jnp.concatenate([damp_ref[...]] * n_src, axis=1)
    place = lax.broadcasted_iota(jnp.int32, damping.shape, 1) // own
    damping = jnp.where(block_at(place, n_src) == src, damping, 0.0)
    fill = [jnp.zeros((1, units - LANES), jnp.float32)] if units > LANES else []
    chi = jnp.concatenate([kept_ref[:, 0:LANES]] + fill, axis=1)
    total = jnp.concatenate([kept_ref[:, LANES:2 * LANES]] + fill, axis=1)
    none = jnp.zeros((FOLD * PACKED - ROWS - 3, units), jnp.float32)
    rows = jnp.concatenate([sums, damping, chi, total, none], axis=0)
    group = lax.broadcasted_iota(jnp.int32, (PACKED, LANES), 1) // AUX
    for k in range(n_solve):
        first = k * lanes // LANES * LANES
        for g in range(FOLD):
            more = rows[g * PACKED:(g + 1) * PACKED, first:first + LANES]
            shift = (g * AUX - k * lanes) % LANES
            more = pltpu.roll(more, shift, 1) if shift else more
            message = jnp.where(group == g, more, message) if g else more
        part[k] = message

    def send_to(k):
        pltpu.make_async_remote_copy(
            src_ref=part.at[k], dst_ref=got.at[src], send_sem=send_a, recv_sem=recv_a,
            device_id={"tm": tm, "src": first_solver + 2 * k},
            device_id_type=pl.DeviceIdType.MESH,
        ).start()

    def wait_bytes(ref, n, sem):
        some = ref.at[pl.ds(0, n)]
        pltpu.make_async_copy(some, some, sem).wait()

    away = jnp.where(up, n_src // 4, -(n_src // 4))

    def hand_over(i, p):
        return pltpu.make_async_remote_copy(
            src_ref=x_away.at[pl.ds(i * own, own)], dst_ref=x_here,
            send_sem=send_c, recv_sem=recv_c,
            device_id={"tm": tm, "src": p}, device_id_type=pl.DeviceIdType.MESH,
        )

    me = tm * n_solve + rank

    def tell(t, p):
        pltpu.make_async_remote_copy(
            src_ref=mine, dst_ref=heard.at[me], send_sem=send_b, recv_sem=recv_b,
            device_id={"tm": t, "src": p}, device_id_type=pl.DeviceIdType.MESH,
        ).start()

    def tell_both(k):
        p = skipping(k, src)
        for t in range(n_tm):
            tell(t, p)

    @pl.when(solves)
    def _():
        pl.semaphore_wait(barrier, n_tm * n_src - 1)
        repeat(n_solve - 1, lambda k: send_to(ranked(k, rank, n_solve, up)))
        got[src] = part[rank]
        wait_bytes(got, n_src - 1, recv_a)
        both = got[0]
        for p in range(1, n_src):
            both = both + got[p]
        for g in range(FOLD):
            more = pltpu.roll(both, LANES - g * AUX, 1) if g else both
            summed[pl.ds(g * PACKED, PACKED), :] = more[:, 0:lanes]
        damping, chi, total = (summed[pl.ds(ROWS + i, 1), :] for i in range(3))
        x, forward = solve(
            lambda i, j: summed[pl.ds(pair_row(i, j), 1), :],
            lambda i: summed[pl.ds(PAIRS + i, 1), :],
            damping,
        )
        terms = jnp.zeros_like(damping)
        squared = jnp.zeros_like(damping)
        for i in range(WIDTH):
            terms = terms + forward[i] * forward[i]
            squared = squared + x[i] * x[i]
        terms = terms + damping * squared
        none = jnp.zeros((1, LANES // 2 - lanes), jnp.float32)
        mine[...] = jnp.concatenate([chi - terms, none, total, none], axis=1)
        heard[me] = mine[...]
        repeat(n_src - 1, tell_both)
        for dt in range(1, n_tm):
            tell((tm + dt) % n_tm, src)
        answer = jnp.transpose(jnp.concatenate(x, axis=0))
        x_away[:, 0:WIDTH] = answer
        for i, p in ((2, src + away), (3, src - 1 + away), (1, src - 1)):
            hand_over(i, p).start()
        out_ref[:, 0:WIDTH] = answer[0:own]
        wait_bytes(part, n_solve - 1, send_a)
        wait_bytes(heard, n_tm * n_solve - 1, recv_b)

    @pl.when(jnp.logical_not(solves))
    def _():
        pl.semaphore_wait(barrier, n_solve)
        repeat(n_solve, lambda k: send_to(jnp.where(up, k, n_solve - 1 - k)))
        hand_over(0, src).wait_recv()
        out_ref[...] = x_here[...]
        wait_bytes(part, n_solve, send_a)
        wait_bytes(heard, n_tm * n_solve, recv_b)

    both = jnp.sum(heard[...].reshape(n_tm * n_solve, LANES), axis=0, keepdims=True)
    front = lax.broadcasted_iota(jnp.int32, (1, LANES), 1) < LANES // 2
    chi_all = jnp.sum(jnp.where(front, both, 0.0), axis=1, keepdims=True)
    total_all = jnp.sum(jnp.where(front, 0.0, both), axis=1, keepdims=True)
    out_ref[0:1, WIDTH:WIDTH + 1] = chi_all / total_all

    @pl.when(solves)
    def _():
        some = x_away.at[pl.ds(own, 3 * own)]
        pltpu.make_async_copy(some, some, send_c).wait()
        rest = n_tm * n_src - 1
        while rest > 0:
            some = min(rest, n_tm * n_solve)
            wait_bytes(heard, some, send_b)
            rest -= some


def hand_on(both_ref, x_out, misfit_out):
    x_out[...] = both_ref[:, 0:WIDTH]
    misfit_out[...] = both_ref[0:1, WIDTH:WIDTH + 1]


def solution(mesh):
    n_tm, n_src = mesh.shape["tm"], mesh.shape["src"]

    def on_device(design, unit_index, residual, weight, obs_count, damping):
        own = damping.shape[0]
        units = own * n_src
        slots = design.shape[1]
        half = slots // 2
        piece = half // 4 if half % 2048 == 0 else half
        pieces = (piece, half - piece) if half > piece else (half,)
        chunk = next(c for c in (4096, 2048, 1024, 512, 256) if (slots - half) % c == 0)
        n_solve, lanes = n_src // SHARE, own * SHARE
        anywhere = pl.BlockSpec(memory_space=pl.ANY)
        vmem = pl.BlockSpec(memory_space=pltpu.VMEM)
        kept = lambda v: pltpu.with_memory_space_constraint(v, pltpu.VMEM)
        unit_index, residual, weight = (
            v.reshape(1, slots) for v in (unit_index, residual, weight)
        )
        rest = slots - half
        sums, weights = pl.pallas_call(
            functools.partial(beyond, half, chunk, n_src),
            out_shape=(
                pltpu.VMEM((ROWS, units), jnp.float32),
                pltpu.VMEM((1, 2 * LANES), jnp.float32),
            ),
            in_specs=[pl.BlockSpec(memory_space=pltpu.SMEM)] + [anywhere] * 4,
            out_specs=(vmem, vmem),
            scratch_shapes=[
                pltpu.VMEM((WIDTH, rest), jnp.float32),
                pltpu.VMEM((1, rest), jnp.int32),
                pltpu.VMEM((1, rest), jnp.float32),
                pltpu.VMEM((1, rest), jnp.float32),
                pltpu.VMEM((units, TILE), jnp.int16),
                pltpu.VMEM((1, (WIDTH + 3) * chunk), jnp.float32),
                pltpu.SemaphoreType.DMA((rest // chunk,)),
            ],
            name="beyond",
        )(obs_count, design, unit_index, residual, weight)
        result = pl.pallas_call(
            functools.partial(kernel, n_tm, n_src, pieces),
            out_shape=pltpu.VMEM((own, LANES), jnp.float32),
            in_specs=[pl.BlockSpec(memory_space=pltpu.SMEM)] + [anywhere] * 5 + [vmem] * 2,
            out_specs=vmem,
            scratch_shapes=[
                pltpu.VMEM((WIDTH, half), jnp.float32),
                pltpu.VMEM((1, half), jnp.int32),
                pltpu.VMEM((1, half), jnp.float32),
                pltpu.VMEM((1, half), jnp.float32),
                pltpu.VMEM((1, own), jnp.float32),
                pltpu.VMEM((ROWS, units), jnp.float32),
                pltpu.VMEM((1, 2 * LANES), jnp.float32),
                pltpu.VMEM((n_solve, PACKED, LANES), jnp.float32),
                pltpu.VMEM((n_src, PACKED, LANES), jnp.float32),
                pltpu.VMEM((FOLD * PACKED, lanes), jnp.float32),
                pltpu.VMEM((1, LANES), jnp.float32),
                pltpu.VMEM((n_tm * n_solve, 1, LANES), jnp.float32),
                pltpu.VMEM((lanes, LANES), jnp.float32),
                pltpu.VMEM((own, LANES), jnp.float32),
                pltpu.VMEM((units, TILE), jnp.int16),
                pltpu.VMEM((1, (WIDTH + 3) * max(pieces)), jnp.float32),
                pltpu.SemaphoreType.DMA((len(pieces),)),
            ] + [pltpu.SemaphoreType.DMA] * 7,
            compiler_params=pltpu.CompilerParams(collective_id=0, has_side_effects=True),
            name="calibrate",
        )(
            obs_count,
            design,
            unit_index,
            residual,
            weight,
            damping.reshape(1, own),
            kept(sums),
            kept(weights),
        )
        result = kept(result)
        x, misfit = pl.pallas_call(
            hand_on,
            out_shape=(
                jax.ShapeDtypeStruct((own, WIDTH), jnp.float32),
                jax.ShapeDtypeStruct((1, 1), jnp.float32),
            ),
            in_specs=[vmem],
            out_specs=(vmem, vmem),
            name="hand_on",
        )(result)
        return x.T, misfit.reshape(())

    both = ("tm", "src")
    return jax.shard_map(
        on_device,
        mesh=mesh,
        in_specs=(P(None, both), P(both), P(both), P(both), P(both), P(both)),
        out_specs=(P(None, both), P()),
        check_vma=False,
    )
```

```python
import functools

import jax
import jax.numpy as jnp
from jax import lax
from jax.experimental import pallas as pl
from jax.experimental.pallas import tpu as pltpu
from jax.sharding import PartitionSpec as P

WIDTH = 16
HALF = 8
PAIRS = WIDTH * (WIDTH + 1) // 2
ROWS = PAIRS + WIDTH
EVEN = ROWS // WIDTH * WIDTH
LANES = 128
TILE = 256
SHARE = 4
FOLD = 4
PACKED = (ROWS + HALF) // FOLD
AUX = LANES // FOLD


def pair_row(i, j):
    k = (j - i) % WIDTH
    if k > HALF or (k == HALF and i >= HALF):
        i, j = j, i
        k = (j - i) % WIDTH
    return k * WIDTH + i


def stacked_rows(d0, d1, w, wr):
    w0, w1 = d0 * w, d1 * w
    rows = [d0 * w0, d1 * w1]
    sub = lax.broadcasted_iota(jnp.int32, d0.shape, 0)
    for k in range(1, HALF):
        r0 = pltpu.roll(w0, HALF - k, 0)
        r1 = pltpu.roll(w1, HALF - k, 0)
        low = sub < HALF - k
        rows.append(d0 * jnp.where(low, r0, r1))
        rows.append(d1 * jnp.where(low, r1, r0))
    rows.append(d0 * w1)
    rows.append(d0 * wr)
    rows.append(d1 * wr)
    return rows


def rsqrt(value):
    guess = lax.rsqrt(value)
    return guess * (1.5 - 0.5 * value * guess * guess)


def solve(entry, rhs, damping):
    a = {}
    for i in range(WIDTH):
        for j in range(i + 1):
            a[i, j] = entry(i, j)
        a[i, i] = a[i, i] + damping
    b = [rhs(i) for i in range(WIDTH)]
    inverse, forward = [], []
    for j in range(WIDTH):
        inv = rsqrt(a[j, j])
        inverse.append(inv)
        for i in range(j + 1, WIDTH):
            a[i, j] = a[i, j] * inv
        y = b[j] * inv
        forward.append(y)
        for i in range(j + 1, WIDTH):
            b[i] = b[i] - a[i, j] * y
            for k in range(j + 1, i + 1):
                a[i, k] = a[i, k] - a[i, j] * a[k, j]
    run = list(forward)
    x = [None] * WIDTH
    for i in reversed(range(WIDTH)):
        x[i] = run[i] * inverse[i]
        for k in range(i):
            run[k] = run[k] - a[i, k] * x[i]
    return x, forward


def skipping(k, me):
    return k + jnp.where(k >= me, 1, 0)


def ranked(k, me, n, up):
    k = skipping(k, jnp.where(up, me, n - 1 - me))
    return jnp.where(up, k, n - 1 - k)


def repeat(n, body):
    if n <= 32:
        for k in range(n):
            body(k)
    elif n:
        lax.fori_loop(0, n, lambda k, c: (body(k), c)[1], 0)


def block_at(place, n_src):
    q = n_src // 4
    solver = q + 1 + 2 * (place // SHARE)
    turn = place % SHARE
    away = jnp.where(solver < 2 * q, -q, q)
    return solver - turn % 2 + jnp.where(turn >= 2, away, 0)


def add_slots(accs, refs, ids, begin, chunk, first_unit, count, weights):
    design_ref, unit_ref, resid_ref, weight_ref = refs
    chi, total = weights
    for t in range(chunk // TILE):
        cols = pl.ds(begin + t * TILE, TILE)
        w = weight_ref[:, cols]
        live = begin + t * TILE + lax.broadcasted_iota(jnp.int32, w.shape, 1) < count
        w = jnp.where(live, w, 0.0)
        r = resid_ref[:, cols]
        wr = w * r
        rows = stacked_rows(design_ref[0:HALF, cols], design_ref[HALF:WIDTH, cols], w, wr)
        lhs = []
        for k in range(0, len(rows) - 1, 2):
            x = jnp.concatenate(rows[k:k + 2], axis=0)
            high = x.astype(jnp.bfloat16)
            lhs += [high, (x - high.astype(jnp.float32)).astype(jnp.bfloat16)]
        high = rows[-1].astype(jnp.bfloat16).astype(jnp.float32)
        lhs.append(jnp.concatenate([high, rows[-1] - high], axis=0).astype(jnp.bfloat16))
        lhs = jnp.concatenate(lhs, axis=0)
        unit = unit_ref[:, cols] - first_unit
        wrr = wr * r
        for k in range(TILE // LANES):
            chi = chi + wrr[:, k * LANES:(k + 1) * LANES]
            total = total + w[:, k * LANES:(k + 1) * LANES]
        q = t % 2
        for n, acc in enumerate(accs[q]):
            pltpu.matmul_push_rhs(
                one_hot(unit, n, ids), staging_register=0, mxu_index=q, transpose=True
            )
            pltpu.matmul_acc_lhs(acc, lhs, load_staged_rhs=0)
    return chi, total


def fill_ids(ids, own, n_src):
    place = lax.broadcasted_iota(jnp.int32, ids.shape, 0)
    unit = block_at(place // own, n_src) * own + place % own
    ids[...] = unit.astype(jnp.int16)


def one_hot(unit, n, ids):
    rows = min(ids.shape[0] - n * TILE, TILE)
    here = ids[pl.ds(n * TILE, rows), :] == unit.astype(jnp.int16)
    hot = jnp.where(here, jnp.bfloat16(1), jnp.bfloat16(0))
    if rows < TILE:
        hot = jnp.concatenate([hot, jnp.zeros((TILE - rows, TILE), jnp.bfloat16)], axis=0)
    return hot


def clear(accs):
    for q in range(2):
        for acc in accs[q]:
            pltpu.matmul_pop(acc)


def drained(accs, units):
    tiles = []
    for n in range(len(accs[0])):
        both = pltpu.matmul_pop(accs[0][n]) + pltpu.matmul_pop(accs[1][n])
        sums = [
            both[2 * k:2 * k + WIDTH] + both[2 * k + WIDTH:2 * k + 2 * WIDTH]
            for k in range(0, EVEN, WIDTH)
        ]
        sums.append(both[2 * EVEN:EVEN + ROWS] + both[EVEN + ROWS:])
        tiles.append(jnp.concatenate(sums, axis=0))
    return jnp.concatenate(tiles, axis=1)[:, 0:units]


def with_sums(body, units):
    tiles = -(-units // TILE)
    shape = (2 * ROWS, TILE)
    return pl.run_scoped(
        lambda *accs: body((accs[0:tiles], accs[tiles:2 * tiles])),
        *[pltpu.ACC(q)(shape, jnp.float32) for q in range(2) for _ in range(tiles)],
    )


def arrived(bytes_ref, chunk, sem):
    some = bytes_ref.at[:, pl.ds(0, (WIDTH + 3) * chunk)]
    pltpu.make_async_copy(some, some, sem).wait()


def beyond(
    start, chunk, n_src,
    count_ref, design_hbm, unit_hbm, resid_hbm, weight_hbm,
    sums_ref, weights_ref,
    design_ref, unit_ref, resid_ref, weight_ref, ids, bytes_ref, load,
):
    units = sums_ref.shape[1]
    slots = design_hbm.shape[1]
    first_unit = lax.axis_index("tm") * units
    count = count_ref[0]
    turns = (jnp.clip(count, start, slots) - start + chunk - 1) // chunk
    arrays = (
        (design_hbm, design_ref), (unit_hbm, unit_ref),
        (resid_hbm, resid_ref), (weight_hbm, weight_ref),
    )

    def fetch(step, which):
        far, here = arrays[which]
        size = pl.ds(pl.multiple_of(start + step * chunk, LANES), chunk)
        to = pl.ds(pl.multiple_of(step * chunk, LANES), chunk)
        return pltpu.make_async_copy(far.at[:, size], here.at[:, to], load.at[step])

    def fetch_all(step, c):
        for which in range(4):
            fetch(step, which).start()
        return c

    lax.fori_loop(0, turns, fetch_all, 0)

    def body(accs):
        zero = jnp.zeros((1, LANES), jnp.float32)

        def add(step, weights):
            arrived(bytes_ref, chunk, load.at[step])
            return add_slots(
                accs, (design_ref, unit_ref, resid_ref, weight_ref), ids,
                pl.multiple_of(step * chunk, LANES), chunk, first_unit, count - start, weights,
            )

        @pl.when(turns > 0)
        def _():
            clear(accs)
            fill_ids(ids, units // n_src, n_src)
            chi, total = lax.fori_loop(0, turns, add, (zero, zero))
            sums_ref[...] = drained(accs, units)
            weights_ref[:, 0:LANES] = chi
            weights_ref[:, LANES:2 * LANES] = total

        @pl.when(turns == 0)
        def _():
            sums_ref[...] = jnp.zeros_like(sums_ref)
            weights_ref[...] = jnp.zeros_like(weights_ref)

    with_sums(body, units)


def kernel(
    n_tm, n_src, pieces,
    count_ref, design_hbm, unit_hbm, resid_hbm, weight_hbm, damp_hbm, beyond_ref, weights_ref,
    out_ref,
    design_ref, unit_ref, resid_ref, weight_ref, damp_ref,
    part, got, summed, mine, heard, x_away, x_here,
    ids, bytes_ref, load, small, send_a, recv_a, send_b, recv_b, send_c, recv_c,
):
    tm, src = lax.axis_index("tm"), lax.axis_index("src")
    own = damp_ref.shape[1]
    units = own * n_src
    n_solve = n_src // SHARE
    first_solver = n_src // 4 + 1
    lanes = own * SHARE
    solves = (src >= first_solver) & (src < first_solver + 2 * n_solve) & (src % 2 == 1)
    rank = (src - first_solver) // 2
    up = src >= n_src // 2
    starts = [sum(pieces[:i]) for i in range(len(pieces))]

    arrays = (
        (design_hbm, design_ref), (unit_hbm, unit_ref),
        (resid_hbm, resid_ref), (weight_hbm, weight_ref),
    )

    def fetch(step, which):
        far, here = arrays[which]
        cols = pl.ds(starts[step], pieces[step])
        return pltpu.make_async_copy(far.at[:, cols], here.at[:, cols], load.at[step])

    x_away[...] = jnp.zeros_like(x_away)
    damp_copy = pltpu.make_async_copy(damp_hbm, damp_ref, small)
    for step in range(len(pieces)):
        for which in range(4):
            fetch(step, which).start()
    damp_copy.start()

    barrier = pltpu.get_barrier_semaphore()

    def greet(t, p):
        pl.semaphore_signal(
            barrier, inc=1, device_id={"tm": t, "src": p}, device_id_type=pl.DeviceIdType.MESH
        )

    @pl.when(solves)
    def _():
        repeat(n_src - 1, lambda k: greet(tm, skipping(k, src)))

    @pl.when(jnp.logical_not(solves))
    def _():
        repeat(n_solve, lambda k: greet(tm, first_solver + 2 * k))

    for dt in range(1, n_tm):
        repeat(n_solve, lambda k: greet((tm + dt) % n_tm, first_solver + 2 * k))

    first_unit = tm * units
    count = count_ref[0]
    fill_ids(ids, own, n_src)

    def body(accs):
        clear(accs)
        weights = weights_ref[:, 0:LANES], weights_ref[:, LANES:2 * LANES]
        for step in range(len(pieces)):
            arrived(bytes_ref, pieces[step], load.at[step])
            weights = add_slots(
                accs, (design_ref, unit_ref, resid_ref, weight_ref), ids,
                starts[step], pieces[step], first_unit, count, weights,
            )
        return (beyond_ref[...] + drained(accs, units), *weights)

    sums, chi, total = with_sums(body, units)
    damp_copy.wait()
    damping = jnp.concatenate([damp_ref[...]] * n_src, axis=1)
    place = lax.broadcasted_iota(jnp.int32, damping.shape, 1) // own
    damping = jnp.where(block_at(place, n_src) == src, damping, 0.0)
    fill = [jnp.zeros((1, units - LANES), jnp.float32)] if units > LANES else []
    chi = jnp.concatenate([chi] + fill, axis=1)
    total = jnp.concatenate([total] + fill, axis=1)
    none = jnp.zeros((FOLD * PACKED - ROWS - 3, units), jnp.float32)
    rows = jnp.concatenate([sums, damping, chi, total, none], axis=0)
    group = lax.broadcasted_iota(jnp.int32, (PACKED, LANES), 1) // AUX
    for k in range(n_solve):
        first = k * lanes // LANES * LANES
        for g in range(FOLD):
            more = rows[g * PACKED:(g + 1) * PACKED, first:first + LANES]
            shift = (g * AUX - k * lanes) % LANES
            more = pltpu.roll(more, shift, 1) if shift else more
            message = jnp.where(group == g, more, message) if g else more
        part[k] = message

    def send_to(k):
        pltpu.make_async_remote_copy(
            src_ref=part.at[k], dst_ref=got.at[src], send_sem=send_a, recv_sem=recv_a,
            device_id={"tm": tm, "src": first_solver + 2 * k},
            device_id_type=pl.DeviceIdType.MESH,
        ).start()

    def wait_bytes(ref, n, sem):
        some = ref.at[pl.ds(0, n)]
        pltpu.make_async_copy(some, some, sem).wait()

    away = jnp.where(up, n_src // 4, -(n_src // 4))

    def hand_over(i, p):
        return pltpu.make_async_remote_copy(
            src_ref=x_away.at[pl.ds(i * own, own)], dst_ref=x_here,
            send_sem=send_c, recv_sem=recv_c,
            device_id={"tm": tm, "src": p}, device_id_type=pl.DeviceIdType.MESH,
        )

    me = tm * n_solve + rank

    def tell(t, p):
        pltpu.make_async_remote_copy(
            src_ref=mine, dst_ref=heard.at[me], send_sem=send_b, recv_sem=recv_b,
            device_id={"tm": t, "src": p}, device_id_type=pl.DeviceIdType.MESH,
        ).start()

    def tell_both(k):
        p = skipping(k, src)
        for t in range(n_tm):
            tell(t, p)

    @pl.when(solves)
    def _():
        pl.semaphore_wait(barrier, n_tm * n_src - 1)
        repeat(n_solve - 1, lambda k: send_to(ranked(k, rank, n_solve, up)))
        got[src] = part[rank]
        wait_bytes(got, n_src - 1, recv_a)
        each = [got[p] for p in range(n_src)]
        while len(each) > 1:
            each = [a + b for a, b in zip(each[::2], each[1::2])] + each[len(each) // 2 * 2:]
        both = each[0]
        for g in range(FOLD):
            more = pltpu.roll(both, LANES - g * AUX, 1) if g else both
            summed[pl.ds(g * PACKED, PACKED), :] = more[:, 0:lanes]
        damping, chi, total = (summed[pl.ds(ROWS + i, 1), :] for i in range(3))
        x, forward = solve(
            lambda i, j: summed[pl.ds(pair_row(i, j), 1), :],
            lambda i: summed[pl.ds(PAIRS + i, 1), :],
            damping,
        )
        terms = jnp.zeros_like(damping)
        squared = jnp.zeros_like(damping)
        for i in reversed(range(WIDTH)):
            terms = terms + forward[i] * forward[i]
            squared = squared + x[i] * x[i]
        terms = terms + damping * squared
        none = jnp.zeros((1, LANES // 2 - lanes), jnp.float32)
        mine[...] = jnp.concatenate([chi - terms, none, total, none], axis=1)
        heard[me] = mine[...]
        repeat(n_src - 1, tell_both)
        for dt in range(1, n_tm):
            tell((tm + dt) % n_tm, src)
        answer = jnp.transpose(jnp.concatenate(x, axis=0))
        x_away[:, 0:WIDTH] = answer
        for i, p in ((2, src + away), (3, src - 1 + away), (1, src - 1)):
            hand_over(i, p).start()
        out_ref[:, 0:WIDTH] = answer[0:own]
        wait_bytes(part, n_solve - 1, send_a)
        wait_bytes(heard, n_tm * n_solve - 1, recv_b)

    @pl.when(jnp.logical_not(solves))
    def _():
        pl.semaphore_wait(barrier, n_solve)
        repeat(n_solve, lambda k: send_to(jnp.where(up, k, n_solve - 1 - k)))
        hand_over(0, src).wait_recv()
        out_ref[...] = x_here[...]
        wait_bytes(part, n_solve, send_a)
        wait_bytes(heard, n_tm * n_solve, recv_b)

    both = jnp.sum(heard[...].reshape(n_tm * n_solve, LANES), axis=0, keepdims=True)
    front = lax.broadcasted_iota(jnp.int32, (1, LANES), 1) < LANES // 2
    chi_all = jnp.sum(jnp.where(front, both, 0.0), axis=1, keepdims=True)
    total_all = jnp.sum(jnp.where(front, 0.0, both), axis=1, keepdims=True)
    out_ref[0:1, WIDTH:WIDTH + 1] = chi_all / total_all

    @pl.when(solves)
    def _():
        some = x_away.at[pl.ds(own, 3 * own)]
        pltpu.make_async_copy(some, some, send_c).wait()
        rest = n_tm * n_src - 1
        while rest > 0:
            some = min(rest, n_tm * n_solve)
            wait_bytes(heard, some, send_b)
            rest -= some


def hand_on(both_ref, x_out, misfit_out):
    x_out[...] = both_ref[:, 0:WIDTH]
    misfit_out[...] = both_ref[0:1, WIDTH:WIDTH + 1]


def solution(mesh):
    n_tm, n_src = mesh.shape["tm"], mesh.shape["src"]

    def on_device(design, unit_index, residual, weight, obs_count, damping):
        own = damping.shape[0]
        units = own * n_src
        slots = design.shape[1]
        half = slots // 2
        piece = half // 4 if half % 2048 == 0 else half
        pieces = (piece, half - piece) if half > piece else (half,)
        chunk = next(c for c in (4096, 2048, 1024, 512, 256) if (slots - half) % c == 0)
        n_solve, lanes = n_src // SHARE, own * SHARE
        anywhere = pl.BlockSpec(memory_space=pl.ANY)
        vmem = pl.BlockSpec(memory_space=pltpu.VMEM)
        kept = lambda v: pltpu.with_memory_space_constraint(v, pltpu.VMEM)
        unit_index, residual, weight = (
            v.reshape(1, slots) for v in (unit_index, residual, weight)
        )
        rest = slots - half
        sums, weights = pl.pallas_call(
            functools.partial(beyond, half, chunk, n_src),
            out_shape=(
                pltpu.VMEM((ROWS, units), jnp.float32),
                pltpu.VMEM((1, 2 * LANES), jnp.float32),
            ),
            in_specs=[pl.BlockSpec(memory_space=pltpu.SMEM)] + [anywhere] * 4,
            out_specs=(vmem, vmem),
            scratch_shapes=[
                pltpu.VMEM((WIDTH, rest), jnp.float32),
                pltpu.VMEM((1, rest), jnp.int32),
                pltpu.VMEM((1, rest), jnp.float32),
                pltpu.VMEM((1, rest), jnp.float32),
                pltpu.VMEM((units, TILE), jnp.int16),
                pltpu.VMEM((1, (WIDTH + 3) * chunk), jnp.float32),
                pltpu.SemaphoreType.DMA((rest // chunk,)),
            ],
            name="beyond",
        )(obs_count, design, unit_index, residual, weight)
        result = pl.pallas_call(
            functools.partial(kernel, n_tm, n_src, pieces),
            out_shape=pltpu.VMEM((own, LANES), jnp.float32),
            in_specs=[pl.BlockSpec(memory_space=pltpu.SMEM)] + [anywhere] * 5 + [vmem] * 2,
            out_specs=vmem,
            scratch_shapes=[
                pltpu.VMEM((WIDTH, half), jnp.float32),
                pltpu.VMEM((1, half), jnp.int32),
                pltpu.VMEM((1, half), jnp.float32),
                pltpu.VMEM((1, half), jnp.float32),
                pltpu.VMEM((1, own), jnp.float32),
                pltpu.VMEM((n_solve, PACKED, LANES), jnp.float32),
                pltpu.VMEM((n_src, PACKED, LANES), jnp.float32),
                pltpu.VMEM((FOLD * PACKED, lanes), jnp.float32),
                pltpu.VMEM((1, LANES), jnp.float32),
                pltpu.VMEM((n_tm * n_solve, 1, LANES), jnp.float32),
                pltpu.VMEM((lanes, LANES), jnp.float32),
                pltpu.VMEM((own, LANES), jnp.float32),
                pltpu.VMEM((units, TILE), jnp.int16),
                pltpu.VMEM((1, (WIDTH + 3) * max(pieces)), jnp.float32),
                pltpu.SemaphoreType.DMA((len(pieces),)),
            ] + [pltpu.SemaphoreType.DMA] * 7,
            compiler_params=pltpu.CompilerParams(collective_id=0, has_side_effects=True),
            name="calibrate",
        )(
            obs_count,
            design,
            unit_index,
            residual,
            weight,
            damping.reshape(1, own),
            kept(sums),
            kept(weights),
        )
        result = kept(result)
        x, misfit = pl.pallas_call(
            hand_on,
            out_shape=(
                jax.ShapeDtypeStruct((own, WIDTH), jnp.float32),
                jax.ShapeDtypeStruct((1, 1), jnp.float32),
            ),
            in_specs=[vmem],
            out_specs=(vmem, vmem),
            name="hand_on",
        )(result)
        return x.T, misfit.reshape(())

    both = ("tm", "src")
    return jax.shard_map(
        on_device,
        mesh=mesh,
        in_specs=(P(None, both), P(both), P(both), P(both), P(both), P(both)),
        out_specs=(P(None, both), P()),
        check_vma=False,
    )
```

```python
import functools

import jax
import jax.numpy as jnp
from jax import lax
from jax.experimental import pallas as pl
from jax.experimental.pallas import tpu as pltpu
from jax.sharding import PartitionSpec as P

WIDTH = 16
HALF = 8
PAIRS = WIDTH * (WIDTH + 1) // 2
ROWS = PAIRS + WIDTH
EVEN = ROWS // WIDTH * WIDTH
LANES = 128
TILE = 256
SHARE = 4
FOLD = 4
PACKED = (ROWS + HALF) // FOLD
AUX = LANES // FOLD


def pair_row(i, j):
    k = (j - i) % WIDTH
    if k > HALF or (k == HALF and i >= HALF):
        i, j = j, i
        k = (j - i) % WIDTH
    return k * WIDTH + i


def stacked_rows(d0, d1, w, wr):
    w0, w1 = d0 * w, d1 * w
    rows = [d0 * w0, d1 * w1]
    sub = lax.broadcasted_iota(jnp.int32, d0.shape, 0)
    for k in range(1, HALF):
        r0 = pltpu.roll(w0, HALF - k, 0)
        r1 = pltpu.roll(w1, HALF - k, 0)
        low = sub < HALF - k
        rows.append(d0 * jnp.where(low, r0, r1))
        rows.append(d1 * jnp.where(low, r1, r0))
    rows.append(d0 * w1)
    rows.append(d0 * wr)
    rows.append(d1 * wr)
    return rows


def rsqrt(value):
    guess = lax.rsqrt(value)
    return guess * (1.5 - 0.5 * value * guess * guess)


def solve(entry, rhs, damping):
    a = {}
    for i in range(WIDTH):
        for j in range(i + 1):
            a[i, j] = entry(i, j)
        a[i, i] = a[i, i] + damping
    b = [rhs(i) for i in range(WIDTH)]
    inverse, forward = [], []
    for j in range(WIDTH):
        inv = rsqrt(a[j, j])
        inverse.append(inv)
        for i in range(j + 1, WIDTH):
            a[i, j] = a[i, j] * inv
        y = b[j] * inv
        forward.append(y)
        for i in range(j + 1, WIDTH):
            b[i] = b[i] - a[i, j] * y
            for k in range(j + 1, i + 1):
                a[i, k] = a[i, k] - a[i, j] * a[k, j]
    run = list(forward)
    x = [None] * WIDTH
    for i in reversed(range(WIDTH)):
        x[i] = run[i] * inverse[i]
        for k in range(i):
            run[k] = run[k] - a[i, k] * x[i]
    return x, forward


def skipping(k, me):
    return k + jnp.where(k >= me, 1, 0)


def ranked(k, me, n, up):
    k = skipping(k, jnp.where(up, me, n - 1 - me))
    return jnp.where(up, k, n - 1 - k)


def repeat(n, body):
    if n <= 32:
        for k in range(n):
            body(k)
    elif n:
        lax.fori_loop(0, n, lambda k, c: (body(k), c)[1], 0)


def block_at(place, n_src):
    q = n_src // 4
    solver = q + 1 + 2 * (place // SHARE)
    turn = place % SHARE
    away = jnp.where(solver < 2 * q, -q, q)
    return solver - turn % 2 + jnp.where(turn >= 2, away, 0)


def add_slots(accs, refs, ids, begin, chunk, first_unit, count, weights):
    design_ref, unit_ref, resid_ref, weight_ref = refs
    chi, total = weights
    for t in range(chunk // TILE):
        cols = pl.ds(begin + t * TILE, TILE)
        w = weight_ref[:, cols]
        live = begin + t * TILE + lax.broadcasted_iota(jnp.int32, w.shape, 1) < count
        w = jnp.where(live, w, 0.0)
        r = resid_ref[:, cols]
        wr = w * r
        rows = stacked_rows(design_ref[0:HALF, cols], design_ref[HALF:WIDTH, cols], w, wr)
        lhs = []
        for k in range(0, len(rows) - 1, 2):
            x = jnp.concatenate(rows[k:k + 2], axis=0)
            high = x.astype(jnp.bfloat16)
            lhs += [high, (x - high.astype(jnp.float32)).astype(jnp.bfloat16)]
        high = rows[-1].astype(jnp.bfloat16).astype(jnp.float32)
        lhs.append(jnp.concatenate([high, rows[-1] - high], axis=0).astype(jnp.bfloat16))
        lhs = jnp.concatenate(lhs, axis=0)
        unit = unit_ref[:, cols] - first_unit
        wrr = wr * r
        for k in range(TILE // LANES):
            chi = chi + wrr[:, k * LANES:(k + 1) * LANES]
            total = total + w[:, k * LANES:(k + 1) * LANES]
        q = t % 2
        for n, acc in enumerate(accs[q]):
            pltpu.matmul_push_rhs(
                one_hot(unit, n, ids), staging_register=0, mxu_index=q, transpose=True
            )
            pltpu.matmul_acc_lhs(acc, lhs, load_staged_rhs=0)
    return chi, total


def fill_ids(ids, own, n_src):
    place = lax.broadcasted_iota(jnp.int32, ids.shape, 0)
    unit = block_at(place // own, n_src) * own + place % own
    ids[...] = unit.astype(jnp.int16)


def one_hot(unit, n, ids):
    rows = min(ids.shape[0] - n * TILE, TILE)
    here = ids[pl.ds(n * TILE, rows), :] == unit.astype(jnp.int16)
    hot = jnp.where(here, jnp.bfloat16(1), jnp.bfloat16(0))
    if rows < TILE:
        hot = jnp.concatenate([hot, jnp.zeros((TILE - rows, TILE), jnp.bfloat16)], axis=0)
    return hot


def clear(accs):
    for q in range(2):
        for acc in accs[q]:
            pltpu.matmul_pop(acc)


def drained(accs, units):
    tiles = []
    for n in range(len(accs[0])):
        both = pltpu.matmul_pop(accs[0][n]) + pltpu.matmul_pop(accs[1][n])
        sums = [
            both[2 * k:2 * k + WIDTH] + both[2 * k + WIDTH:2 * k + 2 * WIDTH]
            for k in range(0, EVEN, WIDTH)
        ]
        sums.append(both[2 * EVEN:EVEN + ROWS] + both[EVEN + ROWS:])
        tiles.append(jnp.concatenate(sums, axis=0))
    return jnp.concatenate(tiles, axis=1)[:, 0:units]


def with_sums(body, units):
    tiles = -(-units // TILE)
    shape = (2 * ROWS, TILE)
    return pl.run_scoped(
        lambda *accs: body((accs[0:tiles], accs[tiles:2 * tiles])),
        *[pltpu.ACC(q)(shape, jnp.float32) for q in range(2) for _ in range(tiles)],
    )


def arrived(bytes_ref, chunk, sem):
    some = bytes_ref.at[:, pl.ds(0, (WIDTH + 3) * chunk)]
    pltpu.make_async_copy(some, some, sem).wait()


def beyond(
    start, chunk, n_src,
    count_ref, design_hbm, unit_hbm, resid_hbm, weight_hbm,
    sums_ref, weights_ref,
    design_ref, unit_ref, resid_ref, weight_ref, ids, bytes_ref, load,
):
    units = sums_ref.shape[1]
    slots = design_hbm.shape[1]
    first_unit = lax.axis_index("tm") * units
    count = count_ref[0]
    turns = (jnp.clip(count, start, slots) - start + chunk - 1) // chunk
    arrays = (
        (design_hbm, design_ref), (unit_hbm, unit_ref),
        (resid_hbm, resid_ref), (weight_hbm, weight_ref),
    )

    def fetch(step, which):
        far, here = arrays[which]
        size = pl.ds(pl.multiple_of(start + step * chunk, LANES), chunk)
        to = pl.ds(pl.multiple_of(step * chunk, LANES), chunk)
        return pltpu.make_async_copy(far.at[:, size], here.at[:, to], load.at[step])

    def fetch_all(step, c):
        for which in range(4):
            fetch(step, which).start()
        return c

    lax.fori_loop(0, turns, fetch_all, 0)

    def body(accs):
        zero = jnp.zeros((1, LANES), jnp.float32)

        def add(step, weights):
            arrived(bytes_ref, chunk, load.at[step])
            return add_slots(
                accs, (design_ref, unit_ref, resid_ref, weight_ref), ids,
                pl.multiple_of(step * chunk, LANES), chunk, first_unit, count - start, weights,
            )

        @pl.when(turns > 0)
        def _():
            clear(accs)
            fill_ids(ids, units // n_src, n_src)
            chi, total = lax.fori_loop(0, turns, add, (zero, zero))
            sums_ref[...] = drained(accs, units)
            weights_ref[:, 0:LANES] = chi
            weights_ref[:, LANES:2 * LANES] = total

        @pl.when(turns == 0)
        def _():
            sums_ref[...] = jnp.zeros_like(sums_ref)
            weights_ref[...] = jnp.zeros_like(weights_ref)

    with_sums(body, units)


def kernel(
    n_tm, n_src, pieces,
    count_ref, design_hbm, unit_hbm, resid_hbm, weight_hbm, damp_hbm, beyond_ref, weights_ref,
    out_ref,
    design_ref, unit_ref, resid_ref, weight_ref, damp_ref,
    part, got, summed, mine, heard, x_away, x_here,
    ids, bytes_ref, load, small, send_a, recv_a, send_b, recv_b, send_c, recv_c,
):
    tm, src = lax.axis_index("tm"), lax.axis_index("src")
    own = damp_ref.shape[1]
    units = own * n_src
    n_solve = n_src // SHARE
    first_solver = n_src // 4 + 1
    lanes = own * SHARE
    solves = (src >= first_solver) & (src < first_solver + 2 * n_solve) & (src % 2 == 1)
    rank = (src - first_solver) // 2
    up = src >= n_src // 2
    starts = [sum(pieces[:i]) for i in range(len(pieces))]

    arrays = (
        (design_hbm, design_ref), (unit_hbm, unit_ref),
        (resid_hbm, resid_ref), (weight_hbm, weight_ref),
    )

    def fetch(step, which):
        far, here = arrays[which]
        cols = pl.ds(starts[step], pieces[step])
        return pltpu.make_async_copy(far.at[:, cols], here.at[:, cols], load.at[step])

    x_away[...] = jnp.zeros_like(x_away)
    damp_copy = pltpu.make_async_copy(damp_hbm, damp_ref, small)
    for step in range(len(pieces)):
        for which in range(4):
            fetch(step, which).start()
    damp_copy.start()

    barrier = pltpu.get_barrier_semaphore()

    def greet(t, p):
        pl.semaphore_signal(
            barrier, inc=1, device_id={"tm": t, "src": p}, device_id_type=pl.DeviceIdType.MESH
        )

    @pl.when(solves)
    def _():
        repeat(n_src - 1, lambda k: greet(tm, skipping(k, src)))

    @pl.when(jnp.logical_not(solves))
    def _():
        repeat(n_solve, lambda k: greet(tm, first_solver + 2 * k))

    for dt in range(1, n_tm):
        repeat(n_solve, lambda k: greet((tm + dt) % n_tm, first_solver + 2 * k))

    first_unit = tm * units
    count = count_ref[0]
    fill_ids(ids, own, n_src)

    def body(accs):
        clear(accs)
        weights = weights_ref[:, 0:LANES], weights_ref[:, LANES:2 * LANES]
        for step in range(len(pieces)):
            arrived(bytes_ref, pieces[step], load.at[step])
            weights = add_slots(
                accs, (design_ref, unit_ref, resid_ref, weight_ref), ids,
                starts[step], pieces[step], first_unit, count, weights,
            )
        return (beyond_ref[...] + drained(accs, units), *weights)

    sums, chi, total = with_sums(body, units)
    damp_copy.wait()
    damping = jnp.concatenate([damp_ref[...]] * n_src, axis=1)
    place = lax.broadcasted_iota(jnp.int32, damping.shape, 1) // own
    damping = jnp.where(block_at(place, n_src) == src, damping, 0.0)
    fill = [jnp.zeros((1, units - LANES), jnp.float32)] if units > LANES else []
    chi = jnp.concatenate([chi] + fill, axis=1)
    total = jnp.concatenate([total] + fill, axis=1)
    none = jnp.zeros((FOLD * PACKED - ROWS - 3, units), jnp.float32)
    rows = jnp.concatenate([sums, damping, chi, total, none], axis=0)
    group = lax.broadcasted_iota(jnp.int32, (PACKED, LANES), 1) // AUX

    def pack(k):
        first = k * lanes // LANES * LANES
        for g in range(FOLD):
            more = rows[g * PACKED:(g + 1) * PACKED, first:first + LANES]
            shift = (g * AUX - k * lanes) % LANES
            more = pltpu.roll(more, shift, 1) if shift else more
            message = jnp.where(group == g, more, message) if g else more
        part[k] = message

    def send_to(k):
        pltpu.make_async_remote_copy(
            src_ref=part.at[k], dst_ref=got.at[src], send_sem=send_a, recv_sem=recv_a,
            device_id={"tm": tm, "src": first_solver + 2 * k},
            device_id_type=pl.DeviceIdType.MESH,
        ).start()

    pack(0)

    @pl.when(jnp.logical_not(solves))
    def _():
        pl.semaphore_wait(barrier, n_solve)
        send_to(0)

    for k in range(1, n_solve):
        pack(k)

    def wait_bytes(ref, n, sem):
        some = ref.at[pl.ds(0, n)]
        pltpu.make_async_copy(some, some, sem).wait()

    away = jnp.where(up, n_src // 4, -(n_src // 4))

    def hand_over(i, p):
        return pltpu.make_async_remote_copy(
            src_ref=x_away.at[pl.ds(i * own, own)], dst_ref=x_here,
            send_sem=send_c, recv_sem=recv_c,
            device_id={"tm": tm, "src": p}, device_id_type=pl.DeviceIdType.MESH,
        )

    me = tm * n_solve + rank

    def tell(t, p):
        pltpu.make_async_remote_copy(
            src_ref=mine, dst_ref=heard.at[me], send_sem=send_b, recv_sem=recv_b,
            device_id={"tm": t, "src": p}, device_id_type=pl.DeviceIdType.MESH,
        ).start()

    def tell_both(k):
        p = skipping(k, src)
        for t in range(n_tm):
            tell(t, p)

    @pl.when(solves)
    def _():
        pl.semaphore_wait(barrier, n_tm * n_src - 1)
        repeat(n_solve - 1, lambda k: send_to(ranked(k, rank, n_solve, up)))
        got[src] = part[rank]
        wait_bytes(got, n_src - 1, recv_a)
        each = [got[p] for p in range(n_src)]
        while len(each) > 1:
            each = [a + b for a, b in zip(each[::2], each[1::2])] + each[len(each) // 2 * 2:]
        both = each[0]
        for g in range(FOLD):
            more = pltpu.roll(both, LANES - g * AUX, 1) if g else both
            summed[pl.ds(g * PACKED, PACKED), :] = more[:, 0:lanes]
        damping, chi, total = (summed[pl.ds(ROWS + i, 1), :] for i in range(3))
        x, forward = solve(
            lambda i, j: summed[pl.ds(pair_row(i, j), 1), :],
            lambda i: summed[pl.ds(PAIRS + i, 1), :],
            damping,
        )
        terms = jnp.zeros_like(damping)
        squared = jnp.zeros_like(damping)
        for i in reversed(range(WIDTH)):
            terms = terms + forward[i] * forward[i]
            squared = squared + x[i] * x[i]
        terms = terms + damping * squared
        none = jnp.zeros((1, LANES // 2 - lanes), jnp.float32)
        mine[...] = jnp.concatenate([chi - terms, none, total, none], axis=1)
        heard[me] = mine[...]
        repeat(n_src - 1, tell_both)
        for dt in range(1, n_tm):
            tell((tm + dt) % n_tm, src)
        answer = jnp.transpose(jnp.concatenate(x, axis=0))
        x_away[:, 0:WIDTH] = answer
        for i, p in ((2, src + away), (3, src - 1 + away), (1, src - 1)):
            hand_over(i, p).start()
        out_ref[:, 0:WIDTH] = answer[0:own]
        wait_bytes(part, n_solve - 1, send_a)
        wait_bytes(heard, n_tm * n_solve - 1, recv_b)

    @pl.when(jnp.logical_not(solves))
    def _():
        repeat(n_solve - 1, lambda k: send_to(k + 1))
        hand_over(0, src).wait_recv()
        out_ref[...] = x_here[...]
        wait_bytes(part, n_solve, send_a)
        wait_bytes(heard, n_tm * n_solve, recv_b)

    both = jnp.sum(heard[...].reshape(n_tm * n_solve, LANES), axis=0, keepdims=True)
    front = lax.broadcasted_iota(jnp.int32, (1, LANES), 1) < LANES // 2
    chi_all = jnp.sum(jnp.where(front, both, 0.0), axis=1, keepdims=True)
    total_all = jnp.sum(jnp.where(front, 0.0, both), axis=1, keepdims=True)
    out_ref[0:1, WIDTH:WIDTH + 1] = chi_all / total_all

    @pl.when(solves)
    def _():
        some = x_away.at[pl.ds(own, 3 * own)]
        pltpu.make_async_copy(some, some, send_c).wait()
        rest = n_tm * n_src - 1
        while rest > 0:
            some = min(rest, n_tm * n_solve)
            wait_bytes(heard, some, send_b)
            rest -= some


def hand_on(both_ref, x_out, misfit_out):
    x_out[...] = both_ref[:, 0:WIDTH]
    misfit_out[...] = both_ref[0:1, WIDTH:WIDTH + 1]


def solution(mesh):
    n_tm, n_src = mesh.shape["tm"], mesh.shape["src"]

    def on_device(design, unit_index, residual, weight, obs_count, damping):
        own = damping.shape[0]
        units = own * n_src
        slots = design.shape[1]
        half = slots // 2
        piece = half // 4 if half % 2048 == 0 else half
        pieces = (piece, half - piece) if half > piece else (half,)
        chunk = next(c for c in (4096, 2048, 1024, 512, 256) if (slots - half) % c == 0)
        n_solve, lanes = n_src // SHARE, own * SHARE
        anywhere = pl.BlockSpec(memory_space=pl.ANY)
        vmem = pl.BlockSpec(memory_space=pltpu.VMEM)
        kept = lambda v: pltpu.with_memory_space_constraint(v, pltpu.VMEM)
        unit_index, residual, weight = (
            v.reshape(1, slots) for v in (unit_index, residual, weight)
        )
        rest = slots - half
        sums, weights = pl.pallas_call(
            functools.partial(beyond, half, chunk, n_src),
            out_shape=(
                pltpu.VMEM((ROWS, units), jnp.float32),
                pltpu.VMEM((1, 2 * LANES), jnp.float32),
            ),
            in_specs=[pl.BlockSpec(memory_space=pltpu.SMEM)] + [anywhere] * 4,
            out_specs=(vmem, vmem),
            scratch_shapes=[
                pltpu.VMEM((WIDTH, rest), jnp.float32),
                pltpu.VMEM((1, rest), jnp.int32),
                pltpu.VMEM((1, rest), jnp.float32),
                pltpu.VMEM((1, rest), jnp.float32),
                pltpu.VMEM((units, TILE), jnp.int16),
                pltpu.VMEM((1, (WIDTH + 3) * chunk), jnp.float32),
                pltpu.SemaphoreType.DMA((rest // chunk,)),
            ],
            name="beyond",
        )(obs_count, design, unit_index, residual, weight)
        result = pl.pallas_call(
            functools.partial(kernel, n_tm, n_src, pieces),
            out_shape=pltpu.VMEM((own, LANES), jnp.float32),
            in_specs=[pl.BlockSpec(memory_space=pltpu.SMEM)] + [anywhere] * 5 + [vmem] * 2,
            out_specs=vmem,
            scratch_shapes=[
                pltpu.VMEM((WIDTH, half), jnp.float32),
                pltpu.VMEM((1, half), jnp.int32),
                pltpu.VMEM((1, half), jnp.float32),
                pltpu.VMEM((1, half), jnp.float32),
                pltpu.VMEM((1, own), jnp.float32),
                pltpu.VMEM((n_solve, PACKED, LANES), jnp.float32),
                pltpu.VMEM((n_src, PACKED, LANES), jnp.float32),
                pltpu.VMEM((FOLD * PACKED, lanes), jnp.float32),
                pltpu.VMEM((1, LANES), jnp.float32),
                pltpu.VMEM((n_tm * n_solve, 1, LANES), jnp.float32),
                pltpu.VMEM((lanes, LANES), jnp.float32),
                pltpu.VMEM((own, LANES), jnp.float32),
                pltpu.VMEM((units, TILE), jnp.int16),
                pltpu.VMEM((1, (WIDTH + 3) * max(pieces)), jnp.float32),
                pltpu.SemaphoreType.DMA((len(pieces),)),
            ] + [pltpu.SemaphoreType.DMA] * 7,
            compiler_params=pltpu.CompilerParams(collective_id=0, has_side_effects=True),
            name="calibrate",
        )(
            obs_count,
            design,
            unit_index,
            residual,
            weight,
            damping.reshape(1, own),
            kept(sums),
            kept(weights),
        )
        result = kept(result)
        x, misfit = pl.pallas_call(
            hand_on,
            out_shape=(
                jax.ShapeDtypeStruct((own, WIDTH), jnp.float32),
                jax.ShapeDtypeStruct((1, 1), jnp.float32),
            ),
            in_specs=[vmem],
            out_specs=(vmem, vmem),
            name="hand_on",
        )(result)
        return x.T, misfit.reshape(())

    both = ("tm", "src")
    return jax.shard_map(
        on_device,
        mesh=mesh,
        in_specs=(P(None, both), P(both), P(both), P(both), P(both), P(both)),
        out_specs=(P(None, both), P()),
        check_vma=False,
    )
```

```python
import functools

import jax
import jax.numpy as jnp
from jax import lax
from jax.experimental import pallas as pl
from jax.experimental.pallas import tpu as pltpu
from jax.sharding import PartitionSpec as P

WIDTH = 16
HALF = 8
PAIRS = WIDTH * (WIDTH + 1) // 2
ROWS = PAIRS + WIDTH
EVEN = ROWS // WIDTH * WIDTH
LANES = 128
TILE = 256
SHARE = 4
FOLD = 4
PACKED = (ROWS + HALF) // FOLD
AUX = LANES // FOLD


def pair_row(i, j):
    k = (j - i) % WIDTH
    if k > HALF or (k == HALF and i >= HALF):
        i, j = j, i
        k = (j - i) % WIDTH
    return k * WIDTH + i


def stacked_rows(d0, d1, w, wr):
    w0, w1 = d0 * w, d1 * w
    rows = [d0 * w0, d1 * w1]
    sub = lax.broadcasted_iota(jnp.int32, d0.shape, 0)
    for k in range(1, HALF):
        r0 = pltpu.roll(w0, HALF - k, 0)
        r1 = pltpu.roll(w1, HALF - k, 0)
        low = sub < HALF - k
        rows.append(d0 * jnp.where(low, r0, r1))
        rows.append(d1 * jnp.where(low, r1, r0))
    rows.append(d0 * w1)
    rows.append(d0 * wr)
    rows.append(d1 * wr)
    return rows


def rsqrt(value):
    guess = lax.rsqrt(value)
    return guess * (1.5 - 0.5 * value * guess * guess)


def solve(entry, rhs, damping):
    a = {}
    for i in range(WIDTH):
        for j in range(i + 1):
            a[i, j] = entry(i, j)
        a[i, i] = a[i, i] + damping
    b = [rhs(i) for i in range(WIDTH)]
    inverse, forward = [], []
    for j in range(WIDTH):
        inv = rsqrt(a[j, j])
        inverse.append(inv)
        for i in range(j + 1, WIDTH):
            a[i, j] = a[i, j] * inv
        y = b[j] * inv
        forward.append(y)
        for i in range(j + 1, WIDTH):
            b[i] = b[i] - a[i, j] * y
            for k in range(j + 1, i + 1):
                a[i, k] = a[i, k] - a[i, j] * a[k, j]
    run = list(forward)
    x = [None] * WIDTH
    for i in reversed(range(WIDTH)):
        x[i] = run[i] * inverse[i]
        for k in range(i):
            run[k] = run[k] - a[i, k] * x[i]
    return x, forward


def skipping(k, me):
    return k + jnp.where(k >= me, 1, 0)


def ranked(k, me, n, up):
    k = skipping(k, jnp.where(up, me, n - 1 - me))
    return jnp.where(up, k, n - 1 - k)


def repeat(n, body):
    if n <= 32:
        for k in range(n):
            body(k)
    elif n:
        lax.fori_loop(0, n, lambda k, c: (body(k), c)[1], 0)


def block_at(place, n_src):
    q = n_src // 4
    solver = q + 1 + 2 * (place // SHARE)
    turn = place % SHARE
    away = jnp.where(solver < 2 * q, -q, q)
    return solver - turn % 2 + jnp.where(turn >= 2, away, 0)


def add_slots(accs, refs, ids, begin, chunk, first_unit, count, weights):
    design_ref, unit_ref, resid_ref, weight_ref = refs
    chi, total = weights
    for t in range(chunk // TILE):
        cols = pl.ds(begin + t * TILE, TILE)
        w = weight_ref[:, cols]
        live = begin + t * TILE + lax.broadcasted_iota(jnp.int32, w.shape, 1) < count
        w = jnp.where(live, w, 0.0)
        r = resid_ref[:, cols]
        wr = w * r
        rows = stacked_rows(design_ref[0:HALF, cols], design_ref[HALF:WIDTH, cols], w, wr)
        lhs = []
        for k in range(0, len(rows) - 1, 2):
            x = jnp.concatenate(rows[k:k + 2], axis=0)
            high = x.astype(jnp.bfloat16)
            lhs += [high, (x - high.astype(jnp.float32)).astype(jnp.bfloat16)]
        high = rows[-1].astype(jnp.bfloat16).astype(jnp.float32)
        lhs.append(jnp.concatenate([high, rows[-1] - high], axis=0).astype(jnp.bfloat16))
        lhs = jnp.concatenate(lhs, axis=0)
        unit = unit_ref[:, cols] - first_unit
        wrr = wr * r
        for k in range(TILE // LANES):
            chi = chi + wrr[:, k * LANES:(k + 1) * LANES]
            total = total + w[:, k * LANES:(k + 1) * LANES]
        q = t % 2
        for n, acc in enumerate(accs[q]):
            pltpu.matmul_push_rhs(
                one_hot(unit, n, ids), staging_register=0, mxu_index=q, transpose=True
            )
            pltpu.matmul_acc_lhs(acc, lhs, load_staged_rhs=0)
    return chi, total


def fill_ids(ids, own, n_src):
    place = lax.broadcasted_iota(jnp.int32, ids.shape, 0)
    unit = block_at(place // own, n_src) * own + place % own
    ids[...] = unit.astype(jnp.int16)


def one_hot(unit, n, ids):
    rows = min(ids.shape[0] - n * TILE, TILE)
    here = ids[pl.ds(n * TILE, rows), :] == unit.astype(jnp.int16)
    hot = jnp.where(here, jnp.bfloat16(1), jnp.bfloat16(0))
    if rows < TILE:
        hot = jnp.concatenate([hot, jnp.zeros((TILE - rows, TILE), jnp.bfloat16)], axis=0)
    return hot


def clear(accs):
    for q in range(2):
        for acc in accs[q]:
            pltpu.matmul_pop(acc)


def drained(accs, units):
    tiles = []
    for n in range(len(accs[0])):
        both = pltpu.matmul_pop(accs[0][n]) + pltpu.matmul_pop(accs[1][n])
        sums = [
            both[2 * k:2 * k + WIDTH] + both[2 * k + WIDTH:2 * k + 2 * WIDTH]
            for k in range(0, EVEN, WIDTH)
        ]
        sums.append(both[2 * EVEN:EVEN + ROWS] + both[EVEN + ROWS:])
        tiles.append(jnp.concatenate(sums, axis=0))
    return jnp.concatenate(tiles, axis=1)[:, 0:units]


def with_sums(body, units):
    tiles = -(-units // TILE)
    shape = (2 * ROWS, TILE)
    return pl.run_scoped(
        lambda *accs: body((accs[0:tiles], accs[tiles:2 * tiles])),
        *[pltpu.ACC(q)(shape, jnp.float32) for q in range(2) for _ in range(tiles)],
    )


def arrived(bytes_ref, chunk, sem):
    some = bytes_ref.at[:, pl.ds(0, (WIDTH + 3) * chunk)]
    pltpu.make_async_copy(some, some, sem).wait()


def beyond(
    start, chunk, n_src,
    count_ref, design_hbm, unit_hbm, resid_hbm, weight_hbm,
    sums_ref, weights_ref,
    design_ref, unit_ref, resid_ref, weight_ref, ids, bytes_ref, load,
):
    units = sums_ref.shape[1]
    slots = design_hbm.shape[1]
    first_unit = lax.axis_index("tm") * units
    count = count_ref[0]
    turns = (jnp.clip(count, start, slots) - start + chunk - 1) // chunk
    arrays = (
        (design_hbm, design_ref), (unit_hbm, unit_ref),
        (resid_hbm, resid_ref), (weight_hbm, weight_ref),
    )

    def fetch(step, which):
        far, here = arrays[which]
        size = pl.ds(pl.multiple_of(start + step * chunk, LANES), chunk)
        to = pl.ds(pl.multiple_of(step * chunk, LANES), chunk)
        return pltpu.make_async_copy(far.at[:, size], here.at[:, to], load.at[step])

    def fetch_all(step, c):
        for which in range(4):
            fetch(step, which).start()
        return c

    lax.fori_loop(0, turns, fetch_all, 0)

    def body(accs):
        zero = jnp.zeros((1, LANES), jnp.float32)

        def add(step, weights):
            arrived(bytes_ref, chunk, load.at[step])
            return add_slots(
                accs, (design_ref, unit_ref, resid_ref, weight_ref), ids,
                pl.multiple_of(step * chunk, LANES), chunk, first_unit, count - start, weights,
            )

        @pl.when(turns > 0)
        def _():
            clear(accs)
            fill_ids(ids, units // n_src, n_src)
            chi, total = lax.fori_loop(0, turns, add, (zero, zero))
            sums_ref[...] = drained(accs, units)
            weights_ref[:, 0:LANES] = chi
            weights_ref[:, LANES:2 * LANES] = total

        @pl.when(turns == 0)
        def _():
            sums_ref[...] = jnp.zeros_like(sums_ref)
            weights_ref[...] = jnp.zeros_like(weights_ref)

    with_sums(body, units)


def kernel(
    n_tm, n_src, pieces,
    count_ref, design_hbm, unit_hbm, resid_hbm, weight_hbm, damp_hbm, beyond_ref, weights_ref,
    out_ref,
    design_ref, unit_ref, resid_ref, weight_ref, damp_ref,
    part, got, summed, mine, heard, x_away, x_here,
    ids, bytes_ref, load, small, send_a, recv_a, send_b, recv_b, send_c, recv_c,
):
    tm, src = lax.axis_index("tm"), lax.axis_index("src")
    own = damp_ref.shape[1]
    units = own * n_src
    n_solve = n_src // SHARE
    first_solver = n_src // 4 + 1
    lanes = own * SHARE
    solves = (src >= first_solver) & (src < first_solver + 2 * n_solve) & (src % 2 == 1)
    rank = (src - first_solver) // 2
    up = src >= n_src // 2
    starts = [sum(pieces[:i]) for i in range(len(pieces))]

    arrays = (
        (design_hbm, design_ref), (unit_hbm, unit_ref),
        (resid_hbm, resid_ref), (weight_hbm, weight_ref),
    )

    def fetch(step, which):
        far, here = arrays[which]
        cols = pl.ds(starts[step], pieces[step])
        return pltpu.make_async_copy(far.at[:, cols], here.at[:, cols], load.at[step])

    x_away[...] = jnp.zeros_like(x_away)
    damp_copy = pltpu.make_async_copy(damp_hbm, damp_ref, small)
    for step in range(len(pieces)):
        for which in range(4):
            fetch(step, which).start()
    damp_copy.start()

    barrier = pltpu.get_barrier_semaphore()

    def greet(t, p):
        pl.semaphore_signal(
            barrier, inc=1, device_id={"tm": t, "src": p}, device_id_type=pl.DeviceIdType.MESH
        )

    @pl.when(solves)
    def _():
        repeat(n_src - 1, lambda k: greet(tm, skipping(k, src)))

    @pl.when(jnp.logical_not(solves))
    def _():
        repeat(n_solve, lambda k: greet(tm, first_solver + 2 * k))

    for dt in range(1, n_tm):
        repeat(n_solve, lambda k: greet((tm + dt) % n_tm, first_solver + 2 * k))

    first_unit = tm * units
    count = count_ref[0]
    fill_ids(ids, own, n_src)

    def body(accs):
        clear(accs)
        weights = weights_ref[:, 0:LANES], weights_ref[:, LANES:2 * LANES]
        for step in range(len(pieces)):
            arrived(bytes_ref, pieces[step], load.at[step])
            weights = add_slots(
                accs, (design_ref, unit_ref, resid_ref, weight_ref), ids,
                starts[step], pieces[step], first_unit, count, weights,
            )
        return (beyond_ref[...] + drained(accs, units), *weights)

    sums, chi, total = with_sums(body, units)
    damp_copy.wait()
    damping = jnp.concatenate([damp_ref[...]] * n_src, axis=1)
    place = lax.broadcasted_iota(jnp.int32, damping.shape, 1) // own
    damping = jnp.where(block_at(place, n_src) == src, damping, 0.0)
    fill = [jnp.zeros((1, units - LANES), jnp.float32)] if units > LANES else []
    chi = jnp.concatenate([chi] + fill, axis=1)
    total = jnp.concatenate([total] + fill, axis=1)
    none = jnp.zeros((FOLD * PACKED - ROWS - 3, units), jnp.float32)
    rows = jnp.concatenate([sums, damping, chi, total, none], axis=0)
    group = lax.broadcasted_iota(jnp.int32, (PACKED, LANES), 1) // AUX

    def pack(k):
        first = k * lanes // LANES * LANES
        for g in range(FOLD):
            more = rows[g * PACKED:(g + 1) * PACKED, first:first + LANES]
            shift = (g * AUX - k * lanes) % LANES
            more = pltpu.roll(more, shift, 1) if shift else more
            message = jnp.where(group == g, more, message) if g else more
        part[k] = message

    def send_to(k):
        pltpu.make_async_remote_copy(
            src_ref=part.at[k], dst_ref=got.at[src], send_sem=send_a, recv_sem=recv_a,
            device_id={"tm": tm, "src": first_solver + 2 * k},
            device_id_type=pl.DeviceIdType.MESH,
        ).start()

    pack(0)

    @pl.when(jnp.logical_not(solves))
    def _():
        pl.semaphore_wait(barrier, n_solve)
        send_to(0)

    for k in range(1, n_solve):
        pack(k)

    def wait_bytes(ref, n, sem):
        some = ref.at[pl.ds(0, n)]
        pltpu.make_async_copy(some, some, sem).wait()

    away = jnp.where(up, n_src // 4, -(n_src // 4))

    def hand_over(i, p):
        return pltpu.make_async_remote_copy(
            src_ref=x_away.at[pl.ds(i * own, own)], dst_ref=x_here,
            send_sem=send_c, recv_sem=recv_c,
            device_id={"tm": tm, "src": p}, device_id_type=pl.DeviceIdType.MESH,
        )

    me = tm * n_solve + rank

    def tell(t, p):
        pltpu.make_async_remote_copy(
            src_ref=mine, dst_ref=heard.at[me], send_sem=send_b, recv_sem=recv_b,
            device_id={"tm": t, "src": p}, device_id_type=pl.DeviceIdType.MESH,
        ).start()

    def tell_both(k):
        p = skipping(k, src)
        for t in range(n_tm):
            tell(t, p)

    @pl.when(solves)
    def _():
        pl.semaphore_wait(barrier, n_tm * n_src - 1)
        repeat(n_solve - 1, lambda k: send_to(ranked(k, rank, n_solve, up)))
        got[src] = part[rank]
        wait_bytes(got, n_src - 1, recv_a)
        each = [got[p] for p in range(n_src)]
        while len(each) > 1:
            each = [a + b for a, b in zip(each[::2], each[1::2])] + each[len(each) // 2 * 2:]
        both = each[0]
        for g in range(FOLD):
            more = pltpu.roll(both, LANES - g * AUX, 1) if g else both
            summed[pl.ds(g * PACKED, PACKED), :] = more[:, 0:lanes]
        damping, chi, total = (summed[pl.ds(ROWS + i, 1), :] for i in range(3))
        x, forward = solve(
            lambda i, j: summed[pl.ds(pair_row(i, j), 1), :],
            lambda i: summed[pl.ds(PAIRS + i, 1), :],
            damping,
        )
        terms = jnp.zeros_like(damping)
        squared = jnp.zeros_like(damping)
        for i in reversed(range(WIDTH)):
            terms = terms + forward[i] * forward[i]
            squared = squared + x[i] * x[i]
        terms = terms + damping * squared
        none = jnp.zeros((1, LANES // 2 - lanes), jnp.float32)
        mine[...] = jnp.concatenate([chi - terms, none, total, none], axis=1)
        heard[me] = mine[...]
        repeat(n_src - 1, tell_both)
        for dt in range(1, n_tm):
            tell((tm + dt) % n_tm, src)
        answer = jnp.transpose(jnp.concatenate(x, axis=0))
        x_away[:, 0:WIDTH] = answer
        for i, p in ((2, src + away), (3, src - 1 + away), (1, src - 1)):
            hand_over(i, p).start()
        out_ref[:, 0:WIDTH] = answer[0:own]
        wait_bytes(part, n_solve - 1, send_a)
        wait_bytes(heard, n_tm * n_solve - 1, recv_b)

    @pl.when(jnp.logical_not(solves))
    def _():
        repeat(n_solve - 1, lambda k: send_to(k + 1))
        hand_over(0, src).wait_recv()
        out_ref[...] = x_here[...]
        wait_bytes(part, n_solve, send_a)
        wait_bytes(heard, n_tm * n_solve, recv_b)

    both = jnp.sum(heard[...].reshape(n_tm * n_solve, LANES), axis=0, keepdims=True)
    front = lax.broadcasted_iota(jnp.int32, (1, LANES), 1) < LANES // 2
    chi_all = jnp.sum(jnp.where(front, both, 0.0), axis=1, keepdims=True)
    total_all = jnp.sum(jnp.where(front, 0.0, both), axis=1, keepdims=True)
    out_ref[0:1, WIDTH:WIDTH + 1] = chi_all / total_all

    @pl.when(solves)
    def _():
        some = x_away.at[pl.ds(own, 3 * own)]
        pltpu.make_async_copy(some, some, send_c).wait()
        rest = n_tm * n_src - 1
        while rest > 0:
            some = min(rest, n_tm * n_solve)
            wait_bytes(heard, some, send_b)
            rest -= some


def hand_on(both_ref, x_out, misfit_out):
    x_out[...] = both_ref[:, 0:WIDTH]
    misfit_out[...] = both_ref[0:1, WIDTH:WIDTH + 1]


def solution(mesh):
    n_tm, n_src = mesh.shape["tm"], mesh.shape["src"]

    def on_device(design, unit_index, residual, weight, obs_count, damping):
        own = damping.shape[0]
        units = own * n_src
        slots = design.shape[1]
        half = slots // 2
        pieces = (half,)
        chunk = next(c for c in (8192, 4096, 2048, 1024, 512, 256) if (slots - half) % c == 0)
        n_solve, lanes = n_src // SHARE, own * SHARE
        anywhere = pl.BlockSpec(memory_space=pl.ANY)
        vmem = pl.BlockSpec(memory_space=pltpu.VMEM)
        kept = lambda v: pltpu.with_memory_space_constraint(v, pltpu.VMEM)
        unit_index, residual, weight = (
            v.reshape(1, slots) for v in (unit_index, residual, weight)
        )
        rest = slots - half
        sums, weights = pl.pallas_call(
            functools.partial(beyond, half, chunk, n_src),
            out_shape=(
                pltpu.VMEM((ROWS, units), jnp.float32),
                pltpu.VMEM((1, 2 * LANES), jnp.float32),
            ),
            in_specs=[pl.BlockSpec(memory_space=pltpu.SMEM)] + [anywhere] * 4,
            out_specs=(vmem, vmem),
            scratch_shapes=[
                pltpu.VMEM((WIDTH, rest), jnp.float32),
                pltpu.VMEM((1, rest), jnp.int32),
                pltpu.VMEM((1, rest), jnp.float32),
                pltpu.VMEM((1, rest), jnp.float32),
                pltpu.VMEM((units, TILE), jnp.int16),
                pltpu.VMEM((1, (WIDTH + 3) * chunk), jnp.float32),
                pltpu.SemaphoreType.DMA((rest // chunk,)),
            ],
            name="beyond",
        )(obs_count, design, unit_index, residual, weight)
        result = pl.pallas_call(
            functools.partial(kernel, n_tm, n_src, pieces),
            out_shape=pltpu.VMEM((own, LANES), jnp.float32),
            in_specs=[pl.BlockSpec(memory_space=pltpu.SMEM)] + [anywhere] * 5 + [vmem] * 2,
            out_specs=vmem,
            scratch_shapes=[
                pltpu.VMEM((WIDTH, half), jnp.float32),
                pltpu.VMEM((1, half), jnp.int32),
                pltpu.VMEM((1, half), jnp.float32),
                pltpu.VMEM((1, half), jnp.float32),
                pltpu.VMEM((1, own), jnp.float32),
                pltpu.VMEM((n_solve, PACKED, LANES), jnp.float32),
                pltpu.VMEM((n_src, PACKED, LANES), jnp.float32),
                pltpu.VMEM((FOLD * PACKED, lanes), jnp.float32),
                pltpu.VMEM((1, LANES), jnp.float32),
                pltpu.VMEM((n_tm * n_solve, 1, LANES), jnp.float32),
                pltpu.VMEM((lanes, LANES), jnp.float32),
                pltpu.VMEM((own, LANES), jnp.float32),
                pltpu.VMEM((units, TILE), jnp.int16),
                pltpu.VMEM((1, (WIDTH + 3) * max(pieces)), jnp.float32),
                pltpu.SemaphoreType.DMA((len(pieces),)),
            ] + [pltpu.SemaphoreType.DMA] * 7,
            compiler_params=pltpu.CompilerParams(collective_id=0, has_side_effects=True),
            name="calibrate",
        )(
            obs_count,
            design,
            unit_index,
            residual,
            weight,
            damping.reshape(1, own),
            kept(sums),
            kept(weights),
        )
        result = kept(result)
        x, misfit = pl.pallas_call(
            hand_on,
            out_shape=(
                jax.ShapeDtypeStruct((own, WIDTH), jnp.float32),
                jax.ShapeDtypeStruct((1, 1), jnp.float32),
            ),
            in_specs=[vmem],
            out_specs=(vmem, vmem),
            name="hand_on",
        )(result)
        return x.T, misfit.reshape(())

    both = ("tm", "src")
    return jax.shard_map(
        on_device,
        mesh=mesh,
        in_specs=(P(None, both), P(both), P(both), P(both), P(both), P(both)),
        out_specs=(P(None, both), P()),
        check_vma=False,
    )
```
